8 devices in a mesh: dp: 2 (over z, y), tp: 4 (over x, core).
Axes of the slice: x: 2, y: 2, z: 1, core: 2. Of those that a mesh axis runs over, the one named last changes fastest.
Arguments:
- token_ids: int32 [512], P('dp'), parts along dimension 0
- emb_table: bfloat16 [50304, 1024], P('tp')
- norm_gain: bfloat16 [1024], replicated
- w_in: bfloat16 [1024, 4096], P(None, 'tp')
- w_out: bfloat16 [4096, 1024], P('tp')
- d_out: bfloat16 [512, 1024], P(('dp', 'tp')), parts along dimension 0
Outputs:
- output 1: bfloat16 [512, 1024], P(('dp', 'tp')), parts along dimension 0
- output 2: float32 [100608, 1024], P(('dp', 'tp')), parts along dimension 0
- output 3: float32 [2048, 4096], P('dp', 'tp'), parts along dimension 0
- output 4: float32 [8192, 1024], P(('dp', 'tp')), parts along dimension 0
There are 2 independent parts. The reference program is written for one: setup_inputs(seed, part) draws one part's arguments, and reference() takes and returns one part's arrays. A program takes and returns all parts, laid end to end along the dimension named above; an argument that names none is the same for every part.
All inputs are finite; a program needn't handle non-finite values.
Results may differ from the reference program's by a relative error of at most 0.00879555.
Values are sent between devices in bfloat16 or wider.
A program may use at most 1 GiB of HBM per device.

```python
import math
import jax
import jax.numpy as jnp
from jax import lax

VOCAB_SIZE = 50304
MODEL_DIM = 1024
HIDDEN_DIM = 4096
TOKENS = 256

EPS = 1e-6
VOCAB_BITS = math.ceil(math.log2(VOCAB_SIZE))


def draw_ids(id_key):
    key_level, key_zipf, key_flat, key_pick = jax.random.split(id_key, 4)
    bit_level = jax.random.randint(key_level, (TOKENS,), 0, VOCAB_BITS + 1, dtype=jnp.int32)
    id_span = jnp.left_shift(jnp.ones_like(bit_level), bit_level)
    zipf_ids = jax.random.randint(key_zipf, (TOKENS,), 0, id_span, dtype=jnp.int32) % VOCAB_SIZE
    flat_ids = jax.random.randint(key_flat, (TOKENS,), 0, VOCAB_SIZE, dtype=jnp.int32)
    choice = jax.random.randint(key_pick, (TOKENS,), 0, 10, dtype=jnp.int32)
    mixed_ids = jnp.where(choice < 7, zipf_ids, flat_ids)
    end_ids = jnp.array([0, VOCAB_SIZE - 1], dtype=jnp.int32)
    return jnp.concatenate([end_ids, mixed_ids[2:]]).astype(jnp.int32)


def setup_inputs(seed: int = 0, part: int = 0) -> dict:
    key_table, key_gain, key_in, key_out = jax.random.split(jax.random.key(seed), 4)
    part_key = jax.random.fold_in(jax.random.key(seed + 1), part)
    key_ids, key_dout = jax.random.split(part_key, 2)
    emb_table = jax.random.normal(key_table, (VOCAB_SIZE, MODEL_DIM), jnp.float32).astype(jnp.bfloat16)
    norm_gain = (1.0 + 0.5 * jax.random.normal(key_gain, (MODEL_DIM,), jnp.float32)).astype(jnp.bfloat16)
    w_in = (jax.random.normal(key_in, (MODEL_DIM, HIDDEN_DIM), jnp.float32) * MODEL_DIM ** -0.5).astype(jnp.bfloat16)
    w_out = (jax.random.normal(key_out, (HIDDEN_DIM, MODEL_DIM), jnp.float32) * (1.5 * HIDDEN_DIM ** -0.5)).astype(jnp.bfloat16)
    token_ids = draw_ids(key_ids)
    d_out = (jax.random.normal(key_dout, (TOKENS, MODEL_DIM), jnp.float32) * TOKENS ** -0.5).astype(jnp.bfloat16)
    return {"token_ids": token_ids, "emb_table": emb_table, "norm_gain": norm_gain, "w_in": w_in, "w_out": w_out, "d_out": d_out}


def reference(token_ids, emb_table, norm_gain, w_in, w_out, d_out):
    embedded = jnp.take(emb_table, token_ids, axis=0)
    embedded_f32 = embedded.astype(jnp.float32)
    inv_rms = lax.rsqrt(jnp.mean(embedded_f32 * embedded_f32, axis=-1, keepdims=True) + EPS)
    gain_f32 = norm_gain.astype(jnp.float32)
    normed = (embedded_f32 * inv_rms * gain_f32).astype(jnp.bfloat16)
    pre_act = jnp.dot(normed, w_in, preferred_element_type=jnp.float32).astype(jnp.bfloat16)
    act_f32, gelu_vjp = jax.vjp(jax.nn.gelu, pre_act.astype(jnp.float32))
    hidden = act_f32.astype(jnp.bfloat16)
    mlp_out = jnp.dot(hidden, w_out, preferred_element_type=jnp.float32)
    block_out = (embedded_f32 + mlp_out).astype(jnp.bfloat16)
    d_hidden = jnp.dot(d_out, w_out.T, preferred_element_type=jnp.float32).astype(jnp.bfloat16)
    d_w_out = jnp.dot(hidden.T, d_out, preferred_element_type=jnp.float32)
    (d_pre_f32,) = gelu_vjp(d_hidden.astype(jnp.float32))
    d_pre = d_pre_f32.astype(jnp.bfloat16)
    d_w_in = jnp.dot(normed.T, d_pre, preferred_element_type=jnp.float32)
    d_normed = jnp.dot(d_pre, w_in.T, preferred_element_type=jnp.float32)
    d_scaled = d_normed * gain_f32
    row_proj = jnp.mean(d_scaled * embedded_f32, axis=-1, keepdims=True)
    d_emb = (d_out.astype(jnp.float32) + inv_rms * (d_scaled - embedded_f32 * inv_rms * inv_rms * row_proj)).astype(jnp.bfloat16)
    d_table = jax.ops.segment_sum(d_emb.astype(jnp.float32), token_ids, num_segments=VOCAB_SIZE)
    return block_out, d_table, d_w_in, d_w_out
```

```python
import jax
import jax.numpy as jnp
from jax import lax
from jax.experimental import pallas as pl
from jax.experimental.pallas import tpu as pltpu
from jax.sharding import PartitionSpec as P

EPS = 1e-6
BF = jnp.bfloat16
F32 = jnp.float32
I32 = jnp.int32
GELU_C = 0.7978845608028654
GELU_A = 0.044715
VMEM = pltpu.VMEM
SMEM_SPEC = pl.BlockSpec(memory_space=pltpu.SMEM)
ANY_SPEC = pl.BlockSpec(memory_space=pl.ANY)
HBM_SPEC = pl.BlockSpec(memory_space=pltpu.HBM)
VMEM_SPEC = pl.BlockSpec(memory_space=VMEM)
DMA = pltpu.SemaphoreType.DMA
TILE = 256
ZERO_ROWS = 96
FILL_0, FILL_1, FILL_2 = 20, 52, 41
MIB = 1 << 20


def mm(a, b, ca, cb):
    return lax.dot_general(a, b, (((ca,), (cb,)), ((), ())), preferred_element_type=F32)


def sh(shape, dtype):
    return jax.ShapeDtypeStruct(shape, dtype)


def fill_copy(zero, table_g, sem, i):
    return pltpu.make_async_copy(zero, table_g.at[pl.ds(pl.multiple_of(i * ZERO_ROWS, ZERO_ROWS), ZERO_ROWS)], sem)


def fill_start(zero, table_g, sem, lo, hi):
    zero[...] = jnp.zeros_like(zero)

    def body(i, carry):
        fill_copy(zero, table_g, sem, i).start()
        return carry

    lax.fori_loop(lo, hi, body, 0)


def fill_wait(zero, table_g, sem, lo, hi):
    def body(i, carry):
        fill_copy(zero, table_g, sem, i).wait()
        return carry

    lax.fori_loop(lo, hi, body, 0)


def swap_with_sibling():
    sib = lax.axis_index("tp") ^ 1
    barrier = pltpu.get_barrier_semaphore()
    pl.semaphore_signal(barrier, inc=1, device_id={"tp": sib}, device_id_type=pl.DeviceIdType.MESH)
    pl.semaphore_wait(barrier, 1)

    def remote(src, dst, sems, i):
        return pltpu.make_async_remote_copy(
            src_ref=src, dst_ref=dst, send_sem=sems.at[0, i], recv_sem=sems.at[1, i],
            device_id={"tp": sib}, device_id_type=pl.DeviceIdType.MESH)

    return remote


def lookup_kernel(ids_s, ids_v, table, d_out, part, flags, same, d_own, table_g, slabs, zero, sems, s_zero, s_d):
    tokens, vocab = part.shape[0], table.shape[0]
    base = lax.axis_index("tp") * vocab
    group = 32
    groups = tokens // group

    def fetch(i, carry):
        lid = ids_s[i] - base
        owned = (lid >= 0) & (lid < vocab)
        slab = jnp.where(owned, lid >> 3, i)
        pltpu.make_async_copy(
            table.at[pl.ds(pl.multiple_of(slab << 3, 8), 8)],
            slabs.at[pl.ds(pl.multiple_of(i * 8, 8), 8)],
            sems.at[i // group],
        ).start()
        return carry

    lax.fori_loop(0, tokens, fetch, 0, unroll=8)
    load = pltpu.make_async_copy(d_out, d_own, s_d)
    load.start()
    fill_start(zero, table_g, s_zero, 0, FILL_0)
    row = jnp.broadcast_to(ids_v[...].astype(F32), (tokens, tokens))
    col = row.T
    equal = row == col
    same[...] = jnp.where(equal, 1.0, 0.0).astype(BF)
    earlier = lax.broadcasted_iota(I32, (tokens, tokens), 0) < lax.broadcasted_iota(I32, (tokens, tokens), 1)
    flags[...] = jnp.max(jnp.where(equal & earlier, 1, 0), axis=0, keepdims=True)
    ids_col = col.astype(I32) - base
    lane = lax.broadcasted_iota(I32, (group, group * 8), 1)
    first = lax.broadcasted_iota(I32, (group, group * 8), 0) * 8
    for k in range(groups):
        lid = ids_col[k * group:(k + 1) * group, :]
        owned = (lid >= 0) & (lid < vocab)
        pick = jnp.where(owned & (lane == first + (lid & 7)), 1.0, 0.0).astype(BF)
        rows = pl.ds(k * group * 8, group * 8)
        pltpu.make_async_copy(table.at[pl.ds(0, group * 8)], slabs.at[rows], sems.at[k]).wait()
        part[pl.ds(k * group, group), :] = mm(pick, slabs[rows, :], 1, 0).astype(BF)
    load.wait()
    fill_wait(zero, table_g, s_zero, 0, FILL_0)


def lookup(ids, table, d_out):
    tokens, (vocab, width) = ids.shape[0], table.shape
    return pl.pallas_call(
        lookup_kernel,
        name="lookup",
        out_shape=[sh((tokens, width), BF), sh((1, tokens), I32), sh((tokens, tokens), BF), sh(d_out.shape, BF), sh((vocab, width), F32)],
        in_specs=[SMEM_SPEC, VMEM_SPEC, HBM_SPEC, HBM_SPEC],
        out_specs=[VMEM_SPEC, VMEM_SPEC, VMEM_SPEC, VMEM_SPEC, HBM_SPEC],
        scratch_shapes=[VMEM((tokens * 8, width), BF), VMEM((ZERO_ROWS, width), F32), DMA((tokens // 32,)), DMA(()), DMA(())],
        compiler_params=pltpu.CompilerParams(vmem_limit_bytes=44 * MIB),
        cost_estimate=pl.CostEstimate(flops=5_000_000_000, bytes_accessed=10 * MIB, transcendentals=0),
    )(ids, ids.reshape(1, tokens), table, d_out)


def pair_kernel(part, d_own, d_far, comb, d_full, part_r, d_r, sems):
    me = lax.axis_index("tp")
    rows = d_own.shape[0]
    half = 2 * rows
    blocks = (me, me ^ 2, me ^ 1, me ^ 3)
    remote = swap_with_sibling()
    block = lambda k: pl.ds(pl.multiple_of(blocks[k] * rows, rows), rows)
    copies = [remote(part.at[block(2)], part_r.at[pl.ds(0, rows)], sems, 0),
              remote(part.at[block(3)], part_r.at[pl.ds(rows, rows)], sems, 1),
              remote(d_own, d_r.at[pl.ds(0, rows)], sems, 2),
              remote(d_far, d_r.at[pl.ds(rows, rows)], sems, 3)]
    for c in copies:
        c.start()
    d_full[pl.ds(0, rows), :] = d_own[...]
    d_full[pl.ds(rows, rows), :] = d_far[...]
    for k in range(2):
        copies[k].wait()
        at = pl.ds(k * rows, rows)
        comb[at, :] = part[block(k), :] + part_r[at, :]
    copies[2].wait()
    copies[3].wait()
    d_full[pl.ds(half, half), :] = d_r[...]


def pair(part, d_own, d_far):
    tokens, width = part.shape
    half = tokens // 2
    return pl.pallas_call(
        pair_kernel,
        name="pair",
        out_shape=[sh((half, width), BF), sh((tokens, width), BF)],
        in_specs=[VMEM_SPEC] * 3,
        out_specs=[VMEM_SPEC] * 2,
        scratch_shapes=[VMEM((half, width), BF), VMEM((half, width), BF), DMA((2, 4))],
        compiler_params=pltpu.CompilerParams(collective_id=0, has_side_effects=True, vmem_limit_bytes=8 * MIB),
        cost_estimate=pl.CostEstimate(flops=3_000_000_000, bytes_accessed=MIB, transcendentals=0),
    )(part, d_own, d_far)


def fill1_kernel(d_full, w2, table_in, dh, table_g, zero, s_zero):
    fill_start(zero, table_g, s_zero, FILL_0, FILL_0 + FILL_1)
    for j in range(dh.shape[1] // TILE):
        at = pl.ds(j * TILE, TILE)
        dh[:, at] = mm(d_full[...], w2[at, :], 1, 1).astype(BF)
    fill_wait(zero, table_g, s_zero, FILL_0, FILL_0 + FILL_1)


def fill1(d_full, w2, table_g):
    tokens, width = d_full.shape
    hid = w2.shape[0]
    return pl.pallas_call(
        fill1_kernel,
        name="fill1",
        out_shape=[sh((tokens, hid), BF), sh(table_g.shape, F32)],
        in_specs=[VMEM_SPEC, VMEM_SPEC, HBM_SPEC],
        out_specs=[VMEM_SPEC, HBM_SPEC],
        input_output_aliases={2: 1},
        scratch_shapes=[VMEM((ZERO_ROWS, width), F32), DMA(())],
        compiler_params=pltpu.CompilerParams(vmem_limit_bytes=12 * MIB),
        cost_estimate=pl.CostEstimate(flops=8_000_000_000, bytes_accessed=20 * MIB, transcendentals=0),
    )(d_full, w2, table_g)


def mlp_kernel(comb, e2, dh, w1, gain, n, h, du, x_own, dn_own, dn_far, x_f, dn_p, g1_r, sems):
    tokens, width = n.shape
    hid = h.shape[1]
    rows = x_own.shape[0]
    half = 2 * rows
    remote = swap_with_sibling()
    e3 = []
    for k in range(2):
        at, other = pl.ds(k * rows, rows), pl.ds((1 - k) * rows, rows)
        x_f[at, :] = comb[at, :] + e2[other, :]
        c = remote(x_f.at[at], x_f.at[pl.ds(half + k * rows, rows)], sems, k)
        c.start()
        e3.append(c)
    gain_f = gain[...].astype(F32).reshape(1, width)

    def norm_half(k):
        for j in range(4):
            at = pl.ds(k * half + j * 32, 32)
            x = x_f[at, :].astype(F32)
            r = lax.rsqrt(jnp.mean(x * x, axis=-1, keepdims=True) + EPS)
            n[at, :] = (x * r * gain_f).astype(BF)

    def fwd_half(k):
        at = pl.ds(k * half, half)
        for j in range(hid // TILE):
            cols = pl.ds(j * TILE, TILE)
            u = mm(n[at, :], w1[:, cols], 1, 0).astype(BF).astype(F32)
            t = jnp.tanh(GELU_C * (u + GELU_A * (u * u * u)))
            cdf = 0.5 * (1.0 + t)
            h[at, cols] = (u * cdf).astype(BF)
            g = dh[at, cols].astype(F32)
            du[at, cols] = (g * (cdf + u * (0.5 * (1.0 - t * t)) * (GELU_C * (1.0 + 3.0 * GELU_A * (u * u))))).astype(BF)

    def dn_half(k):
        at = pl.ds(k * half, half)
        for j in range(width // TILE):
            cols = pl.ds(j * TILE, TILE)
            dn_p[at, cols] = mm(du[at, :], w1[cols, :], 1, 1)

    norm_half(0)
    fwd_half(0)
    for c in e3:
        c.wait()
    norm_half(1)
    fwd_half(1)
    dn_half(1)
    g1 = [remote(dn_p.at[pl.ds(half + k * rows, rows)], g1_r.at[pl.ds(k * rows, rows)], sems, 2 + k) for k in range(2)]
    g1[1].start()
    g1[0].start()
    dn_half(0)
    x_own[...] = x_f[pl.ds(0, rows), :]
    g1[1].wait()
    dn_far[...] = dn_p[pl.ds(rows, rows), :] + g1_r[pl.ds(rows, rows), :]
    g1[0].wait()
    dn_own[...] = dn_p[pl.ds(0, rows), :] + g1_r[pl.ds(0, rows), :]


def mlp(comb, e2, dh, w1, gain):
    half, width = comb.shape
    tokens, rows = 2 * half, half // 2
    hid = w1.shape[1]
    return pl.pallas_call(
        mlp_kernel,
        name="mlp",
        out_shape=[sh((tokens, width), BF), sh((tokens, hid), BF), sh((tokens, hid), BF), sh((rows, width), BF),
                   sh((rows, width), F32), sh((rows, width), F32)],
        in_specs=[VMEM_SPEC] * 5,
        out_specs=[VMEM_SPEC] * 6,
        scratch_shapes=[VMEM((tokens, width), BF), VMEM((tokens, width), F32), VMEM((half, width), F32), DMA((2, 4))],
        compiler_params=pltpu.CompilerParams(collective_id=1, has_side_effects=True, vmem_limit_bytes=16 * MIB),
        cost_estimate=pl.CostEstimate(flops=6_000_000_000, bytes_accessed=4 * MIB, transcendentals=0),
    )(comb, e2, dh, w1, gain)


def grads_kernel(n, h, du, d_full, w2, table_in, y, dw1, dw2, table_g, zero, dw1_v, dw2_v, s_zero, s_w):
    lo, hi = FILL_0 + FILL_1, FILL_0 + FILL_1 + FILL_2
    fill_start(zero, table_g, s_zero, lo, hi)
    width, hid = dw1.shape
    for j in range(width // TILE):
        cols = pl.ds(j * TILE, TILE)
        y[:, cols] = mm(h[...], w2[:, cols], 1, 0)
    n_t = n[...].T
    for j in range(width // TILE):
        at = slice(j * TILE, (j + 1) * TILE)
        dw1_v[at, :] = mm(n_t[at, :], du[...], 1, 0)
        pltpu.make_async_copy(dw1_v.at[pl.ds(j * TILE, TILE)], dw1.at[pl.ds(j * TILE, TILE)], s_w).start()
    h_t = h[...].T
    for j in range(hid // TILE):
        at = slice(j * TILE, (j + 1) * TILE)
        dw2_v[at, :] = mm(h_t[at, :], d_full[...], 1, 0)
        pltpu.make_async_copy(dw2_v.at[pl.ds(j * TILE, TILE)], dw2.at[pl.ds(j * TILE, TILE)], s_w).start()
    pltpu.make_async_copy(dw1_v, dw1, s_w).wait()
    pltpu.make_async_copy(dw2_v, dw2, s_w).wait()
    fill_wait(zero, table_g, s_zero, lo, hi)


def grads(n, h, du, d_full, w2, table_g):
    tokens, width = n.shape
    hid = h.shape[1]
    return pl.pallas_call(
        grads_kernel,
        name="grads",
        out_shape=[sh((tokens, width), F32), sh((width, hid), F32), sh((hid, width), F32), sh(table_g.shape, F32)],
        in_specs=[VMEM_SPEC] * 5 + [HBM_SPEC],
        out_specs=[VMEM_SPEC, HBM_SPEC, HBM_SPEC, HBM_SPEC],
        input_output_aliases={5: 3},
        scratch_shapes=[VMEM((ZERO_ROWS, width), F32), VMEM((width, hid), F32), VMEM((hid, width), F32), DMA(()), DMA(())],
        compiler_params=pltpu.CompilerParams(vmem_limit_bytes=24 * MIB),
        cost_estimate=pl.CostEstimate(flops=8_000_000_000, bytes_accessed=20 * MIB, transcendentals=0),
    )(n, h, du, d_full, w2, table_g)


def ysum_kernel(y, order, y_own, y_far, y_r, sems):
    rows = y_own.shape[0]
    half = 2 * rows
    remote = swap_with_sibling()
    copies = [remote(y.at[pl.ds(half + k * rows, rows)], y_r.at[pl.ds(k * rows, rows)], sems, k) for k in range(2)]
    for c in copies:
        c.start()
    for k, out in enumerate((y_own, y_far)):
        copies[k].wait()
        at = pl.ds(k * rows, rows)
        out[...] = y[at, :] + y_r[at, :]


def ysum(y, order):
    tokens, width = y.shape
    rows = tokens // 4
    return pl.pallas_call(
        ysum_kernel,
        name="ysum",
        out_shape=[sh((rows, width), F32), sh((rows, width), F32)],
        in_specs=[VMEM_SPEC, ANY_SPEC],
        out_specs=[VMEM_SPEC] * 2,
        scratch_shapes=[VMEM((2 * rows, width), F32), DMA((2, 2))],
        compiler_params=pltpu.CompilerParams(collective_id=2, has_side_effects=True, vmem_limit_bytes=8 * MIB),
        cost_estimate=pl.CostEstimate(flops=3_000_000_000, bytes_accessed=4 * MIB, transcendentals=0),
    )(y, order)


def dx_kernel(dn_own, g2, x_own, d_own, gain, order, dx):
    gain_f = gain[...].astype(F32).reshape(1, dx.shape[1])
    for j in range(dx.shape[0] // 16):
        at = pl.ds(j * 16, 16)
        a = (dn_own[at, :] + g2[at, :]) * gain_f
        x = x_own[at, :].astype(F32)
        r = lax.rsqrt(jnp.mean(x * x, axis=-1, keepdims=True) + EPS)
        proj = jnp.mean(a * x, axis=-1, keepdims=True)
        dx[at, :] = (d_own[at, :].astype(F32) + r * (a - x * r * r * proj)).astype(BF)


def dx_rows(dn_own, g2, x_own, d_own, gain, order):
    return pl.pallas_call(
        dx_kernel,
        name="dx_rows",
        out_shape=sh(x_own.shape, BF),
        in_specs=[VMEM_SPEC] * 5 + [ANY_SPEC],
        out_specs=VMEM_SPEC,
        compiler_params=pltpu.CompilerParams(vmem_limit_bytes=4 * MIB),
        cost_estimate=pl.CostEstimate(flops=1_000_000_000, bytes_accessed=MIB, transcendentals=0),
    )(dn_own, g2, x_own, d_own, gain, order)


def fill3_kernel(order, table_in, token, table_g, zero, s_zero):
    lo, hi = FILL_0 + FILL_1 + FILL_2, table_g.shape[0] // ZERO_ROWS
    fill_start(zero, table_g, s_zero, lo, hi)
    token[...] = jnp.zeros_like(token)
    fill_wait(zero, table_g, s_zero, lo, hi)


def fill3(order, table_g):
    return pl.pallas_call(
        fill3_kernel,
        name="fill3",
        out_shape=[sh((8, 128), F32), sh(table_g.shape, F32)],
        in_specs=[ANY_SPEC, HBM_SPEC],
        out_specs=[VMEM_SPEC, HBM_SPEC],
        input_output_aliases={1: 1},
        scratch_shapes=[VMEM((ZERO_ROWS, table_g.shape[1]), F32), DMA(())],
        compiler_params=pltpu.CompilerParams(vmem_limit_bytes=4 * MIB),
        cost_estimate=pl.CostEstimate(flops=5_000_000_000, bytes_accessed=16 * MIB, transcendentals=0),
    )(order, table_g)


def dx_all_kernel(dx, dx_far, order, dx_out, dx_r, sems):
    me = lax.axis_index("tp")
    rows = dx.shape[0]
    remote = swap_with_sibling()
    block = lambda m: pl.ds(pl.multiple_of((me ^ m) * rows, rows), rows)
    copies = [remote(dx, dx_r.at[pl.ds(0, rows)], sems, 0), remote(dx_far, dx_r.at[pl.ds(rows, rows)], sems, 1)]
    for c in copies:
        c.start()
    dx_out[block(0), :] = dx[...]
    dx_out[block(2), :] = dx_far[...]
    copies[0].wait()
    dx_out[block(1), :] = dx_r[pl.ds(0, rows), :]
    copies[1].wait()
    dx_out[block(3), :] = dx_r[pl.ds(rows, rows), :]


def dx_all(dx, dx_far, order):
    rows, width = dx.shape
    return pl.pallas_call(
        dx_all_kernel,
        name="dx_all",
        out_shape=sh((4 * rows, width), BF),
        in_specs=[VMEM_SPEC, VMEM_SPEC, ANY_SPEC],
        out_specs=VMEM_SPEC,
        scratch_shapes=[VMEM((2 * rows, width), BF), DMA((2, 2))],
        compiler_params=pltpu.CompilerParams(collective_id=3, has_side_effects=True, vmem_limit_bytes=4 * MIB),
        cost_estimate=pl.CostEstimate(flops=2_000_000_000, bytes_accessed=MIB, transcendentals=0),
    )(dx, dx_far, order)


def put_kernel(ids_s, repeat_s, same, dx, table_in, table_g, token, total, s_row):
    tokens, vocab = dx.shape[0], table_g.shape[0]
    base = lax.axis_index("tp") * vocab
    total[...] = mm(same[...], dx[...], 1, 0)
    token[...] = jnp.zeros_like(token)

    def put(i, count):
        lid = ids_s[i] - base
        mine = (lid >= 0) & (lid < vocab) & (repeat_s[0, i] == 0)

        @pl.when(mine)
        def _():
            pltpu.make_async_copy(total.at[pl.ds(i, 1)], table_g.at[pl.ds(lid, 1)], s_row).start()

        return count + mine.astype(I32)

    count = lax.fori_loop(0, tokens, put, 0)

    def put_wait(i, carry):
        pltpu.make_async_copy(total.at[pl.ds(0, 1)], table_g.at[pl.ds(0, 1)], s_row).wait()
        return carry

    lax.fori_loop(0, count, put_wait, 0)


def put_rows(ids, repeat, same, dx, table_g):
    return pl.pallas_call(
        put_kernel,
        name="put_rows",
        out_shape=[sh(table_g.shape, F32), sh((8, 128), F32)],
        in_specs=[SMEM_SPEC, SMEM_SPEC, VMEM_SPEC, VMEM_SPEC, HBM_SPEC],
        out_specs=[HBM_SPEC, VMEM_SPEC],
        input_output_aliases={4: 0},
        scratch_shapes=[VMEM(dx.shape, F32), DMA(())],
        compiler_params=pltpu.CompilerParams(vmem_limit_bytes=4 * MIB),
        cost_estimate=pl.CostEstimate(flops=3_000_000_000, bytes_accessed=2 * MIB, transcendentals=0),
    )(ids, repeat, same, dx, table_g)


def finish_kernel(x, y, y_in, order, out):
    out[...] = (x[...].astype(F32) + (y[...] + y_in[...])).astype(BF)


def finish(x, y, y_in, order):
    return pl.pallas_call(
        finish_kernel,
        name="finish",
        out_shape=sh(x.shape, BF),
        in_specs=[VMEM_SPEC] * 3 + [ANY_SPEC],
        out_specs=VMEM_SPEC,
        compiler_params=pltpu.CompilerParams(vmem_limit_bytes=4 * MIB),
        cost_estimate=pl.CostEstimate(flops=1_000_000_000, bytes_accessed=MIB, transcendentals=0),
    )(x, y, y_in, order)


def solution(mesh):
    tp = mesh.shape["tp"]
    far_pairs = [(i, i ^ 2) for i in range(tp)]

    def shard_step(ids, table, gain, w1, w2, d_out):
        d_far = lax.ppermute(d_out, "tp", far_pairs)
        part, repeat, same, d_own, d_table = lookup(ids, table, d_out)
        comb, d_full = pair(part, d_own, d_far)
        e2 = lax.ppermute(comb, "tp", far_pairs)
        dh, d_table = fill1(d_full, w2, d_table)
        n, h, du, x_own, dn_own, dn_far = mlp(comb, e2, dh, w1, gain)
        g2 = lax.ppermute(dn_far, "tp", far_pairs)
        y, d_w1, d_w2, d_table = grads(n, h, du, d_full, w2, d_table)
        dx = dx_rows(dn_own, g2, x_own, d_own, gain, y)
        dx_far = lax.ppermute(dx, "tp", far_pairs)
        y_own, y_far = ysum(y, dx)
        token, d_table = fill3(y_own, d_table)
        y_in = lax.ppermute(y_far, "tp", far_pairs)
        dx_full = dx_all(dx, dx_far, token)
        d_table, done = put_rows(ids, repeat, same, dx_full, d_table)
        out = finish(x_own, y_own, y_in, done)
        return out, d_table, d_w1, d_w2

    return jax.shard_map(
        shard_step,
        mesh=mesh,
        in_specs=(P("dp"), P("tp", None), P(None), P(None, "tp"), P("tp", None), P(("dp", "tp"), None)),
        out_specs=(P(("dp", "tp"), None), P(("dp", "tp"), None), P("dp", "tp"), P(("dp", "tp"), None)),
        check_vma=False,
    )
```

```python
import jax
import jax.numpy as jnp
from jax import lax
from jax.experimental import pallas as pl
from jax.experimental.pallas import tpu as pltpu
from jax.sharding import PartitionSpec as P

EPS = 1e-6
BF = jnp.bfloat16
F32 = jnp.float32
I32 = jnp.int32
GELU_C = 0.7978845608028654
GELU_A = 0.044715
VMEM = pltpu.VMEM
SMEM_SPEC = pl.BlockSpec(memory_space=pltpu.SMEM)
ANY_SPEC = pl.BlockSpec(memory_space=pl.ANY)
HBM_SPEC = pl.BlockSpec(memory_space=pltpu.HBM)
VMEM_SPEC = pl.BlockSpec(memory_space=VMEM)
DMA = pltpu.SemaphoreType.DMA
TILE = 256
ZERO_ROWS = 96
FILL_0, FILL_1, FILL_2 = 25, 60, 36
MIB = 1 << 20
LOOKUP_VMEM = 48 * MIB


def mm(a, b, ca, cb):
    return lax.dot_general(a, b, (((ca,), (cb,)), ((), ())), preferred_element_type=F32)


def sh(shape, dtype):
    return jax.ShapeDtypeStruct(shape, dtype)


def fill_copy(zero, table_g, sem, i):
    return pltpu.make_async_copy(zero, table_g.at[pl.ds(pl.multiple_of(i * ZERO_ROWS, ZERO_ROWS), ZERO_ROWS)], sem)


def fill_start(zero, table_g, sem, lo, hi):
    zero[...] = jnp.zeros_like(zero)

    def body(i, carry):
        fill_copy(zero, table_g, sem, i).start()
        return carry

    lax.fori_loop(lo, hi, body, 0)


def fill_wait(zero, table_g, sem, lo, hi):
    def body(i, carry):
        fill_copy(zero, table_g, sem, i).wait()
        return carry

    lax.fori_loop(lo, hi, body, 0)


def swap_with_sibling():
    sib = lax.axis_index("tp") ^ 1
    barrier = pltpu.get_barrier_semaphore()
    pl.semaphore_signal(barrier, inc=1, device_id={"tp": sib}, device_id_type=pl.DeviceIdType.MESH)
    pl.semaphore_wait(barrier, 1)

    def remote(src, dst, sems, i):
        return pltpu.make_async_remote_copy(
            src_ref=src, dst_ref=dst, send_sem=sems.at[0, i], recv_sem=sems.at[1, i],
            device_id={"tp": sib}, device_id_type=pl.DeviceIdType.MESH)

    return remote


def lookup_kernel(ids_s, ids_v, table, w1, w2, part, flags, same, w1_v, w2_v, table_g, slabs, zero, sems, s_zero, s_in):
    tokens, vocab = part.shape[0], table.shape[0]
    base = lax.axis_index("tp") * vocab
    group = 32
    groups = tokens // group

    def fetch(i, carry):
        lid = ids_s[i] - base
        owned = (lid >= 0) & (lid < vocab)
        slab = jnp.where(owned, lid >> 3, i)
        pltpu.make_async_copy(
            table.at[pl.ds(pl.multiple_of(slab << 3, 8), 8)],
            slabs.at[pl.ds(pl.multiple_of(i * 8, 8), 8)],
            sems.at[i // group],
        ).start()
        return carry

    fill_start(zero, table_g, s_zero, 0, FILL_0)
    lax.fori_loop(0, tokens, fetch, 0, unroll=8)
    loads = [pltpu.make_async_copy(a, b, s_in.at[k]) for k, (a, b) in enumerate(((w2, w2_v), (w1, w1_v)))]
    for c in loads:
        c.start()
    row = jnp.broadcast_to(ids_v[...].astype(F32), (tokens, tokens))
    col = row.T
    equal = row == col
    same[...] = jnp.where(equal, 1.0, 0.0).astype(BF)
    earlier = lax.broadcasted_iota(I32, (tokens, tokens), 0) < lax.broadcasted_iota(I32, (tokens, tokens), 1)
    flags[...] = jnp.max(jnp.where(equal & earlier, 1, 0), axis=0, keepdims=True)
    ids_col = col.astype(I32) - base
    lane = lax.broadcasted_iota(I32, (group, group * 8), 1)
    first = lax.broadcasted_iota(I32, (group, group * 8), 0) * 8
    for k in range(groups):
        lid = ids_col[k * group:(k + 1) * group, :]
        owned = (lid >= 0) & (lid < vocab)
        pick = jnp.where(owned & (lane == first + (lid & 7)), 1.0, 0.0).astype(BF)
        rows = pl.ds(k * group * 8, group * 8)
        pltpu.make_async_copy(table.at[pl.ds(0, group * 8)], slabs.at[rows], sems.at[k]).wait()
        part[pl.ds(k * group, group), :] = mm(pick, slabs[rows, :], 1, 0).astype(BF)
    for c in loads:
        c.wait()
    fill_wait(zero, table_g, s_zero, 0, FILL_0)


def lookup(ids, table, w1, w2):
    tokens, (vocab, width) = ids.shape[0], table.shape
    return pl.pallas_call(
        lookup_kernel,
        name="lookup",
        out_shape=[sh((tokens, width), BF), sh((1, tokens), I32), sh((tokens, tokens), BF),
                   sh(w1.shape, BF), sh(w2.shape, BF), sh((vocab, width), F32)],
        in_specs=[SMEM_SPEC, VMEM_SPEC] + [HBM_SPEC] * 3,
        out_specs=[VMEM_SPEC] * 5 + [HBM_SPEC],
        scratch_shapes=[VMEM((tokens * 8, width), BF), VMEM((ZERO_ROWS, width), F32), DMA((tokens // 32,)), DMA(()), DMA((2,))],
        compiler_params=pltpu.CompilerParams(vmem_limit_bytes=LOOKUP_VMEM),
        cost_estimate=pl.CostEstimate(flops=5_000_000_000, bytes_accessed=10 * MIB, transcendentals=0),
    )(ids, ids.reshape(1, tokens), table, w1, w2)


def pair_kernel(part, comb, part_r, sems):
    me = lax.axis_index("tp")
    rows = part.shape[0] // 4
    blocks = (me, me ^ 2, me ^ 1, me ^ 3)
    remote = swap_with_sibling()
    block = lambda k: pl.ds(pl.multiple_of(blocks[k] * rows, rows), rows)
    copies = [remote(part.at[block(2 + k)], part_r.at[pl.ds(k * rows, rows)], sems, k) for k in range(2)]
    for c in copies:
        c.start()
    for k in range(2):
        copies[k].wait()
        at = pl.ds(k * rows, rows)
        comb[at, :] = part[block(k), :] + part_r[at, :]


def pair(part):
    tokens, width = part.shape
    half = tokens // 2
    return pl.pallas_call(
        pair_kernel,
        name="pair",
        out_shape=sh((half, width), BF),
        in_specs=[VMEM_SPEC],
        out_specs=VMEM_SPEC,
        scratch_shapes=[VMEM((half, width), BF), DMA((2, 2))],
        compiler_params=pltpu.CompilerParams(collective_id=0, has_side_effects=True, vmem_limit_bytes=8 * MIB),
        cost_estimate=pl.CostEstimate(flops=3_000_000_000, bytes_accessed=MIB, transcendentals=0),
    )(part)


def fill1_kernel(ids_s, repeat_s, order, table_in, puts, token, table_g, zero, s_zero):
    fill_start(zero, table_g, s_zero, FILL_0, FILL_0 + FILL_1)
    tokens, vocab = puts.shape[0] // 2, table_g.shape[0]
    base = lax.axis_index("tp") * vocab

    def body(i, count):
        lid = ids_s[i] - base
        mine = (lid >= 0) & (lid < vocab) & (repeat_s[0, i] == 0)
        slot = jnp.where(mine, count, tokens - 1 - (i - count))
        puts[slot] = i
        puts[tokens + slot] = jnp.where(mine, lid, -1)
        return count + mine.astype(I32)

    lax.fori_loop(0, tokens, body, 0, unroll=4)
    token[...] = jnp.zeros_like(token)
    fill_wait(zero, table_g, s_zero, FILL_0, FILL_0 + FILL_1)


def fill1(ids, repeat, order, table_g):
    return pl.pallas_call(
        fill1_kernel,
        name="fill1",
        out_shape=[sh((2 * ids.shape[0],), I32), sh((8, 128), F32), sh(table_g.shape, F32)],
        in_specs=[SMEM_SPEC, SMEM_SPEC, ANY_SPEC, HBM_SPEC],
        out_specs=[SMEM_SPEC, VMEM_SPEC, HBM_SPEC],
        input_output_aliases={3: 2},
        scratch_shapes=[VMEM((ZERO_ROWS, table_g.shape[1]), F32), DMA(())],
        compiler_params=pltpu.CompilerParams(vmem_limit_bytes=12 * MIB),
        cost_estimate=pl.CostEstimate(flops=8_000_000_000, bytes_accessed=20 * MIB, transcendentals=0),
    )(ids, repeat, order, table_g)


def mlp_kernel(comb, e2, d_own, d_far, w1, w2, gain, order, n, h, du, d_full, x_own, dn_own, dn_far, x_f, d_r, dn_p, g1_r, sems):
    tokens, width = n.shape
    hid = h.shape[1]
    rows = x_own.shape[0]
    half = 2 * rows
    remote = swap_with_sibling()
    e3 = []
    for k in range(2):
        at, other = pl.ds(k * rows, rows), pl.ds((1 - k) * rows, rows)
        x_f[at, :] = comb[at, :] + e2[other, :]
        c = remote(x_f.at[at], x_f.at[pl.ds(half + k * rows, rows)], sems, k)
        c.start()
        e3.append(c)
    ds = [remote(src, d_r.at[pl.ds(k * rows, rows)], sems, 4 + k) for k, src in enumerate((d_own, d_far))]
    for c in ds:
        c.start()
    d_full[pl.ds(0, rows), :] = d_own[...]
    d_full[pl.ds(rows, rows), :] = d_far[...]
    gain_f = gain[...].astype(F32).reshape(1, width)

    def norm_half(k):
        for j in range(4):
            at = pl.ds(k * half + j * 32, 32)
            x = x_f[at, :].astype(F32)
            r = lax.rsqrt(jnp.mean(x * x, axis=-1, keepdims=True) + EPS)
            n[at, :] = (x * r * gain_f).astype(BF)

    def fwd_half(k):
        at = pl.ds(k * half, half)
        for j in range(hid // TILE):
            cols = pl.ds(j * TILE, TILE)
            g = mm(d_full[at, :], w2[cols, :], 1, 1).astype(BF).astype(F32)
            u = mm(n[at, :], w1[:, cols], 1, 0).astype(BF).astype(F32)
            t = jnp.tanh(GELU_C * (u + GELU_A * (u * u * u)))
            cdf = 0.5 * (1.0 + t)
            h[at, cols] = (u * cdf).astype(BF)
            du[at, cols] = (g * (cdf + u * (0.5 * (1.0 - t * t)) * (GELU_C * (1.0 + 3.0 * GELU_A * (u * u))))).astype(BF)

    def dn_half(k):
        at = pl.ds(k * half, half)
        for j in range(width // TILE):
            cols = pl.ds(j * TILE, TILE)
            dn_p[at, cols] = mm(du[at, :], w1[cols, :], 1, 1)

    norm_half(0)
    fwd_half(0)
    for c in e3 + ds:
        c.wait()
    d_full[pl.ds(half, half), :] = d_r[...]
    norm_half(1)
    fwd_half(1)
    dn_half(1)
    g1 = [remote(dn_p.at[pl.ds(half + k * rows, rows)], g1_r.at[pl.ds(k * rows, rows)], sems, 2 + k) for k in range(2)]
    g1[1].start()
    g1[0].start()
    dn_half(0)
    x_own[...] = x_f[pl.ds(0, rows), :]
    g1[1].wait()
    dn_far[...] = dn_p[pl.ds(rows, rows), :] + g1_r[pl.ds(rows, rows), :]
    g1[0].wait()
    dn_own[...] = dn_p[pl.ds(0, rows), :] + g1_r[pl.ds(0, rows), :]


def mlp(comb, e2, d_own, d_far, w1, w2, gain, order):
    half, width = comb.shape
    tokens, rows = 2 * half, half // 2
    hid = w1.shape[1]
    return pl.pallas_call(
        mlp_kernel,
        name="mlp",
        out_shape=[sh((tokens, width), BF), sh((tokens, hid), BF), sh((tokens, hid), BF), sh((tokens, width), BF), sh((rows, width), BF),
                   sh((rows, width), F32), sh((rows, width), F32)],
        in_specs=[VMEM_SPEC] * 7 + [ANY_SPEC],
        out_specs=[VMEM_SPEC] * 7,
        scratch_shapes=[VMEM((tokens, width), BF), VMEM((half, width), BF), VMEM((tokens, width), F32), VMEM((half, width), F32), DMA((2, 6))],
        compiler_params=pltpu.CompilerParams(collective_id=1, has_side_effects=True, vmem_limit_bytes=16 * MIB),
        cost_estimate=pl.CostEstimate(flops=6_000_000_000, bytes_accessed=4 * MIB, transcendentals=0),
    )(comb, e2, d_own, d_far, w1, w2, gain, order)


def grads_kernel(n, h, du, d_full, w2, table_in, y, dw1, dw2, table_g, zero, dw1_v, dw2_v, s_zero, s_w):
    lo, hi = FILL_0 + FILL_1, FILL_0 + FILL_1 + FILL_2
    fill_start(zero, table_g, s_zero, lo, hi)
    width, hid = dw1.shape
    for j in range(width // TILE):
        cols = pl.ds(j * TILE, TILE)
        y[:, cols] = mm(h[...], w2[:, cols], 1, 0)
    n_t = n[...].T
    for j in range(width // TILE):
        at = slice(j * TILE, (j + 1) * TILE)
        dw1_v[at, :] = mm(n_t[at, :], du[...], 1, 0)
        pltpu.make_async_copy(dw1_v.at[pl.ds(j * TILE, TILE)], dw1.at[pl.ds(j * TILE, TILE)], s_w).start()
    h_t = h[...].T
    for j in range(hid // TILE):
        at = slice(j * TILE, (j + 1) * TILE)
        dw2_v[at, :] = mm(h_t[at, :], d_full[...], 1, 0)
        pltpu.make_async_copy(dw2_v.at[pl.ds(j * TILE, TILE)], dw2.at[pl.ds(j * TILE, TILE)], s_w).start()
    pltpu.make_async_copy(dw1_v, dw1, s_w).wait()
    pltpu.make_async_copy(dw2_v, dw2, s_w).wait()
    fill_wait(zero, table_g, s_zero, lo, hi)


def grads(n, h, du, d_full, w2, table_g):
    tokens, width = n.shape
    hid = h.shape[1]
    return pl.pallas_call(
        grads_kernel,
        name="grads",
        out_shape=[sh((tokens, width), F32), sh((width, hid), F32), sh((hid, width), F32), sh(table_g.shape, F32)],
        in_specs=[VMEM_SPEC] * 5 + [HBM_SPEC],
        out_specs=[VMEM_SPEC, HBM_SPEC, HBM_SPEC, HBM_SPEC],
        input_output_aliases={5: 3},
        scratch_shapes=[VMEM((ZERO_ROWS, width), F32), VMEM((width, hid), F32), VMEM((hid, width), F32), DMA(()), DMA(())],
        compiler_params=pltpu.CompilerParams(vmem_limit_bytes=24 * MIB),
        cost_estimate=pl.CostEstimate(flops=8_000_000_000, bytes_accessed=20 * MIB, transcendentals=0),
    )(n, h, du, d_full, w2, table_g)


def ysum_kernel(y, dx, y_own, y_far, dx_sib, y_r, dx_r, sems):
    rows = y_own.shape[0]
    half = 2 * rows
    remote = swap_with_sibling()
    copies = [remote(y.at[pl.ds(half + k * rows, rows)], y_r.at[pl.ds(k * rows, rows)], sems, k) for k in (1, 0)]
    copies.append(remote(dx, dx_r, sems, 2))
    for c in copies:
        c.start()
    for c, k, out in zip(copies, (1, 0), (y_far, y_own)):
        c.wait()
        at = pl.ds(k * rows, rows)
        out[...] = y[at, :] + y_r[at, :]
    copies[2].wait()
    dx_sib[...] = dx_r[...]


def ysum(y, dx):
    tokens, width = y.shape
    rows = tokens // 4
    return pl.pallas_call(
        ysum_kernel,
        name="ysum",
        out_shape=[sh((rows, width), F32), sh((rows, width), F32), sh((rows, width), BF)],
        in_specs=[VMEM_SPEC, VMEM_SPEC],
        out_specs=[VMEM_SPEC] * 3,
        scratch_shapes=[VMEM((2 * rows, width), F32), VMEM((rows, width), BF), DMA((2, 3))],
        compiler_params=pltpu.CompilerParams(collective_id=2, has_side_effects=True, vmem_limit_bytes=8 * MIB),
        cost_estimate=pl.CostEstimate(flops=3_000_000_000, bytes_accessed=4 * MIB, transcendentals=0),
    )(y, dx)


def dx_kernel(dn_own, g2, x_own, d_own, gain, order, dx):
    gain_f = gain[...].astype(F32).reshape(1, dx.shape[1])
    for j in range(dx.shape[0] // 16):
        at = pl.ds(j * 16, 16)
        a = (dn_own[at, :] + g2[at, :]) * gain_f
        x = x_own[at, :].astype(F32)
        r = lax.rsqrt(jnp.mean(x * x, axis=-1, keepdims=True) + EPS)
        proj = jnp.mean(a * x, axis=-1, keepdims=True)
        dx[at, :] = (d_own[at, :].astype(F32) + r * (a - x * r * r * proj)).astype(BF)


def dx_rows(dn_own, g2, x_own, d_own, gain, order):
    return pl.pallas_call(
        dx_kernel,
        name="dx_rows",
        out_shape=sh(x_own.shape, BF),
        in_specs=[VMEM_SPEC] * 5 + [ANY_SPEC],
        out_specs=VMEM_SPEC,
        compiler_params=pltpu.CompilerParams(vmem_limit_bytes=4 * MIB),
        cost_estimate=pl.CostEstimate(flops=1_000_000_000, bytes_accessed=MIB, transcendentals=0),
    )(dn_own, g2, x_own, d_own, gain, order)


def fill3_kernel(order, table_in, token, table_g, zero, s_zero):
    lo, hi = FILL_0 + FILL_1 + FILL_2, table_g.shape[0] // ZERO_ROWS
    fill_start(zero, table_g, s_zero, lo, hi)
    token[...] = jnp.zeros_like(token)
    fill_wait(zero, table_g, s_zero, lo, hi)


def fill3(order, table_g):
    return pl.pallas_call(
        fill3_kernel,
        name="fill3",
        out_shape=[sh((8, 128), F32), sh(table_g.shape, F32)],
        in_specs=[ANY_SPEC, HBM_SPEC],
        out_specs=[VMEM_SPEC, HBM_SPEC],
        input_output_aliases={1: 1},
        scratch_shapes=[VMEM((ZERO_ROWS, table_g.shape[1]), F32), DMA(())],
        compiler_params=pltpu.CompilerParams(vmem_limit_bytes=4 * MIB),
        cost_estimate=pl.CostEstimate(flops=5_000_000_000, bytes_accessed=16 * MIB, transcendentals=0),
    )(order, table_g)


def dx_all_kernel(dx, dx_sib, dx_far, order, dx_out, dx_r, sems):
    me = lax.axis_index("tp")
    rows = dx.shape[0]
    remote = swap_with_sibling()
    block = lambda m: pl.ds(pl.multiple_of((me ^ m) * rows, rows), rows)
    copy = remote(dx_far, dx_r, sems, 0)
    copy.start()
    dx_out[block(0), :] = dx[...]
    dx_out[block(1), :] = dx_sib[...]
    dx_out[block(2), :] = dx_far[...]
    copy.wait()
    dx_out[block(3), :] = dx_r[...]


def dx_all(dx, dx_sib, dx_far, order):
    rows, width = dx.shape
    return pl.pallas_call(
        dx_all_kernel,
        name="dx_all",
        out_shape=sh((4 * rows, width), BF),
        in_specs=[VMEM_SPEC] * 3 + [ANY_SPEC],
        out_specs=VMEM_SPEC,
        scratch_shapes=[VMEM((rows, width), BF), DMA((2, 1))],
        compiler_params=pltpu.CompilerParams(collective_id=3, has_side_effects=True, vmem_limit_bytes=4 * MIB),
        cost_estimate=pl.CostEstimate(flops=2_000_000_000, bytes_accessed=MIB, transcendentals=0),
    )(dx, dx_sib, dx_far, order)


def put_kernel(puts, same, dx, table_in, table_g, token, puts_s, total, s_in, s_row):
    tokens = dx.shape[0]
    load = pltpu.make_async_copy(puts, puts_s, s_in)
    load.start()
    total[...] = mm(same[...], dx[...], 1, 0)
    token[...] = jnp.zeros_like(token)
    load.wait()

    def put(i):
        pltpu.make_async_copy(total.at[pl.ds(puts_s[i], 1)], table_g.at[pl.ds(puts_s[tokens + i], 1)], s_row).start()
        return i + 1

    count = lax.while_loop(lambda i: (i < tokens) & (puts_s[tokens + jnp.minimum(i, tokens - 1)] >= 0), put, 0)

    def put_wait(i, carry):
        pltpu.make_async_copy(total.at[pl.ds(0, 1)], table_g.at[pl.ds(0, 1)], s_row).wait()
        return carry

    lax.fori_loop(0, count, put_wait, 0)


def put_rows(puts, same, dx, table_g):
    return pl.pallas_call(
        put_kernel,
        name="put_rows",
        out_shape=[sh(table_g.shape, F32), sh((8, 128), F32)],
        in_specs=[ANY_SPEC, VMEM_SPEC, VMEM_SPEC, HBM_SPEC],
        out_specs=[HBM_SPEC, VMEM_SPEC],
        input_output_aliases={3: 0},
        scratch_shapes=[pltpu.SMEM(puts.shape, I32), VMEM(dx.shape, F32), DMA(()), DMA(())],
        compiler_params=pltpu.CompilerParams(vmem_limit_bytes=4 * MIB),
        cost_estimate=pl.CostEstimate(flops=3_000_000_000, bytes_accessed=2 * MIB, transcendentals=0),
    )(puts, same, dx, table_g)


def finish_kernel(x, y, y_in, order, out):
    out[...] = (x[...].astype(F32) + (y[...] + y_in[...])).astype(BF)


def finish(x, y, y_in, order):
    return pl.pallas_call(
        finish_kernel,
        name="finish",
        out_shape=sh(x.shape, BF),
        in_specs=[VMEM_SPEC] * 3 + [ANY_SPEC],
        out_specs=VMEM_SPEC,
        compiler_params=pltpu.CompilerParams(vmem_limit_bytes=4 * MIB),
        cost_estimate=pl.CostEstimate(flops=1_000_000_000, bytes_accessed=MIB, transcendentals=0),
    )(x, y, y_in, order)


def solution(mesh):
    tp = mesh.shape["tp"]
    far_pairs = [(i, i ^ 2) for i in range(tp)]

    def shard_step(ids, table, gain, w1, w2, d_out):
        part, repeat, same, w1_v, w2_v, d_table = lookup(ids, table, w1, w2)
        part, d_send = lax.optimization_barrier((part, d_out))
        d_far = lax.ppermute(d_send, "tp", far_pairs)
        comb = pair(part)
        e2 = lax.ppermute(comb, "tp", far_pairs)
        puts, token, d_table = fill1(ids, repeat, comb, d_table)
        n, h, du, d_full, x_own, dn_own, dn_far = mlp(comb, e2, d_out, d_far, w1_v, w2_v, gain, token)
        g2 = lax.ppermute(dn_far, "tp", far_pairs)
        y, d_w1, d_w2, d_table = grads(n, h, du, d_full, w2_v, d_table)
        dx = dx_rows(dn_own, g2, x_own, d_out, gain, y)
        dx_far = lax.ppermute(dx, "tp", far_pairs)
        y_own, y_far, dx_sib = ysum(y, dx)
        token, d_table = fill3(y_own, d_table)
        y_in = lax.ppermute(y_far, "tp", far_pairs)
        dx_full = dx_all(dx, dx_sib, dx_far, token)
        d_table, done = put_rows(puts, same, dx_full, d_table)
        out = finish(x_own, y_own, y_in, done)
        return out, d_table, d_w1, d_w2

    return jax.shard_map(
        shard_step,
        mesh=mesh,
        in_specs=(P("dp"), P("tp", None), P(None), P(None, "tp"), P("tp", None), P(("dp", "tp"), None)),
        out_specs=(P(("dp", "tp"), None), P(("dp", "tp"), None), P("dp", "tp"), P(("dp", "tp"), None)),
        check_vma=False,
    )
```

```python
import jax
import jax.numpy as jnp
from jax import lax
from jax.experimental import pallas as pl
from jax.experimental.pallas import tpu as pltpu
from jax.sharding import PartitionSpec as P

EPS = 1e-6
BF = jnp.bfloat16
F32 = jnp.float32
I32 = jnp.int32
GELU_C = 0.7978845608028654
GELU_A = 0.044715
VMEM = pltpu.VMEM
SMEM_SPEC = pl.BlockSpec(memory_space=pltpu.SMEM)
ANY_SPEC = pl.BlockSpec(memory_space=pl.ANY)
HBM_SPEC = pl.BlockSpec(memory_space=pltpu.HBM)
VMEM_SPEC = pl.BlockSpec(memory_space=VMEM)
DMA = pltpu.SemaphoreType.DMA
TILE = 256
ZERO_ROWS = 96
FILL_0, FILL_1, FILL_2 = 15, 62, 20
MIB = 1 << 20
LOOKUP_VMEM = 48 * MIB


def mm(a, b, ca, cb):
    return lax.dot_general(a, b, (((ca,), (cb,)), ((), ())), preferred_element_type=F32)


def sh(shape, dtype):
    return jax.ShapeDtypeStruct(shape, dtype)


def fill_copy(zero, table_g, sem, i):
    return pltpu.make_async_copy(zero, table_g.at[pl.ds(pl.multiple_of(i * ZERO_ROWS, ZERO_ROWS), ZERO_ROWS)], sem)


def fill_start(zero, table_g, sem, lo, hi):
    zero[...] = jnp.zeros_like(zero)

    def body(i, carry):
        fill_copy(zero, table_g, sem, i).start()
        return carry

    lax.fori_loop(lo, hi, body, 0)


def fill_wait(zero, table_g, sem, lo, hi):
    def body(i, carry):
        fill_copy(zero, table_g, sem, i).wait()
        return carry

    lax.fori_loop(lo, hi, body, 0)


def swap_with_sibling():
    sib = lax.axis_index("tp") ^ 1
    barrier = pltpu.get_barrier_semaphore()
    pl.semaphore_signal(barrier, inc=1, device_id={"tp": sib}, device_id_type=pl.DeviceIdType.MESH)
    pl.semaphore_wait(barrier, 1)

    def remote(src, dst, sems, i):
        return pltpu.make_async_remote_copy(
            src_ref=src, dst_ref=dst, send_sem=sems.at[0, i], recv_sem=sems.at[1, i],
            device_id={"tp": sib}, device_id_type=pl.DeviceIdType.MESH)

    return remote


def lookup_kernel(ids_s, ids_v, table, part, rows_mine, same, table_g, pairs, zero, sems, s_zero):
    tokens, vocab = part.shape[0], table.shape[0]
    base = lax.axis_index("tp") * vocab
    group = 64
    groups = tokens // group
    fill_start(zero, table_g, s_zero, 0, FILL_0)
    for k in range(groups):
        def fetch(i, carry):
            lid = ids_s[k * group + i] - base
            owned = (lid >= 0) & (lid < vocab)
            pair_id = jnp.where(owned, lid >> 1, i)
            pltpu.make_async_copy(
                table.at[pl.ds(pl.multiple_of(pair_id << 1, 2), 2)],
                pairs.at[pl.ds(pl.multiple_of(k * group * 2 + i * 2, 2), 2)],
                sems.at[k],
            ).start()
            return carry

        lax.fori_loop(0, group, fetch, 0, unroll=8)
    row = jnp.broadcast_to(ids_v[...].astype(F32), (tokens, tokens))
    col = row.T
    equal = row == col
    same[...] = jnp.where(equal, 1.0, 0.0).astype(BF)
    earlier = lax.broadcasted_iota(I32, (tokens, tokens), 0) < lax.broadcasted_iota(I32, (tokens, tokens), 1)
    repeat = jnp.max(jnp.where(equal & earlier, 1, 0), axis=0, keepdims=True)
    mine = ids_v[...] - base
    rows_mine[...] = jnp.where((mine >= 0) & (mine < vocab) & (repeat == 0), mine, -1)
    lid = col.astype(I32) - base
    lane = lax.broadcasted_iota(I32, (group, 2 * group), 1)
    first = lax.broadcasted_iota(I32, (group, 2 * group), 0) * 2
    for k in range(groups):
        at = lid[k * group:(k + 1) * group, :2 * group]
        owned = (at >= 0) & (at < vocab)
        pick = jnp.where(owned & (lane == first + (at & 1)), 1.0, 0.0).astype(BF)
        rows = pl.ds(k * group * 2, group * 2)
        pltpu.make_async_copy(table.at[pl.ds(0, group * 2)], pairs.at[rows], sems.at[k]).wait()
        part[pl.ds(k * group, group), :] = mm(pick, pairs[rows, :], 1, 0).astype(BF)
    fill_wait(zero, table_g, s_zero, 0, FILL_0)


def lookup(ids, table):
    tokens, (vocab, width) = ids.shape[0], table.shape
    return pl.pallas_call(
        lookup_kernel,
        name="lookup",
        out_shape=[sh((tokens, width), BF), sh((1, tokens), I32), sh((tokens, tokens), BF), sh((vocab, width), F32)],
        in_specs=[SMEM_SPEC, VMEM_SPEC, HBM_SPEC],
        out_specs=[VMEM_SPEC] * 3 + [HBM_SPEC],
        scratch_shapes=[VMEM((tokens * 2, width), BF), VMEM((ZERO_ROWS, width), F32), DMA((4,)), DMA(())],
        compiler_params=pltpu.CompilerParams(vmem_limit_bytes=LOOKUP_VMEM),
        cost_estimate=pl.CostEstimate(flops=5_000_000_000, bytes_accessed=10 * MIB, transcendentals=0),
    )(ids, ids.reshape(1, tokens), table)


def pair_kernel(part, comb, part_r, sems):
    me = lax.axis_index("tp")
    rows = part.shape[0] // 4
    blocks = (me, me ^ 2, me ^ 1, me ^ 3)
    remote = swap_with_sibling()
    block = lambda k: pl.ds(pl.multiple_of(blocks[k] * rows, rows), rows)
    copies = [remote(part.at[block(2 + k)], part_r.at[pl.ds(k * rows, rows)], sems, k) for k in range(2)]
    for c in copies:
        c.start()
    for k in range(2):
        copies[k].wait()
        at = pl.ds(k * rows, rows)
        comb[at, :] = part[block(k), :] + part_r[at, :]


def pair(part):
    tokens, width = part.shape
    half = tokens // 2
    return pl.pallas_call(
        pair_kernel,
        name="pair",
        out_shape=sh((half, width), BF),
        in_specs=[VMEM_SPEC],
        out_specs=VMEM_SPEC,
        scratch_shapes=[VMEM((half, width), BF), DMA((2, 2))],
        compiler_params=pltpu.CompilerParams(collective_id=0, has_side_effects=True, vmem_limit_bytes=8 * MIB),
        cost_estimate=pl.CostEstimate(flops=3_000_000_000, bytes_accessed=MIB, transcendentals=0),
    )(part)


def fill1_kernel(rows_mine, order, table_in, puts, token, table_g, zero, s_zero):
    fill_start(zero, table_g, s_zero, FILL_0, FILL_0 + FILL_1)
    tokens = rows_mine.shape[1]

    def body(i, count):
        lid = rows_mine[0, i]
        puts[count] = lid | (i << 16)
        return count + (lid >= 0).astype(I32)

    puts[tokens] = lax.fori_loop(0, tokens, body, 0, unroll=8)
    token[...] = jnp.zeros_like(token)
    fill_wait(zero, table_g, s_zero, FILL_0, FILL_0 + FILL_1)


def fill1(rows_mine, order, table_g):
    return pl.pallas_call(
        fill1_kernel,
        name="fill1",
        out_shape=[sh((2 * rows_mine.shape[1],), I32), sh((8, 128), F32), sh(table_g.shape, F32)],
        in_specs=[SMEM_SPEC, ANY_SPEC, HBM_SPEC],
        out_specs=[SMEM_SPEC, VMEM_SPEC, HBM_SPEC],
        input_output_aliases={2: 2},
        scratch_shapes=[VMEM((ZERO_ROWS, table_g.shape[1]), F32), DMA(())],
        compiler_params=pltpu.CompilerParams(vmem_limit_bytes=12 * MIB),
        cost_estimate=pl.CostEstimate(flops=8_000_000_000, bytes_accessed=20 * MIB, transcendentals=0),
    )(rows_mine, order, table_g)


def mlp_kernel(comb, e2, d_own, d_far, w1, w2, gain, order, n, h, du, d_full, x_own, dn_own, dn_far, x_f, d_r, dn_p, g1_r, sems):
    tokens, width = n.shape
    hid = h.shape[1]
    rows = x_own.shape[0]
    half = 2 * rows
    remote = swap_with_sibling()
    e3 = []
    for k in range(2):
        at, other = pl.ds(k * rows, rows), pl.ds((1 - k) * rows, rows)
        x_f[at, :] = comb[at, :] + e2[other, :]
        c = remote(x_f.at[at], x_f.at[pl.ds(half + k * rows, rows)], sems, k)
        c.start()
        e3.append(c)
    ds = [remote(src, d_r.at[pl.ds(k * rows, rows)], sems, 2 + k) for k, src in enumerate((d_own, d_far))]
    for c in ds:
        c.start()
    d_full[pl.ds(0, rows), :] = d_own[...]
    d_full[pl.ds(rows, rows), :] = d_far[...]
    gain_f = gain[...].astype(F32).reshape(1, width)

    def norm_half(k):
        for j in range(4):
            at = pl.ds(k * half + j * 32, 32)
            x = x_f[at, :].astype(F32)
            r = lax.rsqrt(jnp.mean(x * x, axis=-1, keepdims=True) + EPS)
            n[at, :] = (x * r * gain_f).astype(BF)

    def fwd_half(k):
        at = pl.ds(k * half, half)
        for j in range(hid // TILE):
            cols = pl.ds(j * TILE, TILE)
            g = mm(d_full[at, :], w2[cols, :], 1, 1).astype(BF).astype(F32)
            u = mm(n[at, :], w1[:, cols], 1, 0).astype(BF).astype(F32)
            t = jnp.tanh(GELU_C * (u + GELU_A * (u * u * u)))
            cdf = 0.5 * (1.0 + t)
            h[at, cols] = (u * cdf).astype(BF)
            du[at, cols] = (g * (cdf + u * (0.5 * (1.0 - t * t)) * (GELU_C * (1.0 + 3.0 * GELU_A * (u * u))))).astype(BF)

    def dn_half(k, sent):
        at = pl.ds(k * half, half)
        for j in range(width // TILE):
            cols = pl.ds(j * TILE, TILE)
            dn_p[at, cols] = mm(du[at, :], w1[cols, :], 1, 1)
            if sent is not None:
                sent.append(remote(dn_p.at[at, cols], g1_r.at[:, cols], sems, 4 + j))
                sent[-1].start()

    norm_half(0)
    fwd_half(0)
    for c in e3 + ds:
        c.wait()
    d_full[pl.ds(half, half), :] = d_r[...]
    norm_half(1)
    fwd_half(1)
    g1 = []
    dn_half(1, g1)
    dn_half(0, None)
    x_own[...] = x_f[pl.ds(0, rows), :]
    for j, c in enumerate(g1):
        c.wait()
        cols = pl.ds(j * TILE, TILE)
        dn_far[:, cols] = dn_p[pl.ds(rows, rows), cols] + g1_r[pl.ds(rows, rows), cols]
        dn_own[:, cols] = dn_p[pl.ds(0, rows), cols] + g1_r[pl.ds(0, rows), cols]


def mlp(comb, e2, d_own, d_far, w1, w2, gain, order):
    half, width = comb.shape
    tokens, rows = 2 * half, half // 2
    hid = w1.shape[1]
    return pl.pallas_call(
        mlp_kernel,
        name="mlp",
        out_shape=[sh((tokens, width), BF), sh((tokens, hid), BF), sh((tokens, hid), BF), sh((tokens, width), BF), sh((rows, width), BF),
                   sh((rows, width), F32), sh((rows, width), F32)],
        in_specs=[VMEM_SPEC] * 7 + [ANY_SPEC],
        out_specs=[VMEM_SPEC] * 7,
        scratch_shapes=[VMEM((tokens, width), BF), VMEM((half, width), BF), VMEM((tokens, width), F32), VMEM((half, width), F32), DMA((2, 8))],
        compiler_params=pltpu.CompilerParams(collective_id=1, has_side_effects=True, vmem_limit_bytes=16 * MIB),
        cost_estimate=pl.CostEstimate(flops=6_000_000_000, bytes_accessed=4 * MIB, transcendentals=0),
    )(comb, e2, d_own, d_far, w1, w2, gain, order)


def ysum_kernel(h, w2, y_own, y_far0, y_far1, y_p, y_r, sems):
    rows, width = y_own.shape
    half = 2 * rows
    remote = swap_with_sibling()
    copies = []
    for k in (1, 0):
        at = pl.ds(k * half, half)
        for j in range(width // TILE):
            cols = pl.ds(j * TILE, TILE)
            y_p[at, cols] = mm(h[at, :], w2[:, cols], 1, 0)
            if k == 1:
                copies.append(remote(y_p.at[at, cols], y_r.at[:, cols], sems, j))
                copies[-1].start()
    for j, c in enumerate(copies):
        c.wait()
        cols = pl.ds(j * TILE, TILE)
        y_own[:, cols] = y_p[pl.ds(0, rows), cols] + y_r[pl.ds(0, rows), cols]
        for k, out in enumerate((y_far0, y_far1)):
            at = pl.ds(rows + k * (rows // 2), rows // 2)
            out[:, cols] = y_p[at, cols] + y_r[at, cols]


def ysum(h, w2):
    tokens, width = h.shape[0], w2.shape[1]
    rows = tokens // 4
    return pl.pallas_call(
        ysum_kernel,
        name="ysum",
        out_shape=[sh((rows, width), F32), sh((rows // 2, width), F32), sh((rows // 2, width), F32)],
        in_specs=[VMEM_SPEC, VMEM_SPEC],
        out_specs=[VMEM_SPEC] * 3,
        scratch_shapes=[VMEM((tokens, width), F32), VMEM((2 * rows, width), F32), DMA((2, 4))],
        compiler_params=pltpu.CompilerParams(collective_id=2, has_side_effects=True, vmem_limit_bytes=12 * MIB),
        cost_estimate=pl.CostEstimate(flops=3_000_000_000, bytes_accessed=4 * MIB, transcendentals=0),
    )(h, w2)


def grads_kernel(n, h, du, d_full, order, table_in, token, dw1, dw2, table_g, zero, dw1_v, dw2_v, s_zero, s_w):
    lo, hi = FILL_0 + FILL_1, FILL_0 + FILL_1 + FILL_2
    fill_start(zero, table_g, s_zero, lo, hi)
    token[...] = jnp.zeros_like(token)
    width, hid = dw1.shape
    n_t = n[...].T
    for j in range(width // TILE):
        at = slice(j * TILE, (j + 1) * TILE)
        dw1_v[at, :] = mm(n_t[at, :], du[...], 1, 0)
        pltpu.make_async_copy(dw1_v.at[pl.ds(j * TILE, TILE)], dw1.at[pl.ds(j * TILE, TILE)], s_w).start()
    h_t = h[...].T
    for j in range(hid // TILE):
        at = slice(j * TILE, (j + 1) * TILE)
        dw2_v[at, :] = mm(h_t[at, :], d_full[...], 1, 0)
        pltpu.make_async_copy(dw2_v.at[pl.ds(j * TILE, TILE)], dw2.at[pl.ds(j * TILE, TILE)], s_w).start()
    pltpu.make_async_copy(dw1_v, dw1, s_w).wait()
    pltpu.make_async_copy(dw2_v, dw2, s_w).wait()
    fill_wait(zero, table_g, s_zero, lo, hi)


def grads(n, h, du, d_full, order, table_g):
    tokens, width = n.shape
    hid = h.shape[1]
    return pl.pallas_call(
        grads_kernel,
        name="grads",
        out_shape=[sh((8, 128), F32), sh((width, hid), F32), sh((hid, width), F32), sh(table_g.shape, F32)],
        in_specs=[VMEM_SPEC] * 4 + [ANY_SPEC, HBM_SPEC],
        out_specs=[VMEM_SPEC, HBM_SPEC, HBM_SPEC, HBM_SPEC],
        input_output_aliases={5: 3},
        scratch_shapes=[VMEM((ZERO_ROWS, width), F32), VMEM((width, hid), F32), VMEM((hid, width), F32), DMA(()), DMA(())],
        compiler_params=pltpu.CompilerParams(vmem_limit_bytes=24 * MIB),
        cost_estimate=pl.CostEstimate(flops=8_000_000_000, bytes_accessed=20 * MIB, transcendentals=0),
    )(n, h, du, d_full, order, table_g)


def dx_kernel(dn_own, g2, x_own, d_own, gain, order, dx):
    gain_f = gain[...].astype(F32).reshape(1, dx.shape[1])
    for j in range(dx.shape[0] // 16):
        at = pl.ds(j * 16, 16)
        a = (dn_own[at, :] + g2[at, :]) * gain_f
        x = x_own[at, :].astype(F32)
        r = lax.rsqrt(jnp.mean(x * x, axis=-1, keepdims=True) + EPS)
        proj = jnp.mean(a * x, axis=-1, keepdims=True)
        dx[at, :] = (d_own[at, :].astype(F32) + r * (a - x * r * r * proj)).astype(BF)


def dx_rows(dn_own, g2, x_own, d_own, gain, order):
    return pl.pallas_call(
        dx_kernel,
        name="dx_rows",
        out_shape=sh(x_own.shape, BF),
        in_specs=[VMEM_SPEC] * 5 + [ANY_SPEC],
        out_specs=VMEM_SPEC,
        compiler_params=pltpu.CompilerParams(vmem_limit_bytes=4 * MIB),
        cost_estimate=pl.CostEstimate(flops=1_000_000_000, bytes_accessed=MIB, transcendentals=0),
    )(dn_own, g2, x_own, d_own, gain, order)


def fill3_kernel(order, table_in, token, table_g, zero, s_zero):
    lo, hi = FILL_0 + FILL_1 + FILL_2, table_g.shape[0] // ZERO_ROWS
    fill_start(zero, table_g, s_zero, lo, hi)
    token[...] = jnp.zeros_like(token)
    fill_wait(zero, table_g, s_zero, lo, hi)


def fill3(order, table_g):
    return pl.pallas_call(
        fill3_kernel,
        name="fill3",
        out_shape=[sh((8, 128), F32), sh(table_g.shape, F32)],
        in_specs=[ANY_SPEC, HBM_SPEC],
        out_specs=[VMEM_SPEC, HBM_SPEC],
        input_output_aliases={1: 1},
        scratch_shapes=[VMEM((ZERO_ROWS, table_g.shape[1]), F32), DMA(())],
        compiler_params=pltpu.CompilerParams(vmem_limit_bytes=4 * MIB),
        cost_estimate=pl.CostEstimate(flops=5_000_000_000, bytes_accessed=16 * MIB, transcendentals=0),
    )(order, table_g)


def dx_all_kernel(dx, dx_far, order, dx_out, dx_r, sems):
    me = lax.axis_index("tp")
    rows = dx.shape[0]
    remote = swap_with_sibling()
    block = lambda m: pl.ds(pl.multiple_of((me ^ m) * rows, rows), rows)
    copies = [remote(src, dx_r.at[pl.ds(k * rows, rows)], sems, k) for k, src in enumerate((dx, dx_far))]
    for c in copies:
        c.start()
    dx_out[block(0), :] = dx[...]
    dx_out[block(2), :] = dx_far[...]
    for k, c in enumerate(copies):
        c.wait()
        dx_out[block(1 + 2 * k), :] = dx_r[pl.ds(k * rows, rows), :]


def dx_all(dx, dx_far, order):
    rows, width = dx.shape
    return pl.pallas_call(
        dx_all_kernel,
        name="dx_all",
        out_shape=sh((4 * rows, width), BF),
        in_specs=[VMEM_SPEC] * 2 + [ANY_SPEC],
        out_specs=VMEM_SPEC,
        scratch_shapes=[VMEM((2 * rows, width), BF), DMA((2, 2))],
        compiler_params=pltpu.CompilerParams(collective_id=3, has_side_effects=True, vmem_limit_bytes=4 * MIB),
        cost_estimate=pl.CostEstimate(flops=2_000_000_000, bytes_accessed=MIB, transcendentals=0),
    )(dx, dx_far, order)


def put_kernel(puts, same, dx, table_in, table_g, token, puts_s, total, s_in, s_row):
    tokens = dx.shape[0]
    load = pltpu.make_async_copy(puts, puts_s, s_in)
    load.start()
    total[...] = mm(same[...], dx[...], 1, 0)
    token[...] = jnp.zeros_like(token)
    load.wait()
    count = puts_s[tokens]

    def put(i, carry):
        word = puts_s[i]
        pltpu.make_async_copy(total.at[pl.ds(word >> 16, 1)], table_g.at[pl.ds(word & 0xFFFF, 1)], s_row).start()
        return carry

    lax.fori_loop(0, count, put, 0)

    def put_wait(size):
        def body(i, carry):
            pltpu.make_async_copy(total.at[pl.ds(0, size)], table_g.at[pl.ds(0, size)], s_row).wait()
            return carry

        return body

    lax.fori_loop(0, count >> 3, put_wait(8), 0)
    lax.fori_loop(0, count & 7, put_wait(1), 0)


def put_rows(puts, same, dx, table_g):
    return pl.pallas_call(
        put_kernel,
        name="put_rows",
        out_shape=[sh(table_g.shape, F32), sh((8, 128), F32)],
        in_specs=[ANY_SPEC, VMEM_SPEC, VMEM_SPEC, HBM_SPEC],
        out_specs=[HBM_SPEC, VMEM_SPEC],
        input_output_aliases={3: 0},
        scratch_shapes=[pltpu.SMEM(puts.shape, I32), VMEM(dx.shape, F32), DMA(()), DMA(())],
        compiler_params=pltpu.CompilerParams(vmem_limit_bytes=4 * MIB),
        cost_estimate=pl.CostEstimate(flops=3_000_000_000, bytes_accessed=2 * MIB, transcendentals=0),
    )(puts, same, dx, table_g)


def finish_kernel(x, y, y_in0, y_in1, order, out):
    part = y_in0.shape[0]
    for k, y_in in enumerate((y_in0, y_in1)):
        at = pl.ds(k * part, part)
        out[at, :] = (x[at, :].astype(F32) + (y[at, :] + y_in[...])).astype(BF)


def finish(x, y, y_in0, y_in1, order):
    return pl.pallas_call(
        finish_kernel,
        name="finish",
        out_shape=sh(x.shape, BF),
        in_specs=[VMEM_SPEC] * 4 + [ANY_SPEC],
        out_specs=VMEM_SPEC,
        compiler_params=pltpu.CompilerParams(vmem_limit_bytes=4 * MIB),
        cost_estimate=pl.CostEstimate(flops=1_000_000_000, bytes_accessed=MIB, transcendentals=0),
    )(x, y, y_in0, y_in1, order)


def solution(mesh):
    tp = mesh.shape["tp"]
    far_pairs = [(i, i ^ 2) for i in range(tp)]

    def shard_step(ids, table, gain, w1, w2, d_out):
        part, rows_mine, same, d_table = lookup(ids, table)
        part, d_send = lax.optimization_barrier((part, d_out))
        d_far = lax.ppermute(d_send, "tp", far_pairs)
        comb = pair(part)
        e2 = lax.ppermute(comb, "tp", far_pairs)
        puts, token, d_table = fill1(rows_mine, comb, d_table)
        n, h, du, d_full, x_own, dn_own, dn_far = mlp(comb, e2, d_out, d_far, w1, w2, gain, token)
        g2 = lax.ppermute(dn_far, "tp", far_pairs)
        y_own, y_far0, y_far1 = ysum(h, w2)
        y_in0 = lax.ppermute(y_far0, "tp", far_pairs)
        token, d_w1, d_w2, d_table = grads(n, h, du, d_full, y_own, d_table)
        dx = dx_rows(dn_own, g2, x_own, d_out, gain, token)
        dx_far = lax.ppermute(dx, "tp", far_pairs)
        dx, y_far1 = lax.optimization_barrier((dx, y_far1))
        y_in1 = lax.ppermute(y_far1, "tp", far_pairs)
        token, d_table = fill3(dx, d_table)
        dx_full = dx_all(dx, dx_far, token)
        d_table, done = put_rows(puts, same, dx_full, d_table)
        out = finish(x_own, y_own, y_in0, y_in1, done)
        return out, d_table, d_w1, d_w2

    return jax.shard_map(
        shard_step,
        mesh=mesh,
        in_specs=(P("dp"), P("tp", None), P(None), P(None, "tp"), P("tp", None), P(("dp", "tp"), None)),
        out_specs=(P(("dp", "tp"), None), P(("dp", "tp"), None), P("dp", "tp"), P(("dp", "tp"), None)),
        check_vma=False,
    )
```

```python
import jax
import jax.numpy as jnp
from jax import lax
from jax.experimental import pallas as pl
from jax.experimental.pallas import tpu as pltpu
from jax.sharding import PartitionSpec as P

EPS = 1e-6
BF = jnp.bfloat16
F32 = jnp.float32
I32 = jnp.int32
GELU_C = 0.7978845608028654
GELU_A = 0.044715
VMEM = pltpu.VMEM
SMEM_SPEC = pl.BlockSpec(memory_space=pltpu.SMEM)
ANY_SPEC = pl.BlockSpec(memory_space=pl.ANY)
HBM_SPEC = pl.BlockSpec(memory_space=pltpu.HBM)
VMEM_SPEC = pl.BlockSpec(memory_space=VMEM)
DMA = pltpu.SemaphoreType.DMA
TILE = 256
ZERO_ROWS = 96
FILL_AT = (0, 15, 83, 102, 124, 131)
MIB = 1 << 20
LOOKUP_VMEM = 48 * MIB
PAIR_VMEM = 8 * MIB


def mm(a, b, ca, cb):
    return lax.dot_general(a, b, (((ca,), (cb,)), ((), ())), preferred_element_type=F32)


def in_hbm(x):
    return pltpu.with_memory_space_constraint(x, pltpu.HBM)


def sh(shape, dtype):
    return jax.ShapeDtypeStruct(shape, dtype)


def fill_copy(zero, table_g, sem, i):
    return pltpu.make_async_copy(zero, table_g.at[pl.ds(pl.multiple_of(i * ZERO_ROWS, ZERO_ROWS), ZERO_ROWS)], sem)


def fill_start(zero, table_g, sem, part):
    def body(i, carry):
        fill_copy(zero, table_g, sem, i).start()
        return carry

    lax.fori_loop(FILL_AT[part], FILL_AT[part + 1], body, 0)


def fill_wait(zero, table_g, sem, part):
    def body(i, carry):
        fill_copy(zero, table_g, sem, i).wait()
        return carry

    lax.fori_loop(FILL_AT[part], FILL_AT[part + 1], body, 0)


def swap_with_sibling():
    sib = lax.axis_index("tp") ^ 1
    barrier = pltpu.get_barrier_semaphore()
    pl.semaphore_signal(barrier, inc=1, device_id={"tp": sib}, device_id_type=pl.DeviceIdType.MESH)
    pl.semaphore_wait(barrier, 1)

    def remote(src, dst, sems, i):
        return pltpu.make_async_remote_copy(
            src_ref=src, dst_ref=dst, send_sem=sems.at[0, i], recv_sem=sems.at[1, i],
            device_id={"tp": sib}, device_id_type=pl.DeviceIdType.MESH)

    return remote


def lookup_kernel(ids, ids_row, table, part, rows_mine, same, zero, table_g, ids_s, ids_v, pairs, sems, s_zero, s_ids):
    tokens, vocab = part.shape[0], table.shape[0]
    base = lax.axis_index("tp") * vocab
    group = 64
    groups = tokens // group
    loads = [pltpu.make_async_copy(ids, ids_s, s_ids.at[0]), pltpu.make_async_copy(ids_row, ids_v, s_ids.at[1])]
    for c in loads:
        c.start()
    zero[...] = jnp.zeros_like(zero)
    fill_start(zero, table_g, s_zero, 0)
    loads[0].wait()
    for k in range(groups):
        def fetch(i, carry):
            lid = ids_s[k * group + i] - base
            owned = (lid >= 0) & (lid < vocab)
            pair_id = jnp.where(owned, lid >> 1, i)
            pltpu.make_async_copy(
                table.at[pl.ds(pl.multiple_of(pair_id << 1, 2), 2)],
                pairs.at[pl.ds(pl.multiple_of(k * group * 2 + i * 2, 2), 2)],
                sems.at[k],
            ).start()
            return carry

        lax.fori_loop(0, group, fetch, 0, unroll=8)
    loads[1].wait()
    row = jnp.broadcast_to(ids_v[...].astype(F32), (tokens, tokens))
    col = row.T
    equal = row == col
    same[...] = jnp.where(equal, 1.0, 0.0).astype(BF)
    earlier = lax.broadcasted_iota(I32, (tokens, tokens), 0) < lax.broadcasted_iota(I32, (tokens, tokens), 1)
    repeat = jnp.max(jnp.where(equal & earlier, 1, 0), axis=0, keepdims=True)
    mine = ids_v[...] - base
    rows_mine[...] = jnp.where((mine >= 0) & (mine < vocab) & (repeat == 0), mine, -1)
    lid = col.astype(I32) - base
    lane = lax.broadcasted_iota(I32, (group, 2 * group), 1)
    first = lax.broadcasted_iota(I32, (group, 2 * group), 0) * 2
    for k in range(groups):
        at = lid[k * group:(k + 1) * group, :2 * group]
        owned = (at >= 0) & (at < vocab)
        pick = jnp.where(owned & (lane == first + (at & 1)), 1.0, 0.0).astype(BF)
        rows = pl.ds(k * group * 2, group * 2)
        pltpu.make_async_copy(table.at[pl.ds(0, group * 2)], pairs.at[rows], sems.at[k]).wait()
        part[pl.ds(k * group, group), :] = mm(pick, pairs[rows, :], 1, 0).astype(BF)
    fill_wait(zero, table_g, s_zero, 0)


def lookup(ids, table):
    tokens, (vocab, width) = ids.shape[0], table.shape
    return pl.pallas_call(
        lookup_kernel,
        name="lookup",
        out_shape=[sh((tokens, width), BF), sh((1, tokens), I32), sh((tokens, tokens), BF), sh((ZERO_ROWS, width), F32), sh((vocab, width), F32)],
        in_specs=[HBM_SPEC] * 3,
        out_specs=[VMEM_SPEC] * 4 + [HBM_SPEC],
        scratch_shapes=[pltpu.SMEM((tokens,), I32), VMEM((1, tokens), I32), VMEM((tokens * 2, width), BF), DMA((4,)), DMA(()), DMA((2,))],
        compiler_params=pltpu.CompilerParams(vmem_limit_bytes=LOOKUP_VMEM),
        cost_estimate=pl.CostEstimate(flops=5_000_000_000, bytes_accessed=10 * MIB, transcendentals=0),
    )(in_hbm(ids), in_hbm(ids.reshape(1, tokens)), in_hbm(table))


def pair_kernel(part, d_out, send, part_r, sems, s_in):
    me = lax.axis_index("tp")
    rows = d_out.shape[0]
    blocks = (me, me ^ 2, me ^ 1, me ^ 3)
    load = pltpu.make_async_copy(d_out, send.at[pl.ds(2 * rows, rows)], s_in)
    load.start()
    remote = swap_with_sibling()
    block = lambda k: pl.ds(pl.multiple_of(blocks[k] * rows, rows), rows)
    copies = [remote(part.at[block(2 + k)], part_r.at[pl.ds(k * rows, rows)], sems, k) for k in range(2)]
    for c in copies:
        c.start()
    for k in range(2):
        copies[k].wait()
        at = pl.ds(k * rows, rows)
        send[at, :] = part[block(k), :] + part_r[at, :]
    load.wait()


def pair(part, d_out):
    rows, width = d_out.shape
    return pl.pallas_call(
        pair_kernel,
        name="pair",
        out_shape=sh((3 * rows, width), BF),
        in_specs=[VMEM_SPEC, HBM_SPEC],
        out_specs=VMEM_SPEC,
        scratch_shapes=[VMEM((2 * rows, width), BF), DMA((2, 2)), DMA(())],
        compiler_params=pltpu.CompilerParams(collective_id=0, has_side_effects=True, vmem_limit_bytes=PAIR_VMEM),
        cost_estimate=pl.CostEstimate(flops=3_000_000_000, bytes_accessed=MIB, transcendentals=0),
    )(part, d_out)


def fill1_kernel(rows_mine, zero, order, table_in, puts, token, table_g, mine_s, puts_s, s_zero, s_list):
    load = pltpu.make_async_copy(rows_mine, mine_s, s_list)
    load.start()
    fill_start(zero, table_g, s_zero, 1)
    tokens = rows_mine.shape[1]
    token[...] = jnp.zeros_like(token)
    load.wait()

    def body(i, count):
        lid = mine_s[0, i]
        puts_s[count] = lid | (i << 16)
        return count + (lid >= 0).astype(I32)

    puts_s[tokens] = lax.fori_loop(0, tokens, body, 0, unroll=8)
    store = pltpu.make_async_copy(puts_s, puts, s_list)
    store.start()
    store.wait()
    fill_wait(zero, table_g, s_zero, 1)


def fill1(rows_mine, zero, order, table_g):
    tokens = rows_mine.shape[1]
    return pl.pallas_call(
        fill1_kernel,
        name="fill1",
        out_shape=[sh((2 * tokens,), I32), sh((8, 128), F32), sh(table_g.shape, F32)],
        in_specs=[ANY_SPEC, VMEM_SPEC, ANY_SPEC, HBM_SPEC],
        out_specs=[ANY_SPEC, VMEM_SPEC, HBM_SPEC],
        input_output_aliases={3: 2},
        scratch_shapes=[pltpu.SMEM((1, tokens), I32), pltpu.SMEM((2 * tokens,), I32), DMA(()), DMA(())],
        compiler_params=pltpu.CompilerParams(vmem_limit_bytes=8 * MIB),
        cost_estimate=pl.CostEstimate(flops=9_000_000_000, bytes_accessed=20 * MIB, transcendentals=0),
    )(rows_mine, zero, order, table_g)


def share_kernel(send, got, order, x_f, d_full, x_r, d_r, sems):
    rows = send.shape[0] // 3
    half = 2 * rows
    remote = swap_with_sibling()
    copies = []
    for k in range(2):
        at, other = pl.ds(k * rows, rows), pl.ds((1 - k) * rows, rows)
        x_f[at, :] = send[at, :] + got[other, :]
        copies.append(remote(x_f.at[at], x_r.at[at], sems, k))
        copies[-1].start()
    for k, src in enumerate((send, got)):
        copies.append(remote(src.at[pl.ds(half, rows)], d_r.at[pl.ds(k * rows, rows)], sems, 2 + k))
        copies[-1].start()
        d_full[pl.ds(k * rows, rows), :] = src[pl.ds(half, rows), :]
    for k in range(2):
        copies[k].wait()
        x_f[pl.ds(half + k * rows, rows), :] = x_r[pl.ds(k * rows, rows), :]
    for k in range(2):
        copies[2 + k].wait()
        d_full[pl.ds(half + k * rows, rows), :] = d_r[pl.ds(k * rows, rows), :]


def share(send, got, order):
    rows, width = send.shape[0] // 3, send.shape[1]
    return pl.pallas_call(
        share_kernel,
        name="share",
        out_shape=[sh((4 * rows, width), BF)] * 2,
        in_specs=[VMEM_SPEC] * 2 + [ANY_SPEC],
        out_specs=[VMEM_SPEC] * 2,
        scratch_shapes=[VMEM((2 * rows, width), BF), VMEM((2 * rows, width), BF), DMA((2, 4))],
        compiler_params=pltpu.CompilerParams(collective_id=1, has_side_effects=True, vmem_limit_bytes=8 * MIB),
        cost_estimate=pl.CostEstimate(flops=3_000_000_000, bytes_accessed=MIB, transcendentals=0),
    )(send, got, order)


def mlp_kernel(x_f, d_full, w1, w2, gain, zero, table_in, n, h, du, dn_p, y_p, table_g, s_zero):
    fill_start(zero, table_g, s_zero, 2)
    tokens, width = n.shape
    hid = h.shape[1]
    gain_f = gain[...].astype(F32).reshape(1, width)
    for j in range(tokens // 32):
        at = pl.ds(j * 32, 32)
        x = x_f[at, :].astype(F32)
        r = lax.rsqrt(jnp.mean(x * x, axis=-1, keepdims=True) + EPS)
        n[at, :] = (x * r * gain_f).astype(BF)
    for j in range(hid // TILE):
        cols = pl.ds(j * TILE, TILE)
        g = mm(d_full[...], w2[cols, :], 1, 1).astype(BF).astype(F32)
        u = mm(n[...], w1[:, cols], 1, 0).astype(BF).astype(F32)
        t = jnp.tanh(GELU_C * (u + GELU_A * (u * u * u)))
        cdf = 0.5 * (1.0 + t)
        h[:, cols] = (u * cdf).astype(BF)
        du[:, cols] = (g * (cdf + u * (0.5 * (1.0 - t * t)) * (GELU_C * (1.0 + 3.0 * GELU_A * (u * u))))).astype(BF)
    for j in range(width // TILE):
        cols = pl.ds(j * TILE, TILE)
        dn_p[:, cols] = mm(du[...], w1[cols, :], 1, 1)
        y_p[:, cols] = mm(h[...], w2[:, cols], 1, 0)
    fill_wait(zero, table_g, s_zero, 2)


def mlp(x_f, d_full, w1, w2, gain, zero, table_g):
    tokens, width = x_f.shape
    hid = w1.shape[1]
    return pl.pallas_call(
        mlp_kernel,
        name="mlp",
        out_shape=[sh((tokens, width), BF), sh((tokens, hid), BF), sh((tokens, hid), BF), sh((tokens, width), F32),
                   sh((tokens, width), F32), sh(table_g.shape, F32)],
        in_specs=[VMEM_SPEC] * 6 + [HBM_SPEC],
        out_specs=[VMEM_SPEC] * 5 + [HBM_SPEC],
        input_output_aliases={6: 5},
        scratch_shapes=[DMA(())],
        compiler_params=pltpu.CompilerParams(vmem_limit_bytes=16 * MIB),
        cost_estimate=pl.CostEstimate(flops=6_000_000_000, bytes_accessed=4 * MIB, transcendentals=0),
    )(x_f, d_full, w1, w2, gain, zero, table_g)


def sums_kernel(dn_p, y_p, dn_own, dn_far, y_own, y_far, dn_r, y_r, sems):
    rows = dn_own.shape[0]
    half = 2 * rows
    remote = swap_with_sibling()
    copies = []
    for i, (src, dst) in enumerate(((dn_p, dn_r), (y_p, y_r))):
        for k in (1, 0):
            copies.append(remote(src.at[pl.ds(half + k * rows, rows)], dst.at[pl.ds(k * rows, rows)], sems, 2 * i + k))
            copies[-1].start()
    for c, out, src, dst, k in zip(copies, (dn_far, dn_own, y_far, y_own), (dn_p, dn_p, y_p, y_p), (dn_r, dn_r, y_r, y_r), (1, 0, 1, 0)):
        c.wait()
        at = pl.ds(k * rows, rows)
        out[...] = src[at, :] + dst[at, :]


def sums(dn_p, y_p):
    tokens, width = dn_p.shape
    rows = tokens // 4
    return pl.pallas_call(
        sums_kernel,
        name="sums",
        out_shape=[sh((rows, width), F32)] * 4,
        in_specs=[VMEM_SPEC] * 2,
        out_specs=[VMEM_SPEC] * 4,
        scratch_shapes=[VMEM((2 * rows, width), F32), VMEM((2 * rows, width), F32), DMA((2, 4))],
        compiler_params=pltpu.CompilerParams(collective_id=2, has_side_effects=True, vmem_limit_bytes=8 * MIB),
        cost_estimate=pl.CostEstimate(flops=4_000_000_000, bytes_accessed=4 * MIB, transcendentals=0),
    )(dn_p, y_p)


def grads_kernel(n, h, du, d_full, zero, order, table_in, token, dw1, dw2, table_g, dw1_v, dw2_v, s_zero, s_w):
    fill_start(zero, table_g, s_zero, 3)
    token[...] = jnp.zeros_like(token)
    width, hid = dw1.shape
    n_t = n[...].T
    for j in range(width // TILE):
        at = slice(j * TILE, (j + 1) * TILE)
        dw1_v[at, :] = mm(n_t[at, :], du[...], 1, 0)
        pltpu.make_async_copy(dw1_v.at[pl.ds(j * TILE, TILE)], dw1.at[pl.ds(j * TILE, TILE)], s_w).start()
    h_t = h[...].T
    for j in range(hid // TILE):
        at = slice(j * TILE, (j + 1) * TILE)
        dw2_v[at, :] = mm(h_t[at, :], d_full[...], 1, 0)
        pltpu.make_async_copy(dw2_v.at[pl.ds(j * TILE, TILE)], dw2.at[pl.ds(j * TILE, TILE)], s_w).start()
    pltpu.make_async_copy(dw1_v, dw1, s_w).wait()
    pltpu.make_async_copy(dw2_v, dw2, s_w).wait()
    fill_wait(zero, table_g, s_zero, 3)


def grads(n, h, du, d_full, zero, order, table_g):
    tokens, width = n.shape
    hid = h.shape[1]
    return pl.pallas_call(
        grads_kernel,
        name="grads",
        out_shape=[sh((8, 128), F32), sh((width, hid), F32), sh((hid, width), F32), sh(table_g.shape, F32)],
        in_specs=[VMEM_SPEC] * 5 + [ANY_SPEC, HBM_SPEC],
        out_specs=[VMEM_SPEC, HBM_SPEC, HBM_SPEC, HBM_SPEC],
        input_output_aliases={6: 3},
        scratch_shapes=[VMEM((width, hid), F32), VMEM((hid, width), F32), DMA(()), DMA(())],
        compiler_params=pltpu.CompilerParams(vmem_limit_bytes=24 * MIB),
        cost_estimate=pl.CostEstimate(flops=8_000_000_000, bytes_accessed=20 * MIB, transcendentals=0),
    )(n, h, du, d_full, zero, order, table_g)


def dx_kernel(dn_own, g2, x_own, d_own, gain, order, dx):
    gain_f = gain[...].astype(F32).reshape(1, dx.shape[1])
    for j in range(dx.shape[0] // 16):
        at = pl.ds(j * 16, 16)
        a = (dn_own[at, :] + g2[at, :]) * gain_f
        x = x_own[at, :].astype(F32)
        r = lax.rsqrt(jnp.mean(x * x, axis=-1, keepdims=True) + EPS)
        proj = jnp.mean(a * x, axis=-1, keepdims=True)
        dx[at, :] = (d_own[at, :].astype(F32) + r * (a - x * r * r * proj)).astype(BF)


def dx_rows(dn_own, g2, x_own, d_own, gain, order):
    return pl.pallas_call(
        dx_kernel,
        name="dx_rows",
        out_shape=sh(d_own.shape, BF),
        in_specs=[VMEM_SPEC] * 5 + [ANY_SPEC],
        out_specs=VMEM_SPEC,
        compiler_params=pltpu.CompilerParams(vmem_limit_bytes=4 * MIB),
        cost_estimate=pl.CostEstimate(flops=1_000_000_000, bytes_accessed=MIB, transcendentals=0),
    )(dn_own, g2, x_own, d_own, gain, order)


def fill3_kernel(zero, order, table_in, token, table_g, s_zero):
    fill_start(zero, table_g, s_zero, 4)
    token[...] = jnp.zeros_like(token)
    fill_wait(zero, table_g, s_zero, 4)


def fill3(zero, order, table_g):
    return pl.pallas_call(
        fill3_kernel,
        name="fill3",
        out_shape=[sh((8, 128), F32), sh(table_g.shape, F32)],
        in_specs=[VMEM_SPEC, ANY_SPEC, HBM_SPEC],
        out_specs=[VMEM_SPEC, HBM_SPEC],
        input_output_aliases={2: 1},
        scratch_shapes=[DMA(())],
        compiler_params=pltpu.CompilerParams(vmem_limit_bytes=4 * MIB),
        cost_estimate=pl.CostEstimate(flops=4_000_000_000, bytes_accessed=16 * MIB, transcendentals=0),
    )(zero, order, table_g)


def dx_all_kernel(dx, dx_far, order, dx_out, dx_r, sems):
    me = lax.axis_index("tp")
    rows = dx.shape[0]
    remote = swap_with_sibling()
    block = lambda m: pl.ds(pl.multiple_of((me ^ m) * rows, rows), rows)
    copies = [remote(src, dx_r.at[pl.ds(k * rows, rows)], sems, k) for k, src in enumerate((dx, dx_far))]
    for c in copies:
        c.start()
    dx_out[block(0), :] = dx[...]
    dx_out[block(2), :] = dx_far[...]
    for k, c in enumerate(copies):
        c.wait()
        dx_out[block(1 + 2 * k), :] = dx_r[pl.ds(k * rows, rows), :]


def dx_all(dx, dx_far, order):
    rows, width = dx.shape
    return pl.pallas_call(
        dx_all_kernel,
        name="dx_all",
        out_shape=sh((4 * rows, width), BF),
        in_specs=[VMEM_SPEC] * 2 + [ANY_SPEC],
        out_specs=VMEM_SPEC,
        scratch_shapes=[VMEM((2 * rows, width), BF), DMA((2, 2))],
        compiler_params=pltpu.CompilerParams(collective_id=3, has_side_effects=True, vmem_limit_bytes=4 * MIB),
        cost_estimate=pl.CostEstimate(flops=2_000_000_000, bytes_accessed=MIB, transcendentals=0),
    )(dx, dx_far, order)


def put_kernel(puts, same, dx, table_in, table_g, token, puts_s, total, s_in, s_row):
    tokens = dx.shape[0]
    load = pltpu.make_async_copy(puts, puts_s, s_in)
    load.start()
    total[...] = mm(same[...], dx[...], 1, 0)
    token[...] = jnp.zeros_like(token)
    load.wait()
    count = puts_s[tokens]

    def put(i, carry):
        word = puts_s[i]
        pltpu.make_async_copy(total.at[pl.ds(word >> 16, 1)], table_g.at[pl.ds(word & 0xFFFF, 1)], s_row).start()
        return carry

    lax.fori_loop(0, count, put, 0)

    def put_wait(size):
        def body(i, carry):
            pltpu.make_async_copy(total.at[pl.ds(0, size)], table_g.at[pl.ds(0, size)], s_row).wait()
            return carry

        return body

    lax.fori_loop(0, count >> 3, put_wait(8), 0)
    lax.fori_loop(0, count & 7, put_wait(1), 0)


def put_rows(puts, same, dx, table_g):
    return pl.pallas_call(
        put_kernel,
        name="put_rows",
        out_shape=[sh(table_g.shape, F32), sh((8, 128), F32)],
        in_specs=[ANY_SPEC, VMEM_SPEC, VMEM_SPEC, HBM_SPEC],
        out_specs=[HBM_SPEC, VMEM_SPEC],
        input_output_aliases={3: 0},
        scratch_shapes=[pltpu.SMEM(puts.shape, I32), VMEM(dx.shape, F32), DMA(()), DMA(())],
        compiler_params=pltpu.CompilerParams(vmem_limit_bytes=4 * MIB),
        cost_estimate=pl.CostEstimate(flops=3_000_000_000, bytes_accessed=2 * MIB, transcendentals=0),
    )(puts, same, dx, table_g)


def finish_kernel(x, y, y_in, order, out):
    out[...] = (x[pl.ds(0, out.shape[0]), :].astype(F32) + (y[...] + y_in[...])).astype(BF)


def finish(x, y, y_in, order):
    return pl.pallas_call(
        finish_kernel,
        name="finish",
        out_shape=sh(y.shape, BF),
        in_specs=[VMEM_SPEC] * 3 + [ANY_SPEC],
        out_specs=VMEM_SPEC,
        compiler_params=pltpu.CompilerParams(vmem_limit_bytes=4 * MIB),
        cost_estimate=pl.CostEstimate(flops=1_000_000_000, bytes_accessed=MIB, transcendentals=0),
    )(x, y, y_in, order)


def solution(mesh):
    tp = mesh.shape["tp"]
    far_pairs = [(i, i ^ 2) for i in range(tp)]

    def shard_step(ids, table, gain, w1, w2, d_out):
        part, rows_mine, same, zero, d_table = lookup(ids, table)
        send = pair(part, in_hbm(d_out))
        got = lax.ppermute(send, "tp", far_pairs)
        puts, token, d_table = fill1(rows_mine, zero, send, d_table)
        x_f, d_full = share(send, got, token)
        n, h, du, dn_p, y_p, d_table = mlp(x_f, d_full, w1, w2, gain, zero, d_table)
        dn_own, dn_far, y_own, y_far = sums(dn_p, y_p)
        g2 = lax.ppermute(dn_far, "tp", far_pairs)
        token, d_w1, d_w2, d_table = grads(n, h, du, d_full, zero, dn_own, d_table)
        dx = dx_rows(dn_own, g2, x_f, d_out, gain, token)
        dx_far = lax.ppermute(dx, "tp", far_pairs)
        dx, y_far = lax.optimization_barrier((dx, y_far))
        y_in = lax.ppermute(y_far, "tp", far_pairs)
        token, d_table = fill3(zero, dx, d_table)
        dx_full = dx_all(dx, dx_far, token)
        d_table, done = put_rows(puts, same, dx_full, d_table)
        out = finish(x_f, y_own, y_in, done)
        return out, d_table, d_w1, d_w2

    return jax.shard_map(
        shard_step,
        mesh=mesh,
        in_specs=(P("dp"), P("tp", None), P(None), P(None, "tp"), P("tp", None), P(("dp", "tp"), None)),
        out_specs=(P(("dp", "tp"), None), P(("dp", "tp"), None), P("dp", "tp"), P(("dp", "tp"), None)),
        check_vma=False,
    )
```

```python
import jax
import jax.numpy as jnp
from jax import lax
from jax.experimental import pallas as pl
from jax.experimental.pallas import tpu as pltpu
from jax.sharding import PartitionSpec as P

EPS = 1e-6
BF = jnp.bfloat16
F32 = jnp.float32
I32 = jnp.int32
GELU_C = 0.7978845608028654
GELU_A = 0.044715
VMEM = pltpu.VMEM
SMEM_SPEC = pl.BlockSpec(memory_space=pltpu.SMEM)
ANY_SPEC = pl.BlockSpec(memory_space=pl.ANY)
HBM_SPEC = pl.BlockSpec(memory_space=pltpu.HBM)
VMEM_SPEC = pl.BlockSpec(memory_space=VMEM)
DMA = pltpu.SemaphoreType.DMA
TILE = 256
ZERO_ROWS = 96
FILL_AT = (0, 15, 95, 106, 108, 131)
MIB = 1 << 20
LOOKUP_VMEM = 48 * MIB
PAIR_VMEM = 8 * MIB


def mm(a, b, ca, cb):
    return lax.dot_general(a, b, (((ca,), (cb,)), ((), ())), preferred_element_type=F32)


def in_hbm(x):
    return pltpu.with_memory_space_constraint(x, pltpu.HBM)


def sh(shape, dtype):
    return jax.ShapeDtypeStruct(shape, dtype)


def fill_copy(zero, table_g, sem, i):
    return pltpu.make_async_copy(zero, table_g.at[pl.ds(pl.multiple_of(i * ZERO_ROWS, ZERO_ROWS), ZERO_ROWS)], sem)


def fill_start(zero, table_g, sem, part):
    def body(i, carry):
        fill_copy(zero, table_g, sem, i).start()
        return carry

    lax.fori_loop(FILL_AT[part], FILL_AT[part + 1], body, 0)


def fill_wait(zero, table_g, sem, part):
    def body(i, carry):
        fill_copy(zero, table_g, sem, i).wait()
        return carry

    lax.fori_loop(FILL_AT[part], FILL_AT[part + 1], body, 0)


def swap_with_sibling():
    sib = lax.axis_index("tp") ^ 1
    barrier = pltpu.get_barrier_semaphore()
    pl.semaphore_signal(barrier, inc=1, device_id={"tp": sib}, device_id_type=pl.DeviceIdType.MESH)
    pl.semaphore_wait(barrier, 1)

    def remote(src, dst, sems, i):
        return pltpu.make_async_remote_copy(
            src_ref=src, dst_ref=dst, send_sem=sems.at[0, i], recv_sem=sems.at[1, i],
            device_id={"tp": sib}, device_id_type=pl.DeviceIdType.MESH)

    return remote


def lookup_kernel(ids, ids_row, table, part, rows_mine, same, zero, table_g, ids_s, ids_v, pairs, sems, s_zero, s_ids):
    tokens, vocab = part.shape[0], table.shape[0]
    base = lax.axis_index("tp") * vocab
    group = 64
    groups = tokens // group
    loads = [pltpu.make_async_copy(ids, ids_s, s_ids.at[0]), pltpu.make_async_copy(ids_row, ids_v, s_ids.at[1])]
    for c in loads:
        c.start()
    zero[...] = jnp.zeros_like(zero)
    fill_start(zero, table_g, s_zero, 0)
    loads[0].wait()

    def fetch(k, carry):
        for i in range(group):
            token = k * group + i
            lid = ids_s[token] - base
            owned = (lid >= 0) & (lid < vocab)
            row = jnp.where(owned, lid & -2, 2 * token)
            pltpu.make_async_copy(table.at[pl.ds(pl.multiple_of(row, 2), 2)], pairs.at[k, pl.ds(2 * i, 2)], sems.at[k]).start()
        return carry

    lax.fori_loop(0, groups, fetch, 0)
    loads[1].wait()
    row = jnp.broadcast_to(ids_v[...].astype(F32), (tokens, tokens))
    col = row.T
    equal = row == col
    same[...] = jnp.where(equal, 1.0, 0.0).astype(BF)
    earlier = lax.broadcasted_iota(I32, (tokens, tokens), 0) < lax.broadcasted_iota(I32, (tokens, tokens), 1)
    repeat = jnp.max(jnp.where(equal & earlier, 1, 0), axis=0, keepdims=True)
    mine = ids_v[...] - base
    rows_mine[...] = jnp.where((mine >= 0) & (mine < vocab) & (repeat == 0), mine, -1)
    lid = col.astype(I32) - base
    lane = lax.broadcasted_iota(I32, (group, 2 * group), 1)
    first = lax.broadcasted_iota(I32, (group, 2 * group), 0) * 2
    for k in range(groups):
        at = lid[k * group:(k + 1) * group, :2 * group]
        owned = (at >= 0) & (at < vocab)
        pick = jnp.where(owned & (lane == first + (at & 1)), 1.0, 0.0).astype(BF)
        pltpu.make_async_copy(table.at[pl.ds(0, group * 2)], pairs.at[k], sems.at[k]).wait()
        part[pl.ds(k * group, group), :] = mm(pick, pairs[k], 1, 0).astype(BF)
    fill_wait(zero, table_g, s_zero, 0)


def lookup(ids, table):
    tokens, (vocab, width) = ids.shape[0], table.shape
    return pl.pallas_call(
        lookup_kernel,
        name="lookup",
        out_shape=[sh((tokens, width), BF), sh((1, tokens), I32), sh((tokens, tokens), BF), sh((ZERO_ROWS, width), F32), sh((vocab, width), F32)],
        in_specs=[HBM_SPEC] * 3,
        out_specs=[VMEM_SPEC] * 4 + [HBM_SPEC],
        scratch_shapes=[pltpu.SMEM((tokens,), I32), VMEM((1, tokens), I32), VMEM((4, tokens // 2, width), BF), DMA((4,)), DMA(()), DMA((2,))],
        compiler_params=pltpu.CompilerParams(vmem_limit_bytes=LOOKUP_VMEM),
        cost_estimate=pl.CostEstimate(flops=5_000_000_000, bytes_accessed=10 * MIB, transcendentals=0),
    )(in_hbm(ids), in_hbm(ids.reshape(1, tokens)), in_hbm(table))


def pair_kernel(part, d_out, send, part_r, sems, s_in):
    me = lax.axis_index("tp")
    rows = d_out.shape[0]
    blocks = (me, me ^ 2, me ^ 1, me ^ 3)
    load = pltpu.make_async_copy(d_out, send.at[pl.ds(2 * rows, rows)], s_in)
    load.start()
    remote = swap_with_sibling()
    block = lambda k: pl.ds(pl.multiple_of(blocks[k] * rows, rows), rows)
    copies = [remote(part.at[block(2 + k)], part_r.at[pl.ds(k * rows, rows)], sems, k) for k in range(2)]
    for c in copies:
        c.start()
    for k in range(2):
        copies[k].wait()
        at = pl.ds(k * rows, rows)
        send[at, :] = part[block(k), :] + part_r[at, :]
    load.wait()


def pair(part, d_out):
    rows, width = d_out.shape
    return pl.pallas_call(
        pair_kernel,
        name="pair",
        out_shape=sh((3 * rows, width), BF),
        in_specs=[VMEM_SPEC, HBM_SPEC],
        out_specs=VMEM_SPEC,
        scratch_shapes=[VMEM((2 * rows, width), BF), DMA((2, 2)), DMA(())],
        compiler_params=pltpu.CompilerParams(collective_id=0, has_side_effects=True, vmem_limit_bytes=PAIR_VMEM),
        cost_estimate=pl.CostEstimate(flops=3_000_000_000, bytes_accessed=MIB, transcendentals=0),
    )(part, d_out)


def fill1_kernel(rows_mine, zero, order, table_in, puts, token, table_g, mine_s, puts_s, s_zero, s_list):
    load = pltpu.make_async_copy(rows_mine, mine_s, s_list)
    load.start()
    fill_start(zero, table_g, s_zero, 1)
    tokens = rows_mine.shape[1]
    token[...] = jnp.zeros_like(token)
    load.wait()

    def body(i, count):
        lid = mine_s[0, i]
        puts_s[count] = lid | (i << 16)
        return count + (lid >= 0).astype(I32)

    puts_s[tokens] = lax.fori_loop(0, tokens, body, 0, unroll=8)
    store = pltpu.make_async_copy(puts_s, puts, s_list)
    store.start()
    store.wait()
    fill_wait(zero, table_g, s_zero, 1)


def fill1(rows_mine, zero, order, table_g):
    tokens = rows_mine.shape[1]
    return pl.pallas_call(
        fill1_kernel,
        name="fill1",
        out_shape=[sh((2 * tokens,), I32), sh((8, 128), F32), sh(table_g.shape, F32)],
        in_specs=[ANY_SPEC, VMEM_SPEC, ANY_SPEC, HBM_SPEC],
        out_specs=[ANY_SPEC, VMEM_SPEC, HBM_SPEC],
        input_output_aliases={3: 2},
        scratch_shapes=[pltpu.SMEM((1, tokens), I32), pltpu.SMEM((2 * tokens,), I32), DMA(()), DMA(())],
        compiler_params=pltpu.CompilerParams(vmem_limit_bytes=8 * MIB),
        cost_estimate=pl.CostEstimate(flops=9_000_000_000, bytes_accessed=20 * MIB, transcendentals=0),
    )(rows_mine, zero, order, table_g)


def share_kernel(send, got, order, x_f, d_full, x_r, d_r, sems):
    rows = send.shape[0] // 3
    half = 2 * rows
    remote = swap_with_sibling()
    copies = []
    for k in range(2):
        at, other = pl.ds(k * rows, rows), pl.ds((1 - k) * rows, rows)
        x_f[at, :] = send[at, :] + got[other, :]
        copies.append(remote(x_f.at[at], x_r.at[at], sems, k))
        copies[-1].start()
    for k, src in enumerate((send, got)):
        copies.append(remote(src.at[pl.ds(half, rows)], d_r.at[pl.ds(k * rows, rows)], sems, 2 + k))
        copies[-1].start()
        d_full[pl.ds(k * rows, rows), :] = src[pl.ds(half, rows), :]
    for k in range(2):
        copies[k].wait()
        x_f[pl.ds(half + k * rows, rows), :] = x_r[pl.ds(k * rows, rows), :]
    for k in range(2):
        copies[2 + k].wait()
        d_full[pl.ds(half + k * rows, rows), :] = d_r[pl.ds(k * rows, rows), :]


def share(send, got, order):
    rows, width = send.shape[0] // 3, send.shape[1]
    return pl.pallas_call(
        share_kernel,
        name="share",
        out_shape=[sh((4 * rows, width), BF)] * 2,
        in_specs=[VMEM_SPEC] * 2 + [ANY_SPEC],
        out_specs=[VMEM_SPEC] * 2,
        scratch_shapes=[VMEM((2 * rows, width), BF), VMEM((2 * rows, width), BF), DMA((2, 4))],
        compiler_params=pltpu.CompilerParams(collective_id=1, has_side_effects=True, vmem_limit_bytes=8 * MIB),
        cost_estimate=pl.CostEstimate(flops=3_000_000_000, bytes_accessed=MIB, transcendentals=0),
    )(send, got, order)


def mlp_kernel(x_f, d_full, w1, w2, gain, zero, table_in, n, h, du, dn_p, table_g, s_zero):
    fill_start(zero, table_g, s_zero, 2)
    tokens, width = n.shape
    hid = h.shape[1]
    gain_f = gain[...].astype(F32).reshape(1, width)
    for j in range(tokens // 32):
        at = pl.ds(j * 32, 32)
        x = x_f[at, :].astype(F32)
        r = lax.rsqrt(jnp.mean(x * x, axis=-1, keepdims=True) + EPS)
        n[at, :] = (x * r * gain_f).astype(BF)
    for j in range(hid // TILE):
        cols = pl.ds(j * TILE, TILE)
        g = mm(d_full[...], w2[cols, :], 1, 1).astype(BF).astype(F32)
        u = mm(n[...], w1[:, cols], 1, 0).astype(BF).astype(F32)
        t = jnp.tanh(GELU_C * (u + GELU_A * (u * u * u)))
        cdf = 0.5 * (1.0 + t)
        h[:, cols] = (u * cdf).astype(BF)
        du[:, cols] = (g * (cdf + u * (0.5 * (1.0 - t * t)) * (GELU_C * (1.0 + 3.0 * GELU_A * (u * u))))).astype(BF)
    half = tokens // 2
    for j in range(width // TILE):
        cols = pl.ds(j * TILE, TILE)
        dn_p[:, cols] = mm(du[pl.ds(half, half), :], w1[cols, :], 1, 1)
    fill_wait(zero, table_g, s_zero, 2)


def mlp(x_f, d_full, w1, w2, gain, zero, table_g):
    tokens, width = x_f.shape
    hid = w1.shape[1]
    return pl.pallas_call(
        mlp_kernel,
        name="mlp",
        out_shape=[sh((tokens, width), BF), sh((tokens, hid), BF), sh((tokens, hid), BF), sh((tokens // 2, width), F32),
                   sh(table_g.shape, F32)],
        in_specs=[VMEM_SPEC] * 6 + [HBM_SPEC],
        out_specs=[VMEM_SPEC] * 4 + [HBM_SPEC],
        input_output_aliases={6: 4},
        scratch_shapes=[DMA(())],
        compiler_params=pltpu.CompilerParams(vmem_limit_bytes=16 * MIB),
        cost_estimate=pl.CostEstimate(flops=6_000_000_000, bytes_accessed=4 * MIB, transcendentals=0),
    )(x_f, d_full, w1, w2, gain, zero, table_g)


def sums_kernel(dn_p, du, h, w1, w2, dn_own, dn_far, y_p, dn_r, dn_m, sems):
    rows, width = dn_own.shape
    half = 2 * rows
    remote = swap_with_sibling()
    copies = [remote(dn_p.at[pl.ds(k * rows, rows)], dn_r.at[pl.ds(k * rows, rows)], sems, k) for k in (1, 0)]
    for c in copies:
        c.start()
    for j in range(width // TILE):
        cols = pl.ds(j * TILE, TILE)
        dn_m[:, cols] = mm(du[pl.ds(0, half), :], w1[cols, :], 1, 1)
    for j in range(width // TILE):
        cols = pl.ds(j * TILE, TILE)
        y_p[:, cols] = mm(h[...], w2[:, cols], 1, 0)
    for c, out, k in zip(copies, (dn_far, dn_own), (1, 0)):
        c.wait()
        at = pl.ds(k * rows, rows)
        out[...] = dn_m[at, :] + dn_r[at, :]


def sums(dn_p, du, h, w1, w2):
    half, width = dn_p.shape
    rows = half // 2
    return pl.pallas_call(
        sums_kernel,
        name="sums",
        out_shape=[sh((rows, width), F32), sh((rows, width), F32), sh((2 * half, width), F32)],
        in_specs=[VMEM_SPEC] * 5,
        out_specs=[VMEM_SPEC] * 3,
        scratch_shapes=[VMEM((half, width), F32), VMEM((half, width), F32), DMA((2, 2))],
        compiler_params=pltpu.CompilerParams(collective_id=2, has_side_effects=True, vmem_limit_bytes=16 * MIB),
        cost_estimate=pl.CostEstimate(flops=4_000_000_000, bytes_accessed=4 * MIB, transcendentals=0),
    )(dn_p, du, h, w1, w2)


def ysum_kernel(y_p, order, y_own, y_far0, y_far1, y_r, sems):
    rows, _ = y_own.shape
    half, part = 2 * rows, rows // 2
    remote = swap_with_sibling()
    places = ((rows, y_far0), (rows + part, y_far1), (0, y_own))
    copies = [remote(y_p.at[pl.ds(half + at, out.shape[0])], y_r.at[pl.ds(at, out.shape[0])], sems, k) for k, (at, out) in enumerate(places)]
    for c in copies:
        c.start()
    for c, (at, out) in zip(copies, places):
        c.wait()
        rows_at = pl.ds(at, out.shape[0])
        out[...] = y_p[rows_at, :] + y_r[rows_at, :]


def ysum(y_p, order):
    tokens, width = y_p.shape
    rows = tokens // 4
    return pl.pallas_call(
        ysum_kernel,
        name="ysum",
        out_shape=[sh((rows, width), F32), sh((rows // 2, width), F32), sh((rows // 2, width), F32)],
        in_specs=[VMEM_SPEC, ANY_SPEC],
        out_specs=[VMEM_SPEC] * 3,
        scratch_shapes=[VMEM((2 * rows, width), F32), DMA((2, 3))],
        compiler_params=pltpu.CompilerParams(collective_id=4, has_side_effects=True, vmem_limit_bytes=8 * MIB),
        cost_estimate=pl.CostEstimate(flops=3_000_000_000, bytes_accessed=4 * MIB, transcendentals=0),
    )(y_p, order)


def grads_kernel(n, h, du, d_full, zero, order, table_in, token, dw1, dw2, table_g, dw1_v, dw2_v, s_zero, s_w):
    fill_start(zero, table_g, s_zero, 3)
    token[...] = jnp.zeros_like(token)
    width, hid = dw1.shape
    n_t = n[...].T
    for j in range(width // TILE):
        at = slice(j * TILE, (j + 1) * TILE)
        dw1_v[at, :] = mm(n_t[at, :], du[...], 1, 0)
        pltpu.make_async_copy(dw1_v.at[pl.ds(j * TILE, TILE)], dw1.at[pl.ds(j * TILE, TILE)], s_w).start()
    h_t = h[...].T
    for j in range(hid // TILE):
        at = slice(j * TILE, (j + 1) * TILE)
        dw2_v[at, :] = mm(h_t[at, :], d_full[...], 1, 0)
        pltpu.make_async_copy(dw2_v.at[pl.ds(j * TILE, TILE)], dw2.at[pl.ds(j * TILE, TILE)], s_w).start()
    pltpu.make_async_copy(dw1_v, dw1, s_w).wait()
    pltpu.make_async_copy(dw2_v, dw2, s_w).wait()
    fill_wait(zero, table_g, s_zero, 3)


def grads(n, h, du, d_full, zero, order, table_g):
    _, width = n.shape
    hid = h.shape[1]
    return pl.pallas_call(
        grads_kernel,
        name="grads",
        out_shape=[sh((8, 128), F32), sh((width, hid), F32), sh((hid, width), F32), sh(table_g.shape, F32)],
        in_specs=[VMEM_SPEC] * 5 + [ANY_SPEC, HBM_SPEC],
        out_specs=[VMEM_SPEC, HBM_SPEC, HBM_SPEC, HBM_SPEC],
        input_output_aliases={6: 3},
        scratch_shapes=[VMEM((width, hid), F32), VMEM((hid, width), F32), DMA(()), DMA(())],
        compiler_params=pltpu.CompilerParams(vmem_limit_bytes=24 * MIB),
        cost_estimate=pl.CostEstimate(flops=8_000_000_000, bytes_accessed=20 * MIB, transcendentals=0),
    )(n, h, du, d_full, zero, order, table_g)


def dx_kernel(dn_own, g2, x_own, d_own, gain, order, dx):
    gain_f = gain[...].astype(F32).reshape(1, dx.shape[1])
    for j in range(dx.shape[0] // 16):
        at = pl.ds(j * 16, 16)
        a = (dn_own[at, :] + g2[at, :]) * gain_f
        x = x_own[at, :].astype(F32)
        r = lax.rsqrt(jnp.mean(x * x, axis=-1, keepdims=True) + EPS)
        proj = jnp.mean(a * x, axis=-1, keepdims=True)
        dx[at, :] = (d_own[at, :].astype(F32) + r * (a - x * r * r * proj)).astype(BF)


def dx_rows(dn_own, g2, x_own, d_own, gain, order):
    return pl.pallas_call(
        dx_kernel,
        name="dx_rows",
        out_shape=sh(d_own.shape, BF),
        in_specs=[VMEM_SPEC] * 5 + [ANY_SPEC],
        out_specs=VMEM_SPEC,
        compiler_params=pltpu.CompilerParams(vmem_limit_bytes=4 * MIB),
        cost_estimate=pl.CostEstimate(flops=1_000_000_000, bytes_accessed=MIB, transcendentals=0),
    )(dn_own, g2, x_own, d_own, gain, order)


def fill3_kernel(zero, order, table_in, token, table_g, s_zero):
    fill_start(zero, table_g, s_zero, 4)
    token[...] = jnp.zeros_like(token)
    fill_wait(zero, table_g, s_zero, 4)


def fill3(zero, order, table_g):
    return pl.pallas_call(
        fill3_kernel,
        name="fill3",
        out_shape=[sh((8, 128), F32), sh(table_g.shape, F32)],
        in_specs=[VMEM_SPEC, ANY_SPEC, HBM_SPEC],
        out_specs=[VMEM_SPEC, HBM_SPEC],
        input_output_aliases={2: 1},
        scratch_shapes=[DMA(())],
        compiler_params=pltpu.CompilerParams(vmem_limit_bytes=4 * MIB),
        cost_estimate=pl.CostEstimate(flops=4_000_000_000, bytes_accessed=16 * MIB, transcendentals=0),
    )(zero, order, table_g)


def dx_all_kernel(dx, dx_far, order, dx_out, dx_r, sems):
    me = lax.axis_index("tp")
    rows = dx.shape[0]
    remote = swap_with_sibling()
    block = lambda m: pl.ds(pl.multiple_of((me ^ m) * rows, rows), rows)
    copies = [remote(src, dx_r.at[pl.ds(k * rows, rows)], sems, k) for k, src in enumerate((dx, dx_far))]
    for c in copies:
        c.start()
    dx_out[block(0), :] = dx[...]
    dx_out[block(2), :] = dx_far[...]
    for k, c in enumerate(copies):
        c.wait()
        dx_out[block(1 + 2 * k), :] = dx_r[pl.ds(k * rows, rows), :]


def dx_all(dx, dx_far, order):
    rows, width = dx.shape
    return pl.pallas_call(
        dx_all_kernel,
        name="dx_all",
        out_shape=sh((4 * rows, width), BF),
        in_specs=[VMEM_SPEC] * 2 + [ANY_SPEC],
        out_specs=VMEM_SPEC,
        scratch_shapes=[VMEM((2 * rows, width), BF), DMA((2, 2))],
        compiler_params=pltpu.CompilerParams(collective_id=3, has_side_effects=True, vmem_limit_bytes=4 * MIB),
        cost_estimate=pl.CostEstimate(flops=2_000_000_000, bytes_accessed=MIB, transcendentals=0),
    )(dx, dx_far, order)


def put_kernel(puts, same, dx, table_in, table_g, token, puts_s, total, s_in, s_row):
    tokens = dx.shape[0]
    load = pltpu.make_async_copy(puts, puts_s, s_in)
    load.start()
    total[...] = mm(same[...], dx[...], 1, 0)
    token[...] = jnp.zeros_like(token)
    load.wait()
    count = puts_s[tokens]

    def put(i):
        word = puts_s[i]
        pltpu.make_async_copy(total.at[pl.ds(word >> 16, 1)], table_g.at[pl.ds(word & 0xFFFF, 1)], s_row).start()

    def put_four(i, carry):
        for k in range(4):
            put(i * 4 + k)
        return carry

    def put_one(i, carry):
        put(i)
        return carry

    lax.fori_loop(0, count >> 2, put_four, 0)
    lax.fori_loop((count >> 2) * 4, count, put_one, 0)

    def put_wait(size):
        def body(i, carry):
            pltpu.make_async_copy(total.at[pl.ds(0, size)], table_g.at[pl.ds(0, size)], s_row).wait()
            return carry

        return body

    lax.fori_loop(0, count >> 3, put_wait(8), 0)
    lax.fori_loop(0, count & 7, put_wait(1), 0)


def put_rows(puts, same, dx, table_g):
    return pl.pallas_call(
        put_kernel,
        name="put_rows",
        out_shape=[sh(table_g.shape, F32), sh((8, 128), F32)],
        in_specs=[ANY_SPEC, VMEM_SPEC, VMEM_SPEC, HBM_SPEC],
        out_specs=[HBM_SPEC, VMEM_SPEC],
        input_output_aliases={3: 0},
        scratch_shapes=[pltpu.SMEM(puts.shape, I32), VMEM(dx.shape, F32), DMA(()), DMA(())],
        compiler_params=pltpu.CompilerParams(vmem_limit_bytes=4 * MIB),
        cost_estimate=pl.CostEstimate(flops=3_000_000_000, bytes_accessed=2 * MIB, transcendentals=0),
    )(puts, same, dx, table_g)


def finish_kernel(x, y, y_in0, y_in1, order, out):
    part = y_in0.shape[0]
    for k, y_in in enumerate((y_in0, y_in1)):
        at = pl.ds(k * part, part)
        out[at, :] = (x[at, :].astype(F32) + (y[at, :] + y_in[...])).astype(BF)


def finish(x, y, y_in0, y_in1, order):
    return pl.pallas_call(
        finish_kernel,
        name="finish",
        out_shape=sh(y.shape, BF),
        in_specs=[VMEM_SPEC] * 4 + [ANY_SPEC],
        out_specs=VMEM_SPEC,
        compiler_params=pltpu.CompilerParams(vmem_limit_bytes=4 * MIB),
        cost_estimate=pl.CostEstimate(flops=1_000_000_000, bytes_accessed=MIB, transcendentals=0),
    )(x, y, y_in0, y_in1, order)


def solution(mesh):
    tp = mesh.shape["tp"]
    far_pairs = [(i, i ^ 2) for i in range(tp)]

    def far_permute(x):
        return lax.ppermute(x, "tp", far_pairs)

    def shard_step(ids, table, gain, w1, w2, d_out):
        part, rows_mine, same, zero, d_table = lookup(ids, table)
        send = pair(part, in_hbm(d_out))
        got = lax.ppermute(send, "tp", far_pairs)
        puts, token, d_table = fill1(rows_mine, zero, send, d_table)
        x_f, d_full = share(send, got, token)
        n, h, du, dn_p, d_table = mlp(x_f, d_full, w1, w2, gain, zero, d_table)
        dn_own, dn_far, y_p = sums(dn_p, du, h, w1, w2)
        g2 = far_permute(dn_far)
        y_own, y_far0, y_far1 = ysum(y_p, dn_own)
        y_in0 = lax.ppermute(y_far0, "tp", far_pairs)
        token, d_w1, d_w2, d_table = grads(n, h, du, d_full, zero, y_own, d_table)
        dx = dx_rows(dn_own, g2, x_f, d_out, gain, token)
        dx_far = far_permute(dx)
        dx, y_far1 = lax.optimization_barrier((dx, y_far1))
        y_in1 = far_permute(y_far1)
        token, d_table = fill3(zero, dx, d_table)
        dx_full = dx_all(dx, dx_far, token)
        d_table, done = put_rows(puts, same, dx_full, d_table)
        out = finish(x_f, y_own, y_in0, y_in1, done)
        return out, d_table, d_w1, d_w2

    return jax.shard_map(
        shard_step,
        mesh=mesh,
        in_specs=(P("dp"), P("tp", None), P(None), P(None, "tp"), P("tp", None), P(("dp", "tp"), None)),
        out_specs=(P(("dp", "tp"), None), P(("dp", "tp"), None), P("dp", "tp"), P(("dp", "tp"), None)),
        check_vma=False,
    )
```

```python
import jax
import jax.numpy as jnp
from jax import lax
from jax.experimental import pallas as pl
from jax.experimental.pallas import tpu as pltpu
from jax.sharding import PartitionSpec as P

EPS = 1e-6
BF = jnp.bfloat16
F32 = jnp.float32
I32 = jnp.int32
GELU_C = 0.7978845608028654
GELU_A = 0.044715
VMEM = pltpu.VMEM
SMEM_SPEC = pl.BlockSpec(memory_space=pltpu.SMEM)
ANY_SPEC = pl.BlockSpec(memory_space=pl.ANY)
HBM_SPEC = pl.BlockSpec(memory_space=pltpu.HBM)
VMEM_SPEC = pl.BlockSpec(memory_space=VMEM)
DMA = pltpu.SemaphoreType.DMA
TILE = 256
ZERO_ROWS = 96
FILL_AT = (0, 12, 92, 103, 117, 131)
MIB = 1 << 20
LOOKUP_VMEM = 48 * MIB
PAIR_VMEM = 8 * MIB


def mm(a, b, ca, cb):
    return lax.dot_general(a, b, (((ca,), (cb,)), ((), ())), preferred_element_type=F32)


def in_hbm(x):
    return pltpu.with_memory_space_constraint(x, pltpu.HBM)


def sh(shape, dtype):
    return jax.ShapeDtypeStruct(shape, dtype)


def fill_copy(zero, table_g, sem, i):
    return pltpu.make_async_copy(zero, table_g.at[pl.ds(pl.multiple_of(i * ZERO_ROWS, ZERO_ROWS), ZERO_ROWS)], sem)


def fill_start(zero, table_g, sem, part):
    def body(i, carry):
        fill_copy(zero, table_g, sem, i).start()
        return carry

    lax.fori_loop(FILL_AT[part], FILL_AT[part + 1], body, 0)


def fill_wait(zero, table_g, sem, part):
    def body(i, carry):
        fill_copy(zero, table_g, sem, i).wait()
        return carry

    lax.fori_loop(FILL_AT[part], FILL_AT[part + 1], body, 0)


def swap_with_sibling():
    sib = lax.axis_index("tp") ^ 1
    barrier = pltpu.get_barrier_semaphore()
    pl.semaphore_signal(barrier, inc=1, device_id={"tp": sib}, device_id_type=pl.DeviceIdType.MESH)
    pl.semaphore_wait(barrier, 1)

    def remote(src, dst, sems, i):
        return pltpu.make_async_remote_copy(
            src_ref=src, dst_ref=dst, send_sem=sems.at[0, i], recv_sem=sems.at[1, i],
            device_id={"tp": sib}, device_id_type=pl.DeviceIdType.MESH)

    return remote


def lookup_kernel(ids, ids_row, table, part, rows_mine, same, zero, table_g, ids_s, ids_v, pairs, sems, s_zero, s_ids):
    tokens, vocab = part.shape[0], table.shape[0]
    base = lax.axis_index("tp") * vocab
    group = 64
    groups = tokens // group
    loads = [pltpu.make_async_copy(ids, ids_s, s_ids.at[0]), pltpu.make_async_copy(ids_row, ids_v, s_ids.at[1])]
    for c in loads:
        c.start()
    zero[...] = jnp.zeros_like(zero)
    fill_start(zero, table_g, s_zero, 0)
    loads[0].wait()

    def fetch(k, carry):
        for i in range(group):
            token = k * group + i
            lid = ids_s[token] - base
            owned = (lid >= 0) & (lid < vocab)
            row = jnp.where(owned, lid & -2, 2 * token)
            pltpu.make_async_copy(table.at[pl.ds(pl.multiple_of(row, 2), 2)], pairs.at[k, pl.ds(2 * i, 2)], sems.at[k]).start()
        return carry

    lax.fori_loop(0, groups, fetch, 0)
    loads[1].wait()
    row = jnp.broadcast_to(ids_v[...].astype(F32), (tokens, tokens))
    col = row.T
    equal = row == col
    same[...] = jnp.where(equal, 1.0, 0.0).astype(BF)
    earlier = lax.broadcasted_iota(I32, (tokens, tokens), 0) < lax.broadcasted_iota(I32, (tokens, tokens), 1)
    repeat = jnp.max(jnp.where(equal & earlier, 1, 0), axis=0, keepdims=True)
    mine = ids_v[...] - base
    rows_mine[...] = jnp.where((mine >= 0) & (mine < vocab) & (repeat == 0), mine, -1)
    lid = col.astype(I32) - base
    lane = lax.broadcasted_iota(I32, (group, 2 * group), 1)
    first = lax.broadcasted_iota(I32, (group, 2 * group), 0) * 2
    for k in range(groups):
        at = lid[k * group:(k + 1) * group, :2 * group]
        owned = (at >= 0) & (at < vocab)
        pick = jnp.where(owned & (lane == first + (at & 1)), 1.0, 0.0).astype(BF)
        pltpu.make_async_copy(table.at[pl.ds(0, group * 2)], pairs.at[k], sems.at[k]).wait()
        part[pl.ds(k * group, group), :] = mm(pick, pairs[k], 1, 0).astype(BF)
    fill_wait(zero, table_g, s_zero, 0)


def lookup(ids, table):
    tokens, (vocab, width) = ids.shape[0], table.shape
    return pl.pallas_call(
        lookup_kernel,
        name="lookup",
        out_shape=[sh((tokens, width), BF), sh((1, tokens), I32), sh((tokens, tokens), BF), sh((ZERO_ROWS, width), F32), sh((vocab, width), F32)],
        in_specs=[HBM_SPEC] * 3,
        out_specs=[VMEM_SPEC] * 4 + [HBM_SPEC],
        scratch_shapes=[pltpu.SMEM((tokens,), I32), VMEM((1, tokens), I32), VMEM((4, tokens // 2, width), BF), DMA((4,)), DMA(()), DMA((2,))],
        compiler_params=pltpu.CompilerParams(vmem_limit_bytes=LOOKUP_VMEM),
        cost_estimate=pl.CostEstimate(flops=5_000_000_000, bytes_accessed=10 * MIB, transcendentals=0),
    )(in_hbm(ids), in_hbm(ids.reshape(1, tokens)), in_hbm(table))


def pair_kernel(part, d_out, w1, send, w1_v, part_r, sems, s_in):
    me = lax.axis_index("tp")
    rows = d_out.shape[0]
    blocks = (me, me ^ 2, me ^ 1, me ^ 3)
    loads = [pltpu.make_async_copy(d_out, send.at[pl.ds(2 * rows, rows)], s_in.at[0]), pltpu.make_async_copy(w1, w1_v, s_in.at[1])]
    for c in loads:
        c.start()
    remote = swap_with_sibling()
    block = lambda k: pl.ds(pl.multiple_of(blocks[k] * rows, rows), rows)
    copies = [remote(part.at[block(2 + k)], part_r.at[pl.ds(k * rows, rows)], sems, k) for k in range(2)]
    for c in copies:
        c.start()
    for k in range(2):
        copies[k].wait()
        at = pl.ds(k * rows, rows)
        send[at, :] = part[block(k), :] + part_r[at, :]
    for c in loads:
        c.wait()


def pair(part, d_out, w1):
    rows, width = d_out.shape
    return pl.pallas_call(
        pair_kernel,
        name="pair",
        out_shape=[sh((3 * rows, width), BF), sh(w1.shape, BF)],
        in_specs=[VMEM_SPEC, HBM_SPEC, HBM_SPEC],
        out_specs=[VMEM_SPEC] * 2,
        scratch_shapes=[VMEM((2 * rows, width), BF), DMA((2, 2)), DMA((2,))],
        compiler_params=pltpu.CompilerParams(collective_id=0, has_side_effects=True, vmem_limit_bytes=PAIR_VMEM),
        cost_estimate=pl.CostEstimate(flops=3_000_000_000, bytes_accessed=MIB, transcendentals=0),
    )(part, in_hbm(d_out), in_hbm(w1))


def fill1_kernel(rows_mine, zero, order, table_in, puts, token, table_g, mine_s, puts_s, s_zero, s_list):
    load = pltpu.make_async_copy(rows_mine, mine_s, s_list)
    load.start()
    fill_start(zero, table_g, s_zero, 1)
    tokens = rows_mine.shape[1]
    token[...] = jnp.zeros_like(token)
    load.wait()

    def body(i, count):
        lid = mine_s[0, i]
        puts_s[count] = lid | (i << 16)
        return count + (lid >= 0).astype(I32)

    puts_s[tokens] = lax.fori_loop(0, tokens, body, 0, unroll=8)
    store = pltpu.make_async_copy(puts_s, puts, s_list)
    store.start()
    store.wait()
    fill_wait(zero, table_g, s_zero, 1)


def fill1(rows_mine, zero, order, table_g):
    tokens = rows_mine.shape[1]
    return pl.pallas_call(
        fill1_kernel,
        name="fill1",
        out_shape=[sh((2 * tokens,), I32), sh((8, 128), F32), sh(table_g.shape, F32)],
        in_specs=[ANY_SPEC, VMEM_SPEC, ANY_SPEC, HBM_SPEC],
        out_specs=[ANY_SPEC, VMEM_SPEC, HBM_SPEC],
        input_output_aliases={3: 2},
        scratch_shapes=[pltpu.SMEM((1, tokens), I32), pltpu.SMEM((2 * tokens,), I32), DMA(()), DMA(())],
        compiler_params=pltpu.CompilerParams(vmem_limit_bytes=8 * MIB),
        cost_estimate=pl.CostEstimate(flops=9_000_000_000, bytes_accessed=20 * MIB, transcendentals=0),
    )(rows_mine, zero, order, table_g)


def share_kernel(send, got, w2, order, x_f, d_full, w2_v, x_r, d_r, sems, s_in):
    rows = send.shape[0] // 3
    half = 2 * rows
    load = pltpu.make_async_copy(w2, w2_v, s_in)
    load.start()
    remote = swap_with_sibling()
    copies = []
    for k in range(2):
        at, other = pl.ds(k * rows, rows), pl.ds((1 - k) * rows, rows)
        x_f[at, :] = send[at, :] + got[other, :]
        copies.append(remote(x_f.at[at], x_r.at[at], sems, k))
        copies[-1].start()
    for k, src in enumerate((send, got)):
        copies.append(remote(src.at[pl.ds(half, rows)], d_r.at[pl.ds(k * rows, rows)], sems, 2 + k))
        copies[-1].start()
        d_full[pl.ds(k * rows, rows), :] = src[pl.ds(half, rows), :]
    for k in range(2):
        copies[k].wait()
        x_f[pl.ds(half + k * rows, rows), :] = x_r[pl.ds(k * rows, rows), :]
    for k in range(2):
        copies[2 + k].wait()
        d_full[pl.ds(half + k * rows, rows), :] = d_r[pl.ds(k * rows, rows), :]
    load.wait()


def share(send, got, w2, order):
    rows, width = send.shape[0] // 3, send.shape[1]
    return pl.pallas_call(
        share_kernel,
        name="share",
        out_shape=[sh((4 * rows, width), BF)] * 2 + [sh(w2.shape, BF)],
        in_specs=[VMEM_SPEC] * 2 + [HBM_SPEC, ANY_SPEC],
        out_specs=[VMEM_SPEC] * 3,
        scratch_shapes=[VMEM((2 * rows, width), BF), VMEM((2 * rows, width), BF), DMA((2, 4)), DMA(())],
        compiler_params=pltpu.CompilerParams(collective_id=1, has_side_effects=True, vmem_limit_bytes=8 * MIB),
        cost_estimate=pl.CostEstimate(flops=3_000_000_000, bytes_accessed=MIB, transcendentals=0),
    )(send, got, in_hbm(w2), order)


def mlp_kernel(x_f, d_full, w1, w2, gain, zero, table_in, n, h, du, dn_p, table_g, s_zero):
    fill_start(zero, table_g, s_zero, 2)
    tokens, width = n.shape
    hid = h.shape[1]
    gain_f = gain[...].astype(F32).reshape(1, width)
    for j in range(tokens // 32):
        at = pl.ds(j * 32, 32)
        x = x_f[at, :].astype(F32)
        r = lax.rsqrt(jnp.mean(x * x, axis=-1, keepdims=True) + EPS)
        n[at, :] = (x * r * gain_f).astype(BF)
    for j in range(hid // TILE):
        cols = pl.ds(j * TILE, TILE)
        g = mm(d_full[...], w2[cols, :], 1, 1).astype(BF).astype(F32)
        u = mm(n[...], w1[:, cols], 1, 0).astype(BF).astype(F32)
        t = jnp.tanh(GELU_C * (u + GELU_A * (u * u * u)))
        cdf = 0.5 * (1.0 + t)
        h[:, cols] = (u * cdf).astype(BF)
        du[:, cols] = (g * (cdf + u * (0.5 * (1.0 - t * t)) * (GELU_C * (1.0 + 3.0 * GELU_A * (u * u))))).astype(BF)
    half = tokens // 2
    for j in range(width // TILE):
        cols = pl.ds(j * TILE, TILE)
        dn_p[:, cols] = mm(du[pl.ds(half, half), :], w1[cols, :], 1, 1)
    fill_wait(zero, table_g, s_zero, 2)


def mlp(x_f, d_full, w1, w2, gain, zero, table_g):
    tokens, width = x_f.shape
    hid = w1.shape[1]
    return pl.pallas_call(
        mlp_kernel,
        name="mlp",
        out_shape=[sh((tokens, width), BF), sh((tokens, hid), BF), sh((tokens, hid), BF), sh((tokens // 2, width), F32),
                   sh(table_g.shape, F32)],
        in_specs=[VMEM_SPEC] * 6 + [HBM_SPEC],
        out_specs=[VMEM_SPEC] * 4 + [HBM_SPEC],
        input_output_aliases={6: 4},
        scratch_shapes=[DMA(())],
        compiler_params=pltpu.CompilerParams(vmem_limit_bytes=16 * MIB),
        cost_estimate=pl.CostEstimate(flops=6_000_000_000, bytes_accessed=4 * MIB, transcendentals=0),
    )(x_f, d_full, w1, w2, gain, zero, table_g)


def sums_kernel(dn_p, du, h, w1, w2, dn_own, dn_far, y_p, dn_r, dn_m, sems):
    rows, width = dn_own.shape
    half = 2 * rows
    remote = swap_with_sibling()
    copies = [remote(dn_p.at[pl.ds(k * rows, rows)], dn_r.at[pl.ds(k * rows, rows)], sems, k) for k in (1, 0)]
    for c in copies:
        c.start()
    for j in range(width // TILE):
        cols = pl.ds(j * TILE, TILE)
        dn_m[:, cols] = mm(du[pl.ds(0, half), :], w1[cols, :], 1, 1)
    for j in range(width // TILE):
        cols = pl.ds(j * TILE, TILE)
        y_p[:, cols] = mm(h[...], w2[:, cols], 1, 0)
    for c, out, k in zip(copies, (dn_far, dn_own), (1, 0)):
        c.wait()
        at = pl.ds(k * rows, rows)
        out[...] = dn_m[at, :] + dn_r[at, :]


def sums(dn_p, du, h, w1, w2):
    half, width = dn_p.shape
    rows = half // 2
    return pl.pallas_call(
        sums_kernel,
        name="sums",
        out_shape=[sh((rows, width), F32), sh((rows, width), F32), sh((2 * half, width), F32)],
        in_specs=[VMEM_SPEC] * 5,
        out_specs=[VMEM_SPEC] * 3,
        scratch_shapes=[VMEM((half, width), F32), VMEM((half, width), F32), DMA((2, 2))],
        compiler_params=pltpu.CompilerParams(collective_id=2, has_side_effects=True, vmem_limit_bytes=16 * MIB),
        cost_estimate=pl.CostEstimate(flops=4_000_000_000, bytes_accessed=4 * MIB, transcendentals=0),
    )(dn_p, du, h, w1, w2)


def ysum_kernel(y_p, order, y_own, y_far0, y_far1, y_r, sems):
    rows, _ = y_own.shape
    half, part = 2 * rows, rows // 2
    remote = swap_with_sibling()
    places = ((rows, y_far0), (rows + part, y_far1), (0, y_own))
    copies = [remote(y_p.at[pl.ds(half + at, out.shape[0])], y_r.at[pl.ds(at, out.shape[0])], sems, k) for k, (at, out) in enumerate(places)]
    for c in copies:
        c.start()
    for c, (at, out) in zip(copies, places):
        c.wait()
        rows_at = pl.ds(at, out.shape[0])
        out[...] = y_p[rows_at, :] + y_r[rows_at, :]


def ysum(y_p, order):
    tokens, width = y_p.shape
    rows = tokens // 4
    return pl.pallas_call(
        ysum_kernel,
        name="ysum",
        out_shape=[sh((rows, width), F32), sh((rows // 2, width), F32), sh((rows // 2, width), F32)],
        in_specs=[VMEM_SPEC, ANY_SPEC],
        out_specs=[VMEM_SPEC] * 3,
        scratch_shapes=[VMEM((2 * rows, width), F32), DMA((2, 3))],
        compiler_params=pltpu.CompilerParams(collective_id=4, has_side_effects=True, vmem_limit_bytes=8 * MIB),
        cost_estimate=pl.CostEstimate(flops=3_000_000_000, bytes_accessed=4 * MIB, transcendentals=0),
    )(y_p, order)


def grads_kernel(n, h, du, d_full, zero, order, table_in, token, dw1, dw2, table_g, dw1_v, dw2_v, s_zero, s_w):
    fill_start(zero, table_g, s_zero, 3)
    token[...] = jnp.zeros_like(token)
    width, hid = dw1.shape
    n_t = n[...].T
    for j in range(width // TILE):
        at = slice(j * TILE, (j + 1) * TILE)
        dw1_v[at, :] = mm(n_t[at, :], du[...], 1, 0)
        pltpu.make_async_copy(dw1_v.at[pl.ds(j * TILE, TILE)], dw1.at[pl.ds(j * TILE, TILE)], s_w).start()
    h_t = h[...].T
    for j in range(hid // TILE):
        at = slice(j * TILE, (j + 1) * TILE)
        dw2_v[at, :] = mm(h_t[at, :], d_full[...], 1, 0)
        pltpu.make_async_copy(dw2_v.at[pl.ds(j * TILE, TILE)], dw2.at[pl.ds(j * TILE, TILE)], s_w).start()
    pltpu.make_async_copy(dw1_v, dw1, s_w).wait()
    pltpu.make_async_copy(dw2_v, dw2, s_w).wait()
    fill_wait(zero, table_g, s_zero, 3)


def grads(n, h, du, d_full, zero, order, table_g):
    _, width = n.shape
    hid = h.shape[1]
    return pl.pallas_call(
        grads_kernel,
        name="grads",
        out_shape=[sh((8, 128), F32), sh((width, hid), F32), sh((hid, width), F32), sh(table_g.shape, F32)],
        in_specs=[VMEM_SPEC] * 5 + [ANY_SPEC, HBM_SPEC],
        out_specs=[VMEM_SPEC, HBM_SPEC, HBM_SPEC, HBM_SPEC],
        input_output_aliases={6: 3},
        scratch_shapes=[VMEM((width, hid), F32), VMEM((hid, width), F32), DMA(()), DMA(())],
        compiler_params=pltpu.CompilerParams(vmem_limit_bytes=24 * MIB),
        cost_estimate=pl.CostEstimate(flops=8_000_000_000, bytes_accessed=20 * MIB, transcendentals=0),
    )(n, h, du, d_full, zero, order, table_g)


def dx_kernel(dn_own, g2, x_own, d_own, gain, order, dx):
    gain_f = gain[...].astype(F32).reshape(1, dx.shape[1])
    for j in range(dx.shape[0] // 16):
        at = pl.ds(j * 16, 16)
        a = (dn_own[at, :] + g2[at, :]) * gain_f
        x = x_own[at, :].astype(F32)
        r = lax.rsqrt(jnp.mean(x * x, axis=-1, keepdims=True) + EPS)
        proj = jnp.mean(a * x, axis=-1, keepdims=True)
        dx[at, :] = (d_own[at, :].astype(F32) + r * (a - x * r * r * proj)).astype(BF)


def dx_rows(dn_own, g2, x_own, d_own, gain, order):
    return pl.pallas_call(
        dx_kernel,
        name="dx_rows",
        out_shape=sh(d_own.shape, BF),
        in_specs=[VMEM_SPEC] * 5 + [ANY_SPEC],
        out_specs=VMEM_SPEC,
        compiler_params=pltpu.CompilerParams(vmem_limit_bytes=4 * MIB),
        cost_estimate=pl.CostEstimate(flops=1_000_000_000, bytes_accessed=MIB, transcendentals=0),
    )(dn_own, g2, x_own, d_own, gain, order)


def fill3_kernel(zero, order, table_in, token, table_g, s_zero):
    fill_start(zero, table_g, s_zero, 4)
    token[...] = jnp.zeros_like(token)
    fill_wait(zero, table_g, s_zero, 4)


def fill3(zero, order, table_g):
    return pl.pallas_call(
        fill3_kernel,
        name="fill3",
        out_shape=[sh((8, 128), F32), sh(table_g.shape, F32)],
        in_specs=[VMEM_SPEC, ANY_SPEC, HBM_SPEC],
        out_specs=[VMEM_SPEC, HBM_SPEC],
        input_output_aliases={2: 1},
        scratch_shapes=[DMA(())],
        compiler_params=pltpu.CompilerParams(vmem_limit_bytes=4 * MIB),
        cost_estimate=pl.CostEstimate(flops=4_000_000_000, bytes_accessed=16 * MIB, transcendentals=0),
    )(zero, order, table_g)


def dx_all_kernel(dx, dx_far, order, dx_out, dx_r, sems):
    me = lax.axis_index("tp")
    rows = dx.shape[0]
    remote = swap_with_sibling()
    block = lambda m: pl.ds(pl.multiple_of((me ^ m) * rows, rows), rows)
    copies = [remote(src, dx_r.at[pl.ds(k * rows, rows)], sems, k) for k, src in enumerate((dx, dx_far))]
    for c in copies:
        c.start()
    dx_out[block(0), :] = dx[...]
    dx_out[block(2), :] = dx_far[...]
    for k, c in enumerate(copies):
        c.wait()
        dx_out[block(1 + 2 * k), :] = dx_r[pl.ds(k * rows, rows), :]


def dx_all(dx, dx_far, order):
    rows, width = dx.shape
    return pl.pallas_call(
        dx_all_kernel,
        name="dx_all",
        out_shape=sh((4 * rows, width), BF),
        in_specs=[VMEM_SPEC] * 2 + [ANY_SPEC],
        out_specs=VMEM_SPEC,
        scratch_shapes=[VMEM((2 * rows, width), BF), DMA((2, 2))],
        compiler_params=pltpu.CompilerParams(collective_id=3, has_side_effects=True, vmem_limit_bytes=4 * MIB),
        cost_estimate=pl.CostEstimate(flops=2_000_000_000, bytes_accessed=MIB, transcendentals=0),
    )(dx, dx_far, order)


def put_kernel(puts, same, dx, table_in, table_g, token, puts_s, total, s_in, s_row):
    tokens = dx.shape[0]
    load = pltpu.make_async_copy(puts, puts_s, s_in)
    load.start()
    total[...] = mm(same[...], dx[...], 1, 0)
    token[...] = jnp.zeros_like(token)
    load.wait()
    count = puts_s[tokens]

    def put(i):
        word = puts_s[i]
        pltpu.make_async_copy(total.at[pl.ds(word >> 16, 1)], table_g.at[pl.ds(word & 0xFFFF, 1)], s_row).start()

    def put_four(i, carry):
        for k in range(4):
            put(i * 4 + k)
        return carry

    def put_one(i, carry):
        put(i)
        return carry

    lax.fori_loop(0, count >> 2, put_four, 0)
    lax.fori_loop((count >> 2) * 4, count, put_one, 0)

    def put_wait(size):
        def body(i, carry):
            pltpu.make_async_copy(total.at[pl.ds(0, size)], table_g.at[pl.ds(0, size)], s_row).wait()
            return carry

        return body

    lax.fori_loop(0, count >> 3, put_wait(8), 0)
    lax.fori_loop(0, count & 7, put_wait(1), 0)


def put_rows(puts, same, dx, table_g):
    return pl.pallas_call(
        put_kernel,
        name="put_rows",
        out_shape=[sh(table_g.shape, F32), sh((8, 128), F32)],
        in_specs=[ANY_SPEC, VMEM_SPEC, VMEM_SPEC, HBM_SPEC],
        out_specs=[HBM_SPEC, VMEM_SPEC],
        input_output_aliases={3: 0},
        scratch_shapes=[pltpu.SMEM(puts.shape, I32), VMEM(dx.shape, F32), DMA(()), DMA(())],
        compiler_params=pltpu.CompilerParams(vmem_limit_bytes=4 * MIB),
        cost_estimate=pl.CostEstimate(flops=3_000_000_000, bytes_accessed=2 * MIB, transcendentals=0),
    )(puts, same, dx, table_g)


def finish_kernel(x, y, y_in0, y_in1, order, out):
    part = y_in0.shape[0]
    for k, y_in in enumerate((y_in0, y_in1)):
        at = pl.ds(k * part, part)
        out[at, :] = (x[at, :].astype(F32) + (y[at, :] + y_in[...])).astype(BF)


def finish(x, y, y_in0, y_in1, order):
    return pl.pallas_call(
        finish_kernel,
        name="finish",
        out_shape=sh(y.shape, BF),
        in_specs=[VMEM_SPEC] * 4 + [ANY_SPEC],
        out_specs=VMEM_SPEC,
        compiler_params=pltpu.CompilerParams(vmem_limit_bytes=4 * MIB),
        cost_estimate=pl.CostEstimate(flops=1_000_000_000, bytes_accessed=MIB, transcendentals=0),
    )(x, y, y_in0, y_in1, order)


def solution(mesh):
    tp = mesh.shape["tp"]
    far_pairs = [(i, i ^ 2) for i in range(tp)]

    def far_permute(x):
        return lax.ppermute(x, "tp", far_pairs)

    def shard_step(ids, table, gain, w1, w2, d_out):
        part, rows_mine, same, zero, d_table = lookup(ids, table)
        send, w1 = pair(part, d_out, w1)
        got = lax.ppermute(send, "tp", far_pairs)
        puts, token, d_table = fill1(rows_mine, zero, send, d_table)
        x_f, d_full, w2 = share(send, got, w2, token)
        n, h, du, dn_p, d_table = mlp(x_f, d_full, w1, w2, gain, zero, d_table)
        dn_own, dn_far, y_p = sums(dn_p, du, h, w1, w2)
        g2 = far_permute(dn_far)
        y_own, y_far0, y_far1 = ysum(y_p, dn_own)
        token, d_w1, d_w2, d_table = grads(n, h, du, d_full, zero, y_own, d_table)
        token, y_far0 = lax.optimization_barrier((token, y_far0))
        y_in0 = lax.ppermute(y_far0, "tp", far_pairs)
        dx = dx_rows(dn_own, g2, x_f, d_out, gain, token)
        dx_far = far_permute(dx)
        dx, y_far1 = lax.optimization_barrier((dx, y_far1))
        y_in1 = far_permute(y_far1)
        token, d_table = fill3(zero, dx, d_table)
        dx_full = dx_all(dx, dx_far, token)
        d_table, done = put_rows(puts, same, dx_full, d_table)
        out = finish(x_f, y_own, y_in0, y_in1, done)
        return out, d_table, d_w1, d_w2

    return jax.shard_map(
        shard_step,
        mesh=mesh,
        in_specs=(P("dp"), P("tp", None), P(None), P(None, "tp"), P("tp", None), P(("dp", "tp"), None)),
        out_specs=(P(("dp", "tp"), None), P(("dp", "tp"), None), P("dp", "tp"), P(("dp", "tp"), None)),
        check_vma=False,
    )
```

```python
import jax
import jax.numpy as jnp
from jax import lax
from jax.experimental import pallas as pl
from jax.experimental.pallas import tpu as pltpu
from jax.sharding import PartitionSpec as P

EPS = 1e-6
BF = jnp.bfloat16
F32 = jnp.float32
I32 = jnp.int32
GELU_C = 0.7978845608028654
GELU_A = 0.044715
VMEM = pltpu.VMEM
SMEM_SPEC = pl.BlockSpec(memory_space=pltpu.SMEM)
ANY_SPEC = pl.BlockSpec(memory_space=pl.ANY)
HBM_SPEC = pl.BlockSpec(memory_space=pltpu.HBM)
VMEM_SPEC = pl.BlockSpec(memory_space=VMEM)
DMA = pltpu.SemaphoreType.DMA
TILE = 256
ZERO_ROWS = 96
FILL_AT = (0, 14, 91, 96, 106, 131)
Y_FIRST = 16
MIB = 1 << 20
LOOKUP_VMEM = 48 * MIB
PAIR_VMEM = 8 * MIB


def mm(a, b, ca, cb):
    return lax.dot_general(a, b, (((ca,), (cb,)), ((), ())), preferred_element_type=F32)


def in_hbm(x):
    return pltpu.with_memory_space_constraint(x, pltpu.HBM)


def sh(shape, dtype):
    return jax.ShapeDtypeStruct(shape, dtype)


def fill_copy(zero, table_g, sem, i):
    return pltpu.make_async_copy(zero, table_g.at[pl.ds(pl.multiple_of(i * ZERO_ROWS, ZERO_ROWS), ZERO_ROWS)], sem)


def fill_start(zero, table_g, sem, part):
    def body(i, carry):
        fill_copy(zero, table_g, sem, i).start()
        return carry

    lax.fori_loop(FILL_AT[part], FILL_AT[part + 1], body, 0)


def fill_wait(zero, table_g, sem, part):
    def body(i, carry):
        fill_copy(zero, table_g, sem, i).wait()
        return carry

    lax.fori_loop(FILL_AT[part], FILL_AT[part + 1], body, 0)


def swap_with_sibling():
    sib = lax.axis_index("tp") ^ 1
    barrier = pltpu.get_barrier_semaphore()
    pl.semaphore_signal(barrier, inc=1, device_id={"tp": sib}, device_id_type=pl.DeviceIdType.MESH)
    pl.semaphore_wait(barrier, 1)

    def remote(src, dst, sems, i):
        return pltpu.make_async_remote_copy(
            src_ref=src, dst_ref=dst, send_sem=sems.at[0, i], recv_sem=sems.at[1, i],
            device_id={"tp": sib}, device_id_type=pl.DeviceIdType.MESH)

    return remote


def lookup_kernel(ids, ids_row, table, part, rows_mine, same, zero, table_g, ids_s, ids_v, pairs, sems, s_zero, s_ids):
    tokens, vocab = part.shape[0], table.shape[0]
    base = lax.axis_index("tp") * vocab
    group = 64
    groups = tokens // group
    loads = [pltpu.make_async_copy(ids, ids_s, s_ids.at[0]), pltpu.make_async_copy(ids_row, ids_v, s_ids.at[1])]
    for c in loads:
        c.start()
    zero[...] = jnp.zeros_like(zero)
    fill_start(zero, table_g, s_zero, 0)
    loads[0].wait()

    def fetch(k, carry):
        for i in range(group):
            token = k * group + i
            lid = ids_s[token] - base
            owned = (lid >= 0) & (lid < vocab)
            row = jnp.where(owned, lid & -2, 2 * token)
            pltpu.make_async_copy(table.at[pl.ds(pl.multiple_of(row, 2), 2)], pairs.at[k, pl.ds(2 * i, 2)], sems.at[k]).start()
        return carry

    lax.fori_loop(0, groups, fetch, 0)
    loads[1].wait()
    row = jnp.broadcast_to(ids_v[...].astype(F32), (tokens, tokens))
    col = row.T
    equal = row == col
    same[...] = jnp.where(equal, 1.0, 0.0).astype(BF)
    earlier = lax.broadcasted_iota(I32, (tokens, tokens), 0) < lax.broadcasted_iota(I32, (tokens, tokens), 1)
    repeat = jnp.max(jnp.where(equal & earlier, 1, 0), axis=0, keepdims=True)
    mine = ids_v[...] - base
    rows_mine[...] = jnp.where((mine >= 0) & (mine < vocab) & (repeat == 0), mine, -1)
    lid = col.astype(I32) - base
    lane = lax.broadcasted_iota(I32, (group, 2 * group), 1)
    first = lax.broadcasted_iota(I32, (group, 2 * group), 0) * 2
    for k in range(groups):
        at = lid[k * group:(k + 1) * group, :2 * group]
        owned = (at >= 0) & (at < vocab)
        pick = jnp.where(owned & (lane == first + (at & 1)), 1.0, 0.0).astype(BF)
        pltpu.make_async_copy(table.at[pl.ds(0, group * 2)], pairs.at[k], sems.at[k]).wait()
        part[pl.ds(k * group, group), :] = mm(pick, pairs[k], 1, 0).astype(BF)
    fill_wait(zero, table_g, s_zero, 0)


def lookup(ids, table):
    tokens, (vocab, width) = ids.shape[0], table.shape
    return pl.pallas_call(
        lookup_kernel,
        name="lookup",
        out_shape=[sh((tokens, width), BF), sh((1, tokens), I32), sh((tokens, tokens), BF), sh((ZERO_ROWS, width), F32), sh((vocab, width), F32)],
        in_specs=[HBM_SPEC] * 3,
        out_specs=[VMEM_SPEC] * 4 + [HBM_SPEC],
        scratch_shapes=[pltpu.SMEM((tokens,), I32), VMEM((1, tokens), I32), VMEM((4, tokens // 2, width), BF), DMA((4,)), DMA(()), DMA((2,))],
        compiler_params=pltpu.CompilerParams(vmem_limit_bytes=LOOKUP_VMEM),
        cost_estimate=pl.CostEstimate(flops=5_000_000_000, bytes_accessed=10 * MIB, transcendentals=0),
    )(in_hbm(ids), in_hbm(ids.reshape(1, tokens)), in_hbm(table))


def pair_kernel(part, d_out, w1, send, w1_v, part_r, sems, s_in):
    me = lax.axis_index("tp")
    rows = d_out.shape[0]
    blocks = (me, me ^ 2, me ^ 1, me ^ 3)
    loads = [pltpu.make_async_copy(d_out, send.at[pl.ds(2 * rows, rows)], s_in.at[0]), pltpu.make_async_copy(w1, w1_v, s_in.at[1])]
    for c in loads:
        c.start()
    remote = swap_with_sibling()
    block = lambda k: pl.ds(pl.multiple_of(blocks[k] * rows, rows), rows)
    copies = [remote(part.at[block(2 + k)], part_r.at[pl.ds(k * rows, rows)], sems, k) for k in range(2)]
    for c in copies:
        c.start()
    for k in range(2):
        copies[k].wait()
        at = pl.ds(k * rows, rows)
        send[at, :] = part[block(k), :] + part_r[at, :]
    for c in loads:
        c.wait()


def pair(part, d_out, w1):
    rows, width = d_out.shape
    return pl.pallas_call(
        pair_kernel,
        name="pair",
        out_shape=[sh((3 * rows, width), BF), sh(w1.shape, BF)],
        in_specs=[VMEM_SPEC, HBM_SPEC, HBM_SPEC],
        out_specs=[VMEM_SPEC] * 2,
        scratch_shapes=[VMEM((2 * rows, width), BF), DMA((2, 2)), DMA((2,))],
        compiler_params=pltpu.CompilerParams(collective_id=0, has_side_effects=True, vmem_limit_bytes=PAIR_VMEM),
        cost_estimate=pl.CostEstimate(flops=3_000_000_000, bytes_accessed=MIB, transcendentals=0),
    )(part, in_hbm(d_out), in_hbm(w1))


def fill1_kernel(rows_mine, zero, w2, order, table_in, puts, w2_v, table_g, mine_s, puts_s, s_zero, s_list, s_w):
    load = pltpu.make_async_copy(rows_mine, mine_s, s_list)
    load.start()
    load_w = pltpu.make_async_copy(w2, w2_v, s_w)
    load_w.start()
    fill_start(zero, table_g, s_zero, 1)
    tokens = rows_mine.shape[1]
    load.wait()

    def body(i, count):
        lid = mine_s[0, i]
        puts_s[count] = lid | (i << 16)
        return count + (lid >= 0).astype(I32)

    puts_s[tokens] = lax.fori_loop(0, tokens, body, 0, unroll=8)
    store = pltpu.make_async_copy(puts_s, puts, s_list)
    store.start()
    store.wait()
    load_w.wait()
    fill_wait(zero, table_g, s_zero, 1)


def fill1(rows_mine, zero, w2, order, table_g):
    tokens = rows_mine.shape[1]
    return pl.pallas_call(
        fill1_kernel,
        name="fill1",
        out_shape=[sh((2 * tokens,), I32), sh(w2.shape, BF), sh(table_g.shape, F32)],
        in_specs=[ANY_SPEC, VMEM_SPEC, HBM_SPEC, ANY_SPEC, HBM_SPEC],
        out_specs=[ANY_SPEC, VMEM_SPEC, HBM_SPEC],
        input_output_aliases={4: 2},
        scratch_shapes=[pltpu.SMEM((1, tokens), I32), pltpu.SMEM((2 * tokens,), I32), DMA(()), DMA(()), DMA(())],
        compiler_params=pltpu.CompilerParams(vmem_limit_bytes=8 * MIB),
        cost_estimate=pl.CostEstimate(flops=9_000_000_000, bytes_accessed=20 * MIB, transcendentals=0),
    )(rows_mine, zero, in_hbm(w2), order, table_g)


def mlp_half(x, d, n, h, du, at, w1, w2, gain):
    first, count = at
    width, hid = n.shape[1], h.shape[1]
    gain_f = gain[...].astype(F32).reshape(1, width)
    for j in range(count // 32):
        rows = pl.ds(first + j * 32, 32)
        x_f = x[rows, :].astype(F32)
        r = lax.rsqrt(jnp.mean(x_f * x_f, axis=-1, keepdims=True) + EPS)
        n[rows, :] = (x_f * r * gain_f).astype(BF)
    rows = pl.ds(first, count)
    for j in range(hid // TILE):
        cols = pl.ds(j * TILE, TILE)
        g = mm(d[rows, :], w2[cols, :], 1, 1).astype(BF).astype(F32)
        u = mm(n[rows, :], w1[:, cols], 1, 0).astype(BF).astype(F32)
        t = jnp.tanh(GELU_C * (u + GELU_A * (u * u * u)))
        cdf = 0.5 * (1.0 + t)
        h[rows, cols] = (u * cdf).astype(BF)
        du[rows, cols] = (g * (cdf + u * (0.5 * (1.0 - t * t)) * (GELU_C * (1.0 + 3.0 * GELU_A * (u * u))))).astype(BF)


def share_kernel(send, got, w1, w2, gain, x_f, d_full, n_a, h_a, du_a, x_r, d_r, sems):
    rows = send.shape[0] // 3
    half = 2 * rows
    remote = swap_with_sibling()
    copies = []
    for k in range(2):
        at, other = pl.ds(k * rows, rows), pl.ds((1 - k) * rows, rows)
        x_f[at, :] = send[at, :] + got[other, :]
        copies.append(remote(x_f.at[at], x_r.at[at], sems, k))
        copies[-1].start()
    for k, src in enumerate((send, got)):
        copies.append(remote(src.at[pl.ds(half, rows)], d_r.at[pl.ds(k * rows, rows)], sems, 2 + k))
        copies[-1].start()
        d_full[pl.ds(k * rows, rows), :] = src[pl.ds(half, rows), :]
    mlp_half(x_f, d_full, n_a, h_a, du_a, (0, half), w1, w2, gain)
    for k in range(2):
        copies[k].wait()
        x_f[pl.ds(half + k * rows, rows), :] = x_r[pl.ds(k * rows, rows), :]
    for k in range(2):
        copies[2 + k].wait()
        d_full[pl.ds(half + k * rows, rows), :] = d_r[pl.ds(k * rows, rows), :]


def share(send, got, w1, w2, gain):
    rows, width = send.shape[0] // 3, send.shape[1]
    hid = w1.shape[1]
    return pl.pallas_call(
        share_kernel,
        name="share",
        out_shape=[sh((4 * rows, width), BF)] * 2 + [sh((2 * rows, width), BF)] + [sh((2 * rows, hid), BF)] * 2,
        in_specs=[VMEM_SPEC] * 5,
        out_specs=[VMEM_SPEC] * 5,
        scratch_shapes=[VMEM((2 * rows, width), BF), VMEM((2 * rows, width), BF), DMA((2, 4))],
        compiler_params=pltpu.CompilerParams(collective_id=1, has_side_effects=True, vmem_limit_bytes=16 * MIB),
        cost_estimate=pl.CostEstimate(flops=3_000_000_000, bytes_accessed=MIB, transcendentals=0),
    )(send, got, w1, w2, gain)


def mlp_kernel(x_f, d_full, n_a, h_a, du_a, w1, w2, gain, zero, table_in, n, h, du, dn_p, table_g, s_zero):
    fill_start(zero, table_g, s_zero, 2)
    tokens, width = n.shape
    half = tokens // 2
    for out, src in ((n, n_a), (h, h_a), (du, du_a)):
        out[pl.ds(0, half), :] = src[...]
    mlp_half(x_f, d_full, n, h, du, (half, half), w1, w2, gain)
    for j in range(width // TILE):
        cols = pl.ds(j * TILE, TILE)
        dn_p[:, cols] = mm(du[pl.ds(half, half), :], w1[cols, :], 1, 1)
    fill_wait(zero, table_g, s_zero, 2)


def mlp(x_f, d_full, n_a, h_a, du_a, w1, w2, gain, zero, table_g):
    tokens, width = x_f.shape
    hid = w1.shape[1]
    return pl.pallas_call(
        mlp_kernel,
        name="mlp",
        out_shape=[sh((tokens, width), BF), sh((tokens, hid), BF), sh((tokens, hid), BF), sh((tokens // 2, width), F32),
                   sh(table_g.shape, F32)],
        in_specs=[VMEM_SPEC] * 9 + [HBM_SPEC],
        out_specs=[VMEM_SPEC] * 4 + [HBM_SPEC],
        input_output_aliases={9: 4},
        scratch_shapes=[DMA(())],
        compiler_params=pltpu.CompilerParams(vmem_limit_bytes=16 * MIB),
        cost_estimate=pl.CostEstimate(flops=6_000_000_000, bytes_accessed=4 * MIB, transcendentals=0),
    )(x_f, d_full, n_a, h_a, du_a, w1, w2, gain, zero, table_g)


def sums_kernel(dn_p, du, h, w1, w2, dn_own, dn_far, y_p, dn_r, dn_m, sems):
    rows, width = dn_own.shape
    half = 2 * rows
    remote = swap_with_sibling()
    copies = [remote(dn_p.at[pl.ds(k * rows, rows)], dn_r.at[pl.ds(k * rows, rows)], sems, k) for k in (1, 0)]
    for c in copies:
        c.start()
    for j in range(width // TILE):
        cols = pl.ds(j * TILE, TILE)
        dn_m[:, cols] = mm(du[pl.ds(0, half), :], w1[cols, :], 1, 1)
    for j in range(width // TILE):
        cols = pl.ds(j * TILE, TILE)
        y_p[:, cols] = mm(h[...], w2[:, cols], 1, 0)
    for c, out, k in zip(copies, (dn_far, dn_own), (1, 0)):
        c.wait()
        at = pl.ds(k * rows, rows)
        out[...] = dn_m[at, :] + dn_r[at, :]


def sums(dn_p, du, h, w1, w2):
    half, width = dn_p.shape
    rows = half // 2
    return pl.pallas_call(
        sums_kernel,
        name="sums",
        out_shape=[sh((rows, width), F32), sh((rows, width), F32), sh((2 * half, width), F32)],
        in_specs=[VMEM_SPEC] * 5,
        out_specs=[VMEM_SPEC] * 3,
        scratch_shapes=[VMEM((half, width), F32), VMEM((half, width), F32), DMA((2, 2))],
        compiler_params=pltpu.CompilerParams(collective_id=2, has_side_effects=True, vmem_limit_bytes=16 * MIB),
        cost_estimate=pl.CostEstimate(flops=4_000_000_000, bytes_accessed=4 * MIB, transcendentals=0),
    )(dn_p, du, h, w1, w2)


def ysum_kernel(y_p, order, y_own, y_far0, y_far1, y_r, sems):
    rows, _ = y_own.shape
    half = 2 * rows
    remote = swap_with_sibling()
    places = ((rows, y_far0), (rows + Y_FIRST, y_far1), (0, y_own))
    copies = [remote(y_p.at[pl.ds(half + at, out.shape[0])], y_r.at[pl.ds(at, out.shape[0])], sems, k) for k, (at, out) in enumerate(places)]
    for c in copies:
        c.start()
    for c, (at, out) in zip(copies, places):
        c.wait()
        rows_at = pl.ds(at, out.shape[0])
        out[...] = y_p[rows_at, :] + y_r[rows_at, :]


def ysum(y_p, order):
    tokens, width = y_p.shape
    rows = tokens // 4
    return pl.pallas_call(
        ysum_kernel,
        name="ysum",
        out_shape=[sh((rows, width), F32), sh((Y_FIRST, width), F32), sh((rows - Y_FIRST, width), F32)],
        in_specs=[VMEM_SPEC, ANY_SPEC],
        out_specs=[VMEM_SPEC] * 3,
        scratch_shapes=[VMEM((2 * rows, width), F32), DMA((2, 3))],
        compiler_params=pltpu.CompilerParams(collective_id=4, has_side_effects=True, vmem_limit_bytes=8 * MIB),
        cost_estimate=pl.CostEstimate(flops=3_000_000_000, bytes_accessed=4 * MIB, transcendentals=0),
    )(y_p, order)


def grads_kernel(n, h, du, d_full, zero, order, table_in, token, dw1, dw2, table_g, dw1_v, dw2_v, s_zero, s_w):
    fill_start(zero, table_g, s_zero, 3)
    token[...] = jnp.zeros_like(token)
    width, hid = dw1.shape
    n_t = n[...].T
    for j in range(width // TILE):
        at = slice(j * TILE, (j + 1) * TILE)
        dw1_v[at, :] = mm(n_t[at, :], du[...], 1, 0)
        pltpu.make_async_copy(dw1_v.at[pl.ds(j * TILE, TILE)], dw1.at[pl.ds(j * TILE, TILE)], s_w).start()
    h_t = h[...].T
    for j in range(hid // TILE):
        at = slice(j * TILE, (j + 1) * TILE)
        dw2_v[at, :] = mm(h_t[at, :], d_full[...], 1, 0)
        pltpu.make_async_copy(dw2_v.at[pl.ds(j * TILE, TILE)], dw2.at[pl.ds(j * TILE, TILE)], s_w).start()
    pltpu.make_async_copy(dw1_v, dw1, s_w).wait()
    pltpu.make_async_copy(dw2_v, dw2, s_w).wait()
    fill_wait(zero, table_g, s_zero, 3)


def grads(n, h, du, d_full, zero, order, table_g):
    _, width = n.shape
    hid = h.shape[1]
    return pl.pallas_call(
        grads_kernel,
        name="grads",
        out_shape=[sh((8, 128), F32), sh((width, hid), F32), sh((hid, width), F32), sh(table_g.shape, F32)],
        in_specs=[VMEM_SPEC] * 5 + [ANY_SPEC, HBM_SPEC],
        out_specs=[VMEM_SPEC, HBM_SPEC, HBM_SPEC, HBM_SPEC],
        input_output_aliases={6: 3},
        scratch_shapes=[VMEM((width, hid), F32), VMEM((hid, width), F32), DMA(()), DMA(())],
        compiler_params=pltpu.CompilerParams(vmem_limit_bytes=24 * MIB),
        cost_estimate=pl.CostEstimate(flops=8_000_000_000, bytes_accessed=20 * MIB, transcendentals=0),
    )(n, h, du, d_full, zero, order, table_g)


def dx_kernel(dn_own, g2, x_own, d_own, gain, order, dx):
    gain_f = gain[...].astype(F32).reshape(1, dx.shape[1])
    for j in range(dx.shape[0] // 16):
        at = pl.ds(j * 16, 16)
        a = (dn_own[at, :] + g2[at, :]) * gain_f
        x = x_own[at, :].astype(F32)
        r = lax.rsqrt(jnp.mean(x * x, axis=-1, keepdims=True) + EPS)
        proj = jnp.mean(a * x, axis=-1, keepdims=True)
        dx[at, :] = (d_own[at, :].astype(F32) + r * (a - x * r * r * proj)).astype(BF)


def dx_rows(dn_own, g2, x_own, d_own, gain, order):
    return pl.pallas_call(
        dx_kernel,
        name="dx_rows",
        out_shape=sh(d_own.shape, BF),
        in_specs=[VMEM_SPEC] * 5 + [ANY_SPEC],
        out_specs=VMEM_SPEC,
        compiler_params=pltpu.CompilerParams(vmem_limit_bytes=4 * MIB),
        cost_estimate=pl.CostEstimate(flops=1_000_000_000, bytes_accessed=MIB, transcendentals=0),
    )(dn_own, g2, x_own, d_own, gain, order)


def fill3_kernel(zero, order, table_in, token, table_g, s_zero):
    fill_start(zero, table_g, s_zero, 4)
    token[...] = jnp.zeros_like(token)
    fill_wait(zero, table_g, s_zero, 4)


def fill3(zero, order, table_g):
    return pl.pallas_call(
        fill3_kernel,
        name="fill3",
        out_shape=[sh((8, 128), F32), sh(table_g.shape, F32)],
        in_specs=[VMEM_SPEC, ANY_SPEC, HBM_SPEC],
        out_specs=[VMEM_SPEC, HBM_SPEC],
        input_output_aliases={2: 1},
        scratch_shapes=[DMA(())],
        compiler_params=pltpu.CompilerParams(vmem_limit_bytes=4 * MIB),
        cost_estimate=pl.CostEstimate(flops=4_000_000_000, bytes_accessed=16 * MIB, transcendentals=0),
    )(zero, order, table_g)


def dx_all_kernel(dx, dx_far, order, dx_out, dx_r, sems):
    me = lax.axis_index("tp")
    rows = dx.shape[0]
    remote = swap_with_sibling()
    block = lambda m: pl.ds(pl.multiple_of((me ^ m) * rows, rows), rows)
    copies = [remote(src, dx_r.at[pl.ds(k * rows, rows)], sems, k) for k, src in enumerate((dx, dx_far))]
    for c in copies:
        c.start()
    dx_out[block(0), :] = dx[...]
    dx_out[block(2), :] = dx_far[...]
    for k, c in enumerate(copies):
        c.wait()
        dx_out[block(1 + 2 * k), :] = dx_r[pl.ds(k * rows, rows), :]


def dx_all(dx, dx_far, order):
    rows, width = dx.shape
    return pl.pallas_call(
        dx_all_kernel,
        name="dx_all",
        out_shape=sh((4 * rows, width), BF),
        in_specs=[VMEM_SPEC] * 2 + [ANY_SPEC],
        out_specs=VMEM_SPEC,
        scratch_shapes=[VMEM((2 * rows, width), BF), DMA((2, 2))],
        compiler_params=pltpu.CompilerParams(collective_id=3, has_side_effects=True, vmem_limit_bytes=4 * MIB),
        cost_estimate=pl.CostEstimate(flops=2_000_000_000, bytes_accessed=MIB, transcendentals=0),
    )(dx, dx_far, order)


def put_kernel(puts, same, dx, table_in, table_g, token, puts_s, total, s_in, s_row):
    tokens = dx.shape[0]
    load = pltpu.make_async_copy(puts, puts_s, s_in)
    load.start()
    total[...] = mm(same[...], dx[...], 1, 0)
    token[...] = jnp.zeros_like(token)
    load.wait()
    count = puts_s[tokens]

    def put(i):
        word = puts_s[i]
        pltpu.make_async_copy(total.at[pl.ds(word >> 16, 1)], table_g.at[pl.ds(word & 0xFFFF, 1)], s_row).start()

    def put_four(i, carry):
        for k in range(4):
            put(i * 4 + k)
        return carry

    def put_one(i, carry):
        put(i)
        return carry

    lax.fori_loop(0, count >> 2, put_four, 0)
    lax.fori_loop((count >> 2) * 4, count, put_one, 0)

    def put_wait(size):
        def body(i, carry):
            pltpu.make_async_copy(total.at[pl.ds(0, size)], table_g.at[pl.ds(0, size)], s_row).wait()
            return carry

        return body

    lax.fori_loop(0, count >> 3, put_wait(8), 0)
    lax.fori_loop(0, count & 7, put_wait(1), 0)


def put_rows(puts, same, dx, table_g):
    return pl.pallas_call(
        put_kernel,
        name="put_rows",
        out_shape=[sh(table_g.shape, F32), sh((8, 128), F32)],
        in_specs=[ANY_SPEC, VMEM_SPEC, VMEM_SPEC, HBM_SPEC],
        out_specs=[HBM_SPEC, VMEM_SPEC],
        input_output_aliases={3: 0},
        scratch_shapes=[pltpu.SMEM(puts.shape, I32), VMEM(dx.shape, F32), DMA(()), DMA(())],
        compiler_params=pltpu.CompilerParams(vmem_limit_bytes=4 * MIB),
        cost_estimate=pl.CostEstimate(flops=3_000_000_000, bytes_accessed=2 * MIB, transcendentals=0),
    )(puts, same, dx, table_g)


def finish_kernel(x, y, y_in0, y_in1, order, out):
    for first, y_in in ((0, y_in0), (Y_FIRST, y_in1)):
        at = pl.ds(first, y_in.shape[0])
        out[at, :] = (x[at, :].astype(F32) + (y[at, :] + y_in[...])).astype(BF)


def finish(x, y, y_in0, y_in1, order):
    return pl.pallas_call(
        finish_kernel,
        name="finish",
        out_shape=sh(y.shape, BF),
        in_specs=[VMEM_SPEC] * 4 + [ANY_SPEC],
        out_specs=VMEM_SPEC,
        compiler_params=pltpu.CompilerParams(vmem_limit_bytes=4 * MIB),
        cost_estimate=pl.CostEstimate(flops=1_000_000_000, bytes_accessed=MIB, transcendentals=0),
    )(x, y, y_in0, y_in1, order)


def solution(mesh):
    tp = mesh.shape["tp"]
    far_pairs = [(i, i ^ 2) for i in range(tp)]

    def far_permute(x):
        return lax.ppermute(x, "tp", far_pairs)

    def shard_step(ids, table, gain, w1, w2, d_out):
        part, rows_mine, same, zero, d_table = lookup(ids, table)
        send, w1 = pair(part, d_out, w1)
        got = lax.ppermute(send, "tp", far_pairs)
        puts, w2, d_table = fill1(rows_mine, zero, w2, send, d_table)
        x_f, d_full, n_a, h_a, du_a = share(send, got, w1, w2, gain)
        n, h, du, dn_p, d_table = mlp(x_f, d_full, n_a, h_a, du_a, w1, w2, gain, zero, d_table)
        dn_own, dn_far, y_p = sums(dn_p, du, h, w1, w2)
        g2 = far_permute(dn_far)
        y_own, y_far0, y_far1 = ysum(y_p, dn_own)
        y_in0 = lax.ppermute(y_far0, "tp", far_pairs)
        token, d_w1, d_w2, d_table = grads(n, h, du, d_full, zero, y_own, d_table)
        dx = dx_rows(dn_own, g2, x_f, d_out, gain, token)
        dx_far = far_permute(dx)
        dx, y_far1 = lax.optimization_barrier((dx, y_far1))
        y_in1 = far_permute(y_far1)
        token, d_table = fill3(zero, dx, d_table)
        dx_full = dx_all(dx, dx_far, token)
        d_table, done = put_rows(puts, same, dx_full, d_table)
        out = finish(x_f, y_own, y_in0, y_in1, done)
        return out, d_table, d_w1, d_w2

    return jax.shard_map(
        shard_step,
        mesh=mesh,
        in_specs=(P("dp"), P("tp", None), P(None), P(None, "tp"), P("tp", None), P(("dp", "tp"), None)),
        out_specs=(P(("dp", "tp"), None), P(("dp", "tp"), None), P("dp", "tp"), P(("dp", "tp"), None)),
        check_vma=False,
    )
```

```python
import jax
import jax.numpy as jnp
from jax import lax
from jax.experimental import pallas as pl
from jax.experimental.pallas import tpu as pltpu
from jax.sharding import PartitionSpec as P

EPS = 1e-6
BF = jnp.bfloat16
F32 = jnp.float32
I32 = jnp.int32
GELU_C = 0.7978845608028654
GELU_A = 0.044715
VMEM = pltpu.VMEM
SMEM_SPEC = pl.BlockSpec(memory_space=pltpu.SMEM)
ANY_SPEC = pl.BlockSpec(memory_space=pl.ANY)
HBM_SPEC = pl.BlockSpec(memory_space=pltpu.HBM)
VMEM_SPEC = pl.BlockSpec(memory_space=VMEM)
DMA = pltpu.SemaphoreType.DMA
TILE = 256
ZERO_ROWS = 96
FILL_AT = (0, 4, 81, 93, 103, 112, 131)
MIB = 1 << 20
LOOKUP_VMEM = 48 * MIB
PAIR_VMEM = 8 * MIB


def mm(a, b, ca, cb):
    return lax.dot_general(a, b, (((ca,), (cb,)), ((), ())), preferred_element_type=F32)


def in_hbm(x):
    return pltpu.with_memory_space_constraint(x, pltpu.HBM)


def sh(shape, dtype):
    return jax.ShapeDtypeStruct(shape, dtype)


def fill_copy(zero, table_g, sem, i):
    return pltpu.make_async_copy(zero, table_g.at[pl.ds(pl.multiple_of(i * ZERO_ROWS, ZERO_ROWS), ZERO_ROWS)], sem)


def fill_start(zero, table_g, sem, part):
    def body(i, carry):
        fill_copy(zero, table_g, sem, i).start()
        return carry

    lax.fori_loop(FILL_AT[part], FILL_AT[part + 1], body, 0)


def fill_wait(zero, table_g, sem, part):
    def body(i, carry):
        fill_copy(zero, table_g, sem, i).wait()
        return carry

    lax.fori_loop(FILL_AT[part], FILL_AT[part + 1], body, 0)


def swap_with_sibling():
    sib = lax.axis_index("tp") ^ 1
    barrier = pltpu.get_barrier_semaphore()
    pl.semaphore_signal(barrier, inc=1, device_id={"tp": sib}, device_id_type=pl.DeviceIdType.MESH)
    pl.semaphore_wait(barrier, 1)

    def remote(src, dst, sems, i):
        return pltpu.make_async_remote_copy(
            src_ref=src, dst_ref=dst, send_sem=sems.at[0, i], recv_sem=sems.at[1, i],
            device_id={"tp": sib}, device_id_type=pl.DeviceIdType.MESH)

    return remote


def lookup_kernel(ids, ids_row, table, part, rows_mine, same, zero, table_g, ids_s, ids_v, pairs, sems, s_zero, s_ids):
    tokens, vocab = part.shape[0], table.shape[0]
    base = lax.axis_index("tp") * vocab
    group = 64
    groups = tokens // group
    loads = [pltpu.make_async_copy(ids, ids_s, s_ids.at[0]), pltpu.make_async_copy(ids_row, ids_v, s_ids.at[1])]
    for c in loads:
        c.start()
    zero[...] = jnp.zeros_like(zero)
    fill_start(zero, table_g, s_zero, 0)
    loads[0].wait()

    def fetch(k, carry):
        for i in range(group):
            token = k * group + i
            lid = ids_s[token] - base
            owned = (lid >= 0) & (lid < vocab)
            row = jnp.where(owned, lid & -2, 2 * token)
            pltpu.make_async_copy(table.at[pl.ds(pl.multiple_of(row, 2), 2)], pairs.at[k, pl.ds(2 * i, 2)], sems.at[k]).start()
        return carry

    lax.fori_loop(0, groups, fetch, 0)
    loads[1].wait()
    row = jnp.broadcast_to(ids_v[...].astype(F32), (tokens, tokens))
    col = row.T
    equal = row == col
    same[...] = jnp.where(equal, 1.0, 0.0).astype(BF)
    earlier = lax.broadcasted_iota(I32, (tokens, tokens), 0) < lax.broadcasted_iota(I32, (tokens, tokens), 1)
    repeat = jnp.max(jnp.where(equal & earlier, 1, 0), axis=0, keepdims=True)
    mine = ids_v[...] - base
    rows_mine[...] = jnp.where((mine >= 0) & (mine < vocab) & (repeat == 0), mine, -1)
    lid = col.astype(I32) - base
    lane = lax.broadcasted_iota(I32, (group, 2 * group), 1)
    first = lax.broadcasted_iota(I32, (group, 2 * group), 0) * 2
    for k in range(groups):
        at = lid[k * group:(k + 1) * group, :2 * group]
        owned = (at >= 0) & (at < vocab)
        pick = jnp.where(owned & (lane == first + (at & 1)), 1.0, 0.0).astype(BF)
        pltpu.make_async_copy(table.at[pl.ds(0, group * 2)], pairs.at[k], sems.at[k]).wait()
        part[pl.ds(k * group, group), :] = mm(pick, pairs[k], 1, 0).astype(BF)
    fill_wait(zero, table_g, s_zero, 0)


def lookup(ids, table):
    tokens, (vocab, width) = ids.shape[0], table.shape
    return pl.pallas_call(
        lookup_kernel,
        name="lookup",
        out_shape=[sh((tokens, width), BF), sh((1, tokens), I32), sh((tokens, tokens), BF), sh((ZERO_ROWS, width), F32), sh((vocab, width), F32)],
        in_specs=[HBM_SPEC] * 3,
        out_specs=[VMEM_SPEC] * 4 + [HBM_SPEC],
        scratch_shapes=[pltpu.SMEM((tokens,), I32), VMEM((1, tokens), I32), VMEM((4, tokens // 2, width), BF), DMA((4,)), DMA(()), DMA((2,))],
        compiler_params=pltpu.CompilerParams(vmem_limit_bytes=LOOKUP_VMEM),
        cost_estimate=pl.CostEstimate(flops=5_000_000_000, bytes_accessed=10 * MIB, transcendentals=0),
    )(in_hbm(ids), in_hbm(ids.reshape(1, tokens)), in_hbm(table))


def pair_kernel(part, d_out, w1, send, w1_v, part_r, sems, s_in):
    me = lax.axis_index("tp")
    rows = d_out.shape[0]
    blocks = (me, me ^ 2, me ^ 1, me ^ 3)
    loads = [pltpu.make_async_copy(d_out, send.at[pl.ds(2 * rows, rows)], s_in.at[0]), pltpu.make_async_copy(w1, w1_v, s_in.at[1])]
    for c in loads:
        c.start()
    remote = swap_with_sibling()
    block = lambda k: pl.ds(pl.multiple_of(blocks[k] * rows, rows), rows)
    copies = [remote(part.at[block(2 + k)], part_r.at[pl.ds(k * rows, rows)], sems, k) for k in range(2)]
    for c in copies:
        c.start()
    for k in range(2):
        copies[k].wait()
        at = pl.ds(k * rows, rows)
        send[at, :] = part[block(k), :] + part_r[at, :]
    for c in loads:
        c.wait()


def pair(part, d_out, w1):
    rows, width = d_out.shape
    return pl.pallas_call(
        pair_kernel,
        name="pair",
        out_shape=[sh((3 * rows, width), BF), sh(w1.shape, BF)],
        in_specs=[VMEM_SPEC, HBM_SPEC, HBM_SPEC],
        out_specs=[VMEM_SPEC] * 2,
        scratch_shapes=[VMEM((2 * rows, width), BF), DMA((2, 2)), DMA((2,))],
        compiler_params=pltpu.CompilerParams(collective_id=0, has_side_effects=True, vmem_limit_bytes=PAIR_VMEM),
        cost_estimate=pl.CostEstimate(flops=3_000_000_000, bytes_accessed=MIB, transcendentals=0),
    )(part, in_hbm(d_out), in_hbm(w1))


def fill1_kernel(rows_mine, zero, w2, order, table_in, puts, w2_v, table_g, mine_s, puts_s, s_zero, s_list, s_w):
    load = pltpu.make_async_copy(rows_mine, mine_s, s_list)
    load.start()
    load_w = pltpu.make_async_copy(w2, w2_v, s_w)
    load_w.start()
    fill_start(zero, table_g, s_zero, 1)
    tokens = rows_mine.shape[1]
    load.wait()

    def body(i, count):
        lid = mine_s[0, i]
        puts_s[count] = lid | (i << 16)
        return count + (lid >= 0).astype(I32)

    puts_s[tokens] = lax.fori_loop(0, tokens, body, 0, unroll=8)
    store = pltpu.make_async_copy(puts_s, puts, s_list)
    store.start()
    store.wait()
    load_w.wait()
    fill_wait(zero, table_g, s_zero, 1)


def fill1(rows_mine, zero, w2, order, table_g):
    tokens = rows_mine.shape[1]
    return pl.pallas_call(
        fill1_kernel,
        name="fill1",
        out_shape=[sh((2 * tokens,), I32), sh(w2.shape, BF), sh(table_g.shape, F32)],
        in_specs=[ANY_SPEC, VMEM_SPEC, HBM_SPEC, ANY_SPEC, HBM_SPEC],
        out_specs=[ANY_SPEC, VMEM_SPEC, HBM_SPEC],
        input_output_aliases={4: 2},
        scratch_shapes=[pltpu.SMEM((1, tokens), I32), pltpu.SMEM((2 * tokens,), I32), DMA(()), DMA(()), DMA(())],
        compiler_params=pltpu.CompilerParams(vmem_limit_bytes=8 * MIB),
        cost_estimate=pl.CostEstimate(flops=9_000_000_000, bytes_accessed=20 * MIB, transcendentals=0),
    )(rows_mine, zero, in_hbm(w2), order, table_g)


def mlp_half(x, d, n, h, du, at, w1, w2, gain):
    first, count = at
    width, hid = n.shape[1], h.shape[1]
    gain_f = gain[...].astype(F32).reshape(1, width)
    for j in range(count // 32):
        rows = pl.ds(first + j * 32, 32)
        x_f = x[rows, :].astype(F32)
        r = lax.rsqrt(jnp.mean(x_f * x_f, axis=-1, keepdims=True) + EPS)
        n[rows, :] = (x_f * r * gain_f).astype(BF)
    rows = pl.ds(first, count)
    for j in range(hid // TILE):
        cols = pl.ds(j * TILE, TILE)
        g = mm(d[rows, :], w2[cols, :], 1, 1).astype(BF).astype(F32)
        u = mm(n[rows, :], w1[:, cols], 1, 0).astype(BF).astype(F32)
        t = jnp.tanh(GELU_C * (u + GELU_A * (u * u * u)))
        cdf = 0.5 * (1.0 + t)
        h[rows, cols] = (u * cdf).astype(BF)
        du[rows, cols] = (g * (cdf + u * (0.5 * (1.0 - t * t)) * (GELU_C * (1.0 + 3.0 * GELU_A * (u * u))))).astype(BF)


def share_kernel(send, got, w1, w2, gain, x_f, d_full, n_a, h_a, du_a, x_r, d_r, sems):
    rows = send.shape[0] // 3
    half = 2 * rows
    remote = swap_with_sibling()
    copies = []
    for k in range(2):
        at, other = pl.ds(k * rows, rows), pl.ds((1 - k) * rows, rows)
        x_f[at, :] = send[at, :] + got[other, :]
        copies.append(remote(x_f.at[at], x_r.at[at], sems, k))
        copies[-1].start()
    for k, src in enumerate((send, got)):
        copies.append(remote(src.at[pl.ds(half, rows)], d_r.at[pl.ds(k * rows, rows)], sems, 2 + k))
        copies[-1].start()
        d_full[pl.ds(k * rows, rows), :] = src[pl.ds(half, rows), :]
    mlp_half(x_f, d_full, n_a, h_a, du_a, (0, half), w1, w2, gain)
    for k in range(2):
        copies[k].wait()
        x_f[pl.ds(half + k * rows, rows), :] = x_r[pl.ds(k * rows, rows), :]
    for k in range(2):
        copies[2 + k].wait()
        d_full[pl.ds(half + k * rows, rows), :] = d_r[pl.ds(k * rows, rows), :]


def share(send, got, w1, w2, gain):
    rows, width = send.shape[0] // 3, send.shape[1]
    hid = w1.shape[1]
    return pl.pallas_call(
        share_kernel,
        name="share",
        out_shape=[sh((4 * rows, width), BF)] * 2 + [sh((2 * rows, width), BF)] + [sh((2 * rows, hid), BF)] * 2,
        in_specs=[VMEM_SPEC] * 5,
        out_specs=[VMEM_SPEC] * 5,
        scratch_shapes=[VMEM((2 * rows, width), BF), VMEM((2 * rows, width), BF), DMA((2, 4))],
        compiler_params=pltpu.CompilerParams(collective_id=1, has_side_effects=True, vmem_limit_bytes=16 * MIB),
        cost_estimate=pl.CostEstimate(flops=3_000_000_000, bytes_accessed=MIB, transcendentals=0),
    )(send, got, w1, w2, gain)


def mlp_kernel(x_f, d_full, n_a, h_a, du_a, w1, w2, gain, zero, table_in, n, h, du, dn_p, table_g, s_zero):
    fill_start(zero, table_g, s_zero, 2)
    tokens, width = n.shape
    half = tokens // 2
    for out, src in ((n, n_a), (h, h_a), (du, du_a)):
        out[pl.ds(0, half), :] = src[...]
    mlp_half(x_f, d_full, n, h, du, (half, half), w1, w2, gain)
    for j in range(width // TILE):
        cols = pl.ds(j * TILE, TILE)
        dn_p[:, cols] = mm(du[pl.ds(half, half), :], w1[cols, :], 1, 1)
    fill_wait(zero, table_g, s_zero, 2)


def mlp(x_f, d_full, n_a, h_a, du_a, w1, w2, gain, zero, table_g):
    tokens, width = x_f.shape
    hid = w1.shape[1]
    return pl.pallas_call(
        mlp_kernel,
        name="mlp",
        out_shape=[sh((tokens, width), BF), sh((tokens, hid), BF), sh((tokens, hid), BF), sh((tokens // 2, width), F32),
                   sh(table_g.shape, F32)],
        in_specs=[VMEM_SPEC] * 9 + [HBM_SPEC],
        out_specs=[VMEM_SPEC] * 4 + [HBM_SPEC],
        input_output_aliases={9: 4},
        scratch_shapes=[DMA(())],
        compiler_params=pltpu.CompilerParams(vmem_limit_bytes=16 * MIB),
        cost_estimate=pl.CostEstimate(flops=6_000_000_000, bytes_accessed=4 * MIB, transcendentals=0),
    )(x_f, d_full, n_a, h_a, du_a, w1, w2, gain, zero, table_g)


def sums_kernel(dn_p, du, h, w1, w2, dn_own, dn_far, y_a, y_b, dn_r, dn_m, sems):
    rows, width = dn_own.shape
    half = 2 * rows
    remote = swap_with_sibling()
    copies = [remote(dn_p.at[pl.ds(k * rows, rows)], dn_r.at[pl.ds(k * rows, rows)], sems, k) for k in (1, 0)]
    for c in copies:
        c.start()
    for j in range(width // TILE):
        cols = pl.ds(j * TILE, TILE)
        dn_m[:, cols] = mm(du[pl.ds(0, half), :], w1[cols, :], 1, 1)
    for j in range(width // TILE):
        cols = pl.ds(j * TILE, TILE)
        y = mm(h[...], w2[:, cols], 1, 0)
        y_a[:, cols] = y[:half]
        y_b[:, cols] = y[half:]
    for c, out, k in zip(copies, (dn_far, dn_own), (1, 0)):
        c.wait()
        at = pl.ds(k * rows, rows)
        out[...] = dn_m[at, :] + dn_r[at, :]


def sums(dn_p, du, h, w1, w2):
    half, width = dn_p.shape
    rows = half // 2
    return pl.pallas_call(
        sums_kernel,
        name="sums",
        out_shape=[sh((rows, width), F32)] * 2 + [sh((half, width), F32)] * 2,
        in_specs=[VMEM_SPEC] * 5,
        out_specs=[VMEM_SPEC] * 4,
        scratch_shapes=[VMEM((half, width), F32), VMEM((half, width), F32), DMA((2, 2))],
        compiler_params=pltpu.CompilerParams(collective_id=2, has_side_effects=True, vmem_limit_bytes=16 * MIB),
        cost_estimate=pl.CostEstimate(flops=4_000_000_000, bytes_accessed=4 * MIB, transcendentals=0),
    )(dn_p, du, h, w1, w2)


def grads1_kernel(n, du, zero, order, table_in, dw1, table_g, dw1_v, s_zero, s_w):
    width = n.shape[1]
    n_t = n[...].T
    for j in range(width // TILE):
        at = slice(j * TILE, (j + 1) * TILE)
        dw1_v[at, :] = mm(n_t[at, :], du[...], 1, 0)
        pltpu.make_async_copy(dw1_v.at[pl.ds(j * TILE, TILE)], dw1.at[pl.ds(j * TILE, TILE)], s_w).start()
        if j == 0:
            fill_start(zero, table_g, s_zero, 3)
    pltpu.make_async_copy(dw1_v, dw1, s_w).wait()
    fill_wait(zero, table_g, s_zero, 3)


def grads1(n, du, zero, order, table_g):
    width, hid = n.shape[1], du.shape[1]
    return pl.pallas_call(
        grads1_kernel,
        name="grads1",
        out_shape=[sh((width, hid), F32), sh(table_g.shape, F32)],
        in_specs=[VMEM_SPEC] * 3 + [ANY_SPEC, HBM_SPEC],
        out_specs=[HBM_SPEC, HBM_SPEC],
        input_output_aliases={4: 1},
        scratch_shapes=[VMEM((width, hid), F32), DMA(()), DMA(())],
        compiler_params=pltpu.CompilerParams(vmem_limit_bytes=16 * MIB),
        cost_estimate=pl.CostEstimate(flops=4_000_000_000, bytes_accessed=8 * MIB, transcendentals=0),
    )(n, du, zero, order, table_g)


def grads2_kernel(h, d_full, y_a, y_sib, zero, table_in, dw2, y_own, y_far, table_g, dw2_v, s_zero, s_w):
    rows = y_own.shape[0]
    hid = h.shape[1]
    fill_start(zero, table_g, s_zero, 4)
    for k, out in enumerate((y_own, y_far)):
        at = pl.ds(k * rows, rows)
        out[...] = y_a[at, :] + y_sib[at, :]
    h_t = h[...].T
    for j in range(hid // TILE):
        at = slice(j * TILE, (j + 1) * TILE)
        dw2_v[at, :] = mm(h_t[at, :], d_full[...], 1, 0)
        pltpu.make_async_copy(dw2_v.at[pl.ds(j * TILE, TILE)], dw2.at[pl.ds(j * TILE, TILE)], s_w).start()
    pltpu.make_async_copy(dw2_v, dw2, s_w).wait()
    fill_wait(zero, table_g, s_zero, 4)


def grads2(h, d_full, y_a, y_sib, zero, table_g):
    hid, width = h.shape[1], d_full.shape[1]
    rows = y_a.shape[0] // 2
    return pl.pallas_call(
        grads2_kernel,
        name="grads2",
        out_shape=[sh((hid, width), F32)] + [sh((rows, width), F32)] * 2 + [sh(table_g.shape, F32)],
        in_specs=[VMEM_SPEC] * 5 + [HBM_SPEC],
        out_specs=[HBM_SPEC, VMEM_SPEC, VMEM_SPEC, HBM_SPEC],
        input_output_aliases={5: 3},
        scratch_shapes=[VMEM((hid, width), F32), DMA(()), DMA(())],
        compiler_params=pltpu.CompilerParams(vmem_limit_bytes=16 * MIB),
        cost_estimate=pl.CostEstimate(flops=4_000_000_000, bytes_accessed=8 * MIB, transcendentals=0),
    )(h, d_full, y_a, y_sib, zero, table_g)


def dx_kernel(dn_own, g2, x_own, d_own, gain, order, dx):
    gain_f = gain[...].astype(F32).reshape(1, dx.shape[1])
    for j in range(dx.shape[0] // 16):
        at = pl.ds(j * 16, 16)
        a = (dn_own[at, :] + g2[at, :]) * gain_f
        x = x_own[at, :].astype(F32)
        r = lax.rsqrt(jnp.mean(x * x, axis=-1, keepdims=True) + EPS)
        proj = jnp.mean(a * x, axis=-1, keepdims=True)
        dx[at, :] = (d_own[at, :].astype(F32) + r * (a - x * r * r * proj)).astype(BF)


def dx_rows(dn_own, g2, x_own, d_own, gain, order):
    return pl.pallas_call(
        dx_kernel,
        name="dx_rows",
        out_shape=sh(d_own.shape, BF),
        in_specs=[VMEM_SPEC] * 5 + [ANY_SPEC],
        out_specs=VMEM_SPEC,
        compiler_params=pltpu.CompilerParams(vmem_limit_bytes=4 * MIB),
        cost_estimate=pl.CostEstimate(flops=1_000_000_000, bytes_accessed=MIB, transcendentals=0),
    )(dn_own, g2, x_own, d_own, gain, order)


def fill3_kernel(zero, order, table_in, token, table_g, s_zero):
    fill_start(zero, table_g, s_zero, 5)
    token[...] = jnp.zeros_like(token)
    fill_wait(zero, table_g, s_zero, 5)


def fill3(zero, order, table_g):
    return pl.pallas_call(
        fill3_kernel,
        name="fill3",
        out_shape=[sh((8, 128), F32), sh(table_g.shape, F32)],
        in_specs=[VMEM_SPEC, ANY_SPEC, HBM_SPEC],
        out_specs=[VMEM_SPEC, HBM_SPEC],
        input_output_aliases={2: 1},
        scratch_shapes=[DMA(())],
        compiler_params=pltpu.CompilerParams(vmem_limit_bytes=4 * MIB),
        cost_estimate=pl.CostEstimate(flops=4_000_000_000, bytes_accessed=16 * MIB, transcendentals=0),
    )(zero, order, table_g)


def dx_all_kernel(dx, dx_far, order, dx_out, dx_r, sems):
    me = lax.axis_index("tp")
    rows = dx.shape[0]
    remote = swap_with_sibling()
    block = lambda m: pl.ds(pl.multiple_of((me ^ m) * rows, rows), rows)
    copies = [remote(src, dx_r.at[pl.ds(k * rows, rows)], sems, k) for k, src in enumerate((dx, dx_far))]
    for c in copies:
        c.start()
    dx_out[block(0), :] = dx[...]
    dx_out[block(2), :] = dx_far[...]
    for k, c in enumerate(copies):
        c.wait()
        dx_out[block(1 + 2 * k), :] = dx_r[pl.ds(k * rows, rows), :]


def dx_all(dx, dx_far, order):
    rows, width = dx.shape
    return pl.pallas_call(
        dx_all_kernel,
        name="dx_all",
        out_shape=sh((4 * rows, width), BF),
        in_specs=[VMEM_SPEC] * 2 + [ANY_SPEC],
        out_specs=VMEM_SPEC,
        scratch_shapes=[VMEM((2 * rows, width), BF), DMA((2, 2))],
        compiler_params=pltpu.CompilerParams(collective_id=3, has_side_effects=True, vmem_limit_bytes=4 * MIB),
        cost_estimate=pl.CostEstimate(flops=2_000_000_000, bytes_accessed=MIB, transcendentals=0),
    )(dx, dx_far, order)


def put_kernel(puts, same, dx, table_in, table_g, token, puts_s, total, s_in, s_row):
    tokens = dx.shape[0]
    load = pltpu.make_async_copy(puts, puts_s, s_in)
    load.start()
    total[...] = mm(same[...], dx[...], 1, 0)
    token[...] = jnp.zeros_like(token)
    load.wait()
    count = puts_s[tokens]

    def put(i):
        word = puts_s[i]
        pltpu.make_async_copy(total.at[pl.ds(word >> 16, 1)], table_g.at[pl.ds(word & 0xFFFF, 1)], s_row).start()

    def put_four(i, carry):
        for k in range(4):
            put(i * 4 + k)
        return carry

    def put_one(i, carry):
        put(i)
        return carry

    lax.fori_loop(0, count >> 2, put_four, 0)
    lax.fori_loop((count >> 2) * 4, count, put_one, 0)

    def put_wait(size):
        def body(i, carry):
            pltpu.make_async_copy(total.at[pl.ds(0, size)], table_g.at[pl.ds(0, size)], s_row).wait()
            return carry

        return body

    lax.fori_loop(0, count >> 3, put_wait(8), 0)
    lax.fori_loop(0, count & 7, put_wait(1), 0)


def put_rows(puts, same, dx, table_g):
    return pl.pallas_call(
        put_kernel,
        name="put_rows",
        out_shape=[sh(table_g.shape, F32), sh((8, 128), F32)],
        in_specs=[ANY_SPEC, VMEM_SPEC, VMEM_SPEC, HBM_SPEC],
        out_specs=[HBM_SPEC, VMEM_SPEC],
        input_output_aliases={3: 0},
        scratch_shapes=[pltpu.SMEM(puts.shape, I32), VMEM(dx.shape, F32), DMA(()), DMA(())],
        compiler_params=pltpu.CompilerParams(vmem_limit_bytes=4 * MIB),
        cost_estimate=pl.CostEstimate(flops=3_000_000_000, bytes_accessed=2 * MIB, transcendentals=0),
    )(puts, same, dx, table_g)


def finish_kernel(x, y, y_in, order, out):
    out[...] = (x[pl.ds(0, out.shape[0]), :].astype(F32) + (y[...] + y_in[...])).astype(BF)


def finish(x, y, y_in, order):
    return pl.pallas_call(
        finish_kernel,
        name="finish",
        out_shape=sh(y.shape, BF),
        in_specs=[VMEM_SPEC] * 3 + [ANY_SPEC],
        out_specs=VMEM_SPEC,
        compiler_params=pltpu.CompilerParams(vmem_limit_bytes=4 * MIB),
        cost_estimate=pl.CostEstimate(flops=1_000_000_000, bytes_accessed=MIB, transcendentals=0),
    )(x, y, y_in, order)


def solution(mesh):
    tp = mesh.shape["tp"]

    def permute(x, hop):
        return lax.ppermute(x, "tp", [(i, i ^ hop) for i in range(tp)])

    def shard_step(ids, table, gain, w1, w2, d_out):
        part, rows_mine, same, zero, d_table = lookup(ids, table)
        send, w1 = pair(part, d_out, w1)
        got = permute(send, 2)
        puts, w2, d_table = fill1(rows_mine, zero, w2, send, d_table)
        x_f, d_full, n_a, h_a, du_a = share(send, got, w1, w2, gain)
        n, h, du, dn_p, d_table = mlp(x_f, d_full, n_a, h_a, du_a, w1, w2, gain, zero, d_table)
        dn_own, dn_far, y_a, y_b = sums(dn_p, du, h, w1, w2)
        g2 = permute(dn_far, 2)
        y_sib = permute(y_b, 1)
        d_w1, d_table = grads1(n, du, zero, dn_own, d_table)
        d_w2, y_own, y_far, d_table = grads2(h, d_full, y_a, y_sib, zero, d_table)
        dx = dx_rows(dn_own, g2, x_f, d_out, gain, y_own)
        dx_far = permute(dx, 2)
        dx, y_far = lax.optimization_barrier((dx, y_far))
        y_in = permute(y_far, 2)
        token, d_table = fill3(zero, dx, d_table)
        dx_full = dx_all(dx, dx_far, token)
        d_table, done = put_rows(puts, same, dx_full, d_table)
        out = finish(x_f, y_own, y_in, done)
        return out, d_table, d_w1, d_w2

    return jax.shard_map(
        shard_step,
        mesh=mesh,
        in_specs=(P("dp"), P("tp", None), P(None), P(None, "tp"), P("tp", None), P(("dp", "tp"), None)),
        out_specs=(P(("dp", "tp"), None), P(("dp", "tp"), None), P("dp", "tp"), P(("dp", "tp"), None)),
        check_vma=False,
    )
```

```python
import jax
import jax.numpy as jnp
from jax import lax
from jax.experimental import pallas as pl
from jax.experimental.pallas import tpu as pltpu
from jax.sharding import PartitionSpec as P

EPS = 1e-6
BF = jnp.bfloat16
F32 = jnp.float32
I32 = jnp.int32
GELU_C = 0.7978845608028654
GELU_A = 0.044715
VMEM = pltpu.VMEM
SMEM_SPEC = pl.BlockSpec(memory_space=pltpu.SMEM)
ANY_SPEC = pl.BlockSpec(memory_space=pl.ANY)
HBM_SPEC = pl.BlockSpec(memory_space=pltpu.HBM)
VMEM_SPEC = pl.BlockSpec(memory_space=VMEM)
DMA = pltpu.SemaphoreType.DMA
TILE = 256
ZERO_ROWS = 96
FILL_AT = (0, 4, 69, 82, 93, 102, 131)
LATE_FILL = 8
MIB = 1 << 20
LOOKUP_VMEM = 48 * MIB
PAIR_VMEM = 8 * MIB


def mm(a, b, ca, cb):
    return lax.dot_general(a, b, (((ca,), (cb,)), ((), ())), preferred_element_type=F32)


def in_hbm(x):
    return pltpu.with_memory_space_constraint(x, pltpu.HBM)


def sh(shape, dtype):
    return jax.ShapeDtypeStruct(shape, dtype)


def fill_copy(zero, table_g, sem, i):
    return pltpu.make_async_copy(zero, table_g.at[pl.ds(pl.multiple_of(i * ZERO_ROWS, ZERO_ROWS), ZERO_ROWS)], sem)


def fill_range(part):
    late = (lax.axis_index("tp") >> 1) * LATE_FILL
    if part == "late":
        return FILL_AT[2] - late, FILL_AT[2]
    return FILL_AT[part], FILL_AT[part + 1] - (late if part == 1 else 0)


def fill_start(zero, table_g, sem, part):
    def body(i, carry):
        fill_copy(zero, table_g, sem, i).start()
        return carry

    lax.fori_loop(*fill_range(part), body, 0)


def fill_wait(zero, table_g, sem, part):
    def body(i, carry):
        fill_copy(zero, table_g, sem, i).wait()
        return carry

    lax.fori_loop(*fill_range(part), body, 0)


def swap_with_sibling():
    sib = lax.axis_index("tp") ^ 1
    barrier = pltpu.get_barrier_semaphore()
    pl.semaphore_signal(barrier, inc=1, device_id={"tp": sib}, device_id_type=pl.DeviceIdType.MESH)
    pl.semaphore_wait(barrier, 1)

    def remote(src, dst, sems, i):
        return pltpu.make_async_remote_copy(
            src_ref=src, dst_ref=dst, send_sem=sems.at[0, i], recv_sem=sems.at[1, i],
            device_id={"tp": sib}, device_id_type=pl.DeviceIdType.MESH)

    return remote


def lookup_kernel(ids, ids_row, table, part, rows_mine, same, zero, table_g, ids_s, ids_v, pairs, sems, s_zero, s_ids):
    tokens, vocab = part.shape[0], table.shape[0]
    base = lax.axis_index("tp") * vocab
    group = 64
    groups = tokens // group
    loads = [pltpu.make_async_copy(ids, ids_s, s_ids.at[0]), pltpu.make_async_copy(ids_row, ids_v, s_ids.at[1])]
    for c in loads:
        c.start()
    zero[...] = jnp.zeros_like(zero)
    fill_start(zero, table_g, s_zero, 0)
    loads[0].wait()

    def fetch(k, carry):
        for i in range(group):
            token = k * group + i
            lid = ids_s[token] - base
            owned = (lid >= 0) & (lid < vocab)
            row = jnp.where(owned, lid & -2, 2 * token)
            pltpu.make_async_copy(table.at[pl.ds(pl.multiple_of(row, 2), 2)], pairs.at[k, pl.ds(2 * i, 2)], sems.at[k]).start()
        return carry

    lax.fori_loop(0, groups, fetch, 0)
    loads[1].wait()
    row = jnp.broadcast_to(ids_v[...].astype(F32), (tokens, tokens))
    col = row.T
    equal = row == col
    same[...] = jnp.where(equal, 1.0, 0.0).astype(BF)
    earlier = lax.broadcasted_iota(I32, (tokens, tokens), 0) < lax.broadcasted_iota(I32, (tokens, tokens), 1)
    repeat = jnp.max(jnp.where(equal & earlier, 1, 0), axis=0, keepdims=True)
    mine = ids_v[...] - base
    rows_mine[...] = jnp.where((mine >= 0) & (mine < vocab) & (repeat == 0), mine, -1)
    lid = col.astype(I32) - base
    lane = lax.broadcasted_iota(I32, (group, 2 * group), 1)
    first = lax.broadcasted_iota(I32, (group, 2 * group), 0) * 2
    for k in range(groups):
        at = lid[k * group:(k + 1) * group, :2 * group]
        owned = (at >= 0) & (at < vocab)
        pick = jnp.where(owned & (lane == first + (at & 1)), 1.0, 0.0).astype(BF)
        pltpu.make_async_copy(table.at[pl.ds(0, group * 2)], pairs.at[k], sems.at[k]).wait()
        part[pl.ds(k * group, group), :] = mm(pick, pairs[k], 1, 0).astype(BF)
    fill_wait(zero, table_g, s_zero, 0)


def lookup(ids, table):
    tokens, (vocab, width) = ids.shape[0], table.shape
    return pl.pallas_call(
        lookup_kernel,
        name="lookup",
        out_shape=[sh((tokens, width), BF), sh((1, tokens), I32), sh((tokens, tokens), BF), sh((ZERO_ROWS, width), F32), sh((vocab, width), F32)],
        in_specs=[HBM_SPEC] * 3,
        out_specs=[VMEM_SPEC] * 4 + [HBM_SPEC],
        scratch_shapes=[pltpu.SMEM((tokens,), I32), VMEM((1, tokens), I32), VMEM((4, tokens // 2, width), BF), DMA((4,)), DMA(()), DMA((2,))],
        compiler_params=pltpu.CompilerParams(vmem_limit_bytes=LOOKUP_VMEM),
        cost_estimate=pl.CostEstimate(flops=5_000_000_000, bytes_accessed=10 * MIB, transcendentals=0),
    )(in_hbm(ids), in_hbm(ids.reshape(1, tokens)), in_hbm(table))


def pair_kernel(part, w1, send, w1_v, part_r, sems, s_in):
    me = lax.axis_index("tp")
    rows = part.shape[0] // 4
    blocks = (me, me ^ 2, me ^ 1, me ^ 3)
    load = pltpu.make_async_copy(w1, w1_v, s_in)
    load.start()
    remote = swap_with_sibling()
    block = lambda k: pl.ds(pl.multiple_of(blocks[k] * rows, rows), rows)
    copies = [remote(part.at[block(2 + k)], part_r.at[pl.ds(k * rows, rows)], sems, k) for k in range(2)]
    for c in copies:
        c.start()
    for k in range(2):
        copies[k].wait()
        at = pl.ds(k * rows, rows)
        send[at, :] = part[block(k), :] + part_r[at, :]
    load.wait()


def pair(part, w1):
    rows, width = part.shape[0] // 4, part.shape[1]
    return pl.pallas_call(
        pair_kernel,
        name="pair",
        out_shape=[sh((2 * rows, width), BF), sh(w1.shape, BF)],
        in_specs=[VMEM_SPEC, HBM_SPEC],
        out_specs=[VMEM_SPEC] * 2,
        scratch_shapes=[VMEM((2 * rows, width), BF), DMA((2, 2)), DMA(())],
        compiler_params=pltpu.CompilerParams(collective_id=0, has_side_effects=True, vmem_limit_bytes=PAIR_VMEM),
        cost_estimate=pl.CostEstimate(flops=3_000_000_000, bytes_accessed=MIB, transcendentals=0),
    )(part, in_hbm(w1))


def fill1_kernel(rows_mine, zero, w2, order, table_in, puts, w2_v, table_g, mine_s, puts_s, s_zero, s_list, s_w):
    load = pltpu.make_async_copy(rows_mine, mine_s, s_list)
    load.start()
    load_w = pltpu.make_async_copy(w2, w2_v, s_w)
    load_w.start()
    fill_start(zero, table_g, s_zero, 1)
    tokens = rows_mine.shape[1]
    load.wait()

    def body(i, count):
        lid = mine_s[0, i]
        puts_s[count] = lid | (i << 16)
        return count + (lid >= 0).astype(I32)

    puts_s[tokens] = lax.fori_loop(0, tokens, body, 0, unroll=8)
    store = pltpu.make_async_copy(puts_s, puts, s_list)
    store.start()
    store.wait()
    load_w.wait()
    fill_wait(zero, table_g, s_zero, 1)


def fill1(rows_mine, zero, w2, order, table_g):
    tokens = rows_mine.shape[1]
    return pl.pallas_call(
        fill1_kernel,
        name="fill1",
        out_shape=[sh((2 * tokens,), I32), sh(w2.shape, BF), sh(table_g.shape, F32)],
        in_specs=[ANY_SPEC, VMEM_SPEC, HBM_SPEC, ANY_SPEC, HBM_SPEC],
        out_specs=[ANY_SPEC, VMEM_SPEC, HBM_SPEC],
        input_output_aliases={4: 2},
        scratch_shapes=[pltpu.SMEM((1, tokens), I32), pltpu.SMEM((2 * tokens,), I32), DMA(()), DMA(()), DMA(())],
        compiler_params=pltpu.CompilerParams(vmem_limit_bytes=8 * MIB),
        cost_estimate=pl.CostEstimate(flops=9_000_000_000, bytes_accessed=20 * MIB, transcendentals=0),
    )(rows_mine, zero, in_hbm(w2), order, table_g)


def mlp_half(x, d, n, h, du, at, w1, w2, gain):
    first, count = at
    width, hid = n.shape[1], h.shape[1]
    gain_f = gain[...].astype(F32).reshape(1, width)
    for j in range(count // 32):
        rows = pl.ds(first + j * 32, 32)
        x_f = x[rows, :].astype(F32)
        r = lax.rsqrt(jnp.mean(x_f * x_f, axis=-1, keepdims=True) + EPS)
        n[rows, :] = (x_f * r * gain_f).astype(BF)
    rows = pl.ds(first, count)
    for j in range(hid // TILE):
        cols = pl.ds(j * TILE, TILE)
        g = mm(d[rows, :], w2[cols, :], 1, 1).astype(BF).astype(F32)
        u = mm(n[rows, :], w1[:, cols], 1, 0).astype(BF).astype(F32)
        t = jnp.tanh(GELU_C * (u + GELU_A * (u * u * u)))
        cdf = 0.5 * (1.0 + t)
        h[rows, cols] = (u * cdf).astype(BF)
        du[rows, cols] = (g * (cdf + u * (0.5 * (1.0 - t * t)) * (GELU_C * (1.0 + 3.0 * GELU_A * (u * u))))).astype(BF)


def share_kernel(send, got, d_own, d_far, w1, w2, gain, x_f, d_full, n_a, h_a, du_a, x_r, d_r, sems):
    rows = d_own.shape[0]
    half = 2 * rows
    remote = swap_with_sibling()
    copies = []
    for k in range(2):
        at, other = pl.ds(k * rows, rows), pl.ds((1 - k) * rows, rows)
        x_f[at, :] = send[at, :] + got[other, :]
        copies.append(remote(x_f.at[at], x_r.at[at], sems, k))
        copies[-1].start()
    for k, src in enumerate((d_own, d_far)):
        copies.append(remote(src, d_r.at[pl.ds(k * rows, rows)], sems, 2 + k))
        copies[-1].start()
        d_full[pl.ds(k * rows, rows), :] = src[...]
    mlp_half(x_f, d_full, n_a, h_a, du_a, (0, half), w1, w2, gain)
    for k in range(2):
        copies[k].wait()
        x_f[pl.ds(half + k * rows, rows), :] = x_r[pl.ds(k * rows, rows), :]
    for k in range(2):
        copies[2 + k].wait()
        d_full[pl.ds(half + k * rows, rows), :] = d_r[pl.ds(k * rows, rows), :]


def share(send, got, d_own, d_far, w1, w2, gain):
    rows, width = d_own.shape
    hid = w1.shape[1]
    return pl.pallas_call(
        share_kernel,
        name="share",
        out_shape=[sh((4 * rows, width), BF)] * 2 + [sh((2 * rows, width), BF)] + [sh((2 * rows, hid), BF)] * 2,
        in_specs=[VMEM_SPEC] * 7,
        out_specs=[VMEM_SPEC] * 5,
        scratch_shapes=[VMEM((2 * rows, width), BF), VMEM((2 * rows, width), BF), DMA((2, 4))],
        compiler_params=pltpu.CompilerParams(collective_id=1, has_side_effects=True, vmem_limit_bytes=16 * MIB),
        cost_estimate=pl.CostEstimate(flops=3_000_000_000, bytes_accessed=MIB, transcendentals=0),
    )(send, got, d_own, d_far, w1, w2, gain)


def mlp_kernel(x_f, d_full, n_a, h_a, du_a, w1, w2, gain, zero, table_in, n, h, du, dn_p, table_g, s_zero):
    fill_start(zero, table_g, s_zero, 2)
    tokens, width = n.shape
    half = tokens // 2
    for out, src in ((n, n_a), (h, h_a), (du, du_a)):
        out[pl.ds(0, half), :] = src[...]
    mlp_half(x_f, d_full, n, h, du, (half, half), w1, w2, gain)
    for j in range(width // TILE):
        cols = pl.ds(j * TILE, TILE)
        dn_p[:, cols] = mm(du[pl.ds(half, half), :], w1[cols, :], 1, 1)
    fill_wait(zero, table_g, s_zero, 2)


def mlp(x_f, d_full, n_a, h_a, du_a, w1, w2, gain, zero, table_g):
    tokens, width = x_f.shape
    hid = w1.shape[1]
    return pl.pallas_call(
        mlp_kernel,
        name="mlp",
        out_shape=[sh((tokens, width), BF), sh((tokens, hid), BF), sh((tokens, hid), BF), sh((tokens // 2, width), F32),
                   sh(table_g.shape, F32)],
        in_specs=[VMEM_SPEC] * 9 + [HBM_SPEC],
        out_specs=[VMEM_SPEC] * 4 + [HBM_SPEC],
        input_output_aliases={9: 4},
        scratch_shapes=[DMA(())],
        compiler_params=pltpu.CompilerParams(vmem_limit_bytes=16 * MIB),
        cost_estimate=pl.CostEstimate(flops=6_000_000_000, bytes_accessed=4 * MIB, transcendentals=0),
    )(x_f, d_full, n_a, h_a, du_a, w1, w2, gain, zero, table_g)


def sums_kernel(dn_p, du, h, w1, w2, dn_own, dn_far, y_a, y_b, dn_r, dn_m, sems):
    rows, width = dn_own.shape
    half = 2 * rows
    remote = swap_with_sibling()
    copies = [remote(dn_p.at[pl.ds(k * rows, rows)], dn_r.at[pl.ds(k * rows, rows)], sems, k) for k in (1, 0)]
    for c in copies:
        c.start()
    for j in range(width // TILE):
        cols = pl.ds(j * TILE, TILE)
        dn_m[:, cols] = mm(du[pl.ds(0, half), :], w1[cols, :], 1, 1)
    for j in range(width // TILE):
        cols = pl.ds(j * TILE, TILE)
        y = mm(h[...], w2[:, cols], 1, 0)
        y_a[:, cols] = y[:half]
        y_b[:, cols] = y[half:]
    for c, out, k in zip(copies, (dn_far, dn_own), (1, 0)):
        c.wait()
        at = pl.ds(k * rows, rows)
        out[...] = dn_m[at, :] + dn_r[at, :]


def sums(dn_p, du, h, w1, w2):
    half, width = dn_p.shape
    rows = half // 2
    return pl.pallas_call(
        sums_kernel,
        name="sums",
        out_shape=[sh((rows, width), F32)] * 2 + [sh((half, width), F32)] * 2,
        in_specs=[VMEM_SPEC] * 5,
        out_specs=[VMEM_SPEC] * 4,
        scratch_shapes=[VMEM((half, width), F32), VMEM((half, width), F32), DMA((2, 2))],
        compiler_params=pltpu.CompilerParams(collective_id=2, has_side_effects=True, vmem_limit_bytes=16 * MIB),
        cost_estimate=pl.CostEstimate(flops=4_000_000_000, bytes_accessed=4 * MIB, transcendentals=0),
    )(dn_p, du, h, w1, w2)


def grads1_kernel(n, du, zero, order, table_in, dw1, table_g, dw1_v, s_zero, s_w):
    width = n.shape[1]
    n_t = n[...].T
    for j in range(width // TILE):
        at = slice(j * TILE, (j + 1) * TILE)
        dw1_v[at, :] = mm(n_t[at, :], du[...], 1, 0)
        pltpu.make_async_copy(dw1_v.at[pl.ds(j * TILE, TILE)], dw1.at[pl.ds(j * TILE, TILE)], s_w).start()
        if j == 0:
            fill_start(zero, table_g, s_zero, 3)
    pltpu.make_async_copy(dw1_v, dw1, s_w).wait()
    fill_wait(zero, table_g, s_zero, 3)


def grads1(n, du, zero, order, table_g):
    width, hid = n.shape[1], du.shape[1]
    return pl.pallas_call(
        grads1_kernel,
        name="grads1",
        out_shape=[sh((width, hid), F32), sh(table_g.shape, F32)],
        in_specs=[VMEM_SPEC] * 3 + [ANY_SPEC, HBM_SPEC],
        out_specs=[HBM_SPEC, HBM_SPEC],
        input_output_aliases={4: 1},
        scratch_shapes=[VMEM((width, hid), F32), DMA(()), DMA(())],
        compiler_params=pltpu.CompilerParams(vmem_limit_bytes=16 * MIB),
        cost_estimate=pl.CostEstimate(flops=4_000_000_000, bytes_accessed=8 * MIB, transcendentals=0),
    )(n, du, zero, order, table_g)


def grads2_kernel(h, d_full, y_a, y_sib, zero, table_in, dw2, y_own, y_far, table_g, dw2_v, s_zero, s_w):
    rows = y_own.shape[0]
    hid = h.shape[1]
    fill_start(zero, table_g, s_zero, 4)
    for k, out in enumerate((y_own, y_far)):
        at = pl.ds(k * rows, rows)
        out[...] = y_a[at, :] + y_sib[at, :]
    h_t = h[...].T
    for j in range(hid // TILE):
        at = slice(j * TILE, (j + 1) * TILE)
        dw2_v[at, :] = mm(h_t[at, :], d_full[...], 1, 0)
        pltpu.make_async_copy(dw2_v.at[pl.ds(j * TILE, TILE)], dw2.at[pl.ds(j * TILE, TILE)], s_w).start()
    pltpu.make_async_copy(dw2_v, dw2, s_w).wait()
    fill_wait(zero, table_g, s_zero, 4)


def grads2(h, d_full, y_a, y_sib, zero, table_g):
    hid, width = h.shape[1], d_full.shape[1]
    rows = y_a.shape[0] // 2
    return pl.pallas_call(
        grads2_kernel,
        name="grads2",
        out_shape=[sh((hid, width), F32)] + [sh((rows, width), F32)] * 2 + [sh(table_g.shape, F32)],
        in_specs=[VMEM_SPEC] * 5 + [HBM_SPEC],
        out_specs=[HBM_SPEC, VMEM_SPEC, VMEM_SPEC, HBM_SPEC],
        input_output_aliases={5: 3},
        scratch_shapes=[VMEM((hid, width), F32), DMA(()), DMA(())],
        compiler_params=pltpu.CompilerParams(vmem_limit_bytes=16 * MIB),
        cost_estimate=pl.CostEstimate(flops=4_000_000_000, bytes_accessed=8 * MIB, transcendentals=0),
    )(h, d_full, y_a, y_sib, zero, table_g)


def dx_kernel(dn_own, g2, x_own, d_own, gain, order, dx):
    gain_f = gain[...].astype(F32).reshape(1, dx.shape[1])
    for j in range(dx.shape[0] // 16):
        at = pl.ds(j * 16, 16)
        a = (dn_own[at, :] + g2[at, :]) * gain_f
        x = x_own[at, :].astype(F32)
        r = lax.rsqrt(jnp.mean(x * x, axis=-1, keepdims=True) + EPS)
        proj = jnp.mean(a * x, axis=-1, keepdims=True)
        dx[at, :] = (d_own[at, :].astype(F32) + r * (a - x * r * r * proj)).astype(BF)


def dx_rows(dn_own, g2, x_own, d_own, gain, order):
    return pl.pallas_call(
        dx_kernel,
        name="dx_rows",
        out_shape=sh(d_own.shape, BF),
        in_specs=[VMEM_SPEC] * 5 + [ANY_SPEC],
        out_specs=VMEM_SPEC,
        compiler_params=pltpu.CompilerParams(vmem_limit_bytes=4 * MIB),
        cost_estimate=pl.CostEstimate(flops=1_000_000_000, bytes_accessed=MIB, transcendentals=0),
    )(dn_own, g2, x_own, d_own, gain, order)


def fill3_kernel(zero, order, table_in, token, table_g, s_zero):
    fill_start(zero, table_g, s_zero, 5)
    token[...] = jnp.zeros_like(token)
    fill_wait(zero, table_g, s_zero, 5)


def fill3(zero, order, table_g):
    return pl.pallas_call(
        fill3_kernel,
        name="fill3",
        out_shape=[sh((8, 128), F32), sh(table_g.shape, F32)],
        in_specs=[VMEM_SPEC, ANY_SPEC, HBM_SPEC],
        out_specs=[VMEM_SPEC, HBM_SPEC],
        input_output_aliases={2: 1},
        scratch_shapes=[DMA(())],
        compiler_params=pltpu.CompilerParams(vmem_limit_bytes=4 * MIB),
        cost_estimate=pl.CostEstimate(flops=4_000_000_000, bytes_accessed=16 * MIB, transcendentals=0),
    )(zero, order, table_g)


def dx_all_kernel(dx, dx_far, order, dx_out, dx_r, sems):
    me = lax.axis_index("tp")
    rows = dx.shape[0]
    remote = swap_with_sibling()
    block = lambda m: pl.ds(pl.multiple_of((me ^ m) * rows, rows), rows)
    copies = [remote(src, dx_r.at[pl.ds(k * rows, rows)], sems, k) for k, src in enumerate((dx, dx_far))]
    for c in copies:
        c.start()
    dx_out[block(0), :] = dx[...]
    dx_out[block(2), :] = dx_far[...]
    for k, c in enumerate(copies):
        c.wait()
        dx_out[block(1 + 2 * k), :] = dx_r[pl.ds(k * rows, rows), :]


def dx_all(dx, dx_far, order):
    rows, width = dx.shape
    return pl.pallas_call(
        dx_all_kernel,
        name="dx_all",
        out_shape=sh((4 * rows, width), BF),
        in_specs=[VMEM_SPEC] * 2 + [ANY_SPEC],
        out_specs=VMEM_SPEC,
        scratch_shapes=[VMEM((2 * rows, width), BF), DMA((2, 2))],
        compiler_params=pltpu.CompilerParams(collective_id=3, has_side_effects=True, vmem_limit_bytes=4 * MIB),
        cost_estimate=pl.CostEstimate(flops=2_000_000_000, bytes_accessed=MIB, transcendentals=0),
    )(dx, dx_far, order)


def put_kernel(puts, same, dx, zero, table_in, table_g, token, puts_s, total, s_in, s_row, s_zero):
    fill_start(zero, table_g, s_zero, "late")
    tokens = dx.shape[0]
    load = pltpu.make_async_copy(puts, puts_s, s_in)
    load.start()
    total[...] = mm(same[...], dx[...], 1, 0)
    token[...] = jnp.zeros_like(token)
    load.wait()
    fill_wait(zero, table_g, s_zero, "late")
    count = puts_s[tokens]

    def put(i):
        word = puts_s[i]
        pltpu.make_async_copy(total.at[pl.ds(word >> 16, 1)], table_g.at[pl.ds(word & 0xFFFF, 1)], s_row).start()

    def put_four(i, carry):
        for k in range(4):
            put(i * 4 + k)
        return carry

    def put_one(i, carry):
        put(i)
        return carry

    lax.fori_loop(0, count >> 2, put_four, 0)
    lax.fori_loop((count >> 2) * 4, count, put_one, 0)

    def put_wait(size):
        def body(i, carry):
            pltpu.make_async_copy(total.at[pl.ds(0, size)], table_g.at[pl.ds(0, size)], s_row).wait()
            return carry

        return body

    lax.fori_loop(0, count >> 3, put_wait(8), 0)
    lax.fori_loop(0, count & 7, put_wait(1), 0)


def put_rows(puts, same, dx, zero, table_g):
    return pl.pallas_call(
        put_kernel,
        name="put_rows",
        out_shape=[sh(table_g.shape, F32), sh((8, 128), F32)],
        in_specs=[ANY_SPEC, VMEM_SPEC, VMEM_SPEC, VMEM_SPEC, HBM_SPEC],
        out_specs=[HBM_SPEC, VMEM_SPEC],
        input_output_aliases={4: 0},
        scratch_shapes=[pltpu.SMEM(puts.shape, I32), VMEM(dx.shape, F32), DMA(()), DMA(()), DMA(())],
        compiler_params=pltpu.CompilerParams(vmem_limit_bytes=4 * MIB),
        cost_estimate=pl.CostEstimate(flops=3_000_000_000, bytes_accessed=2 * MIB, transcendentals=0),
    )(puts, same, dx, zero, table_g)


def finish_kernel(x, y, y_in, order, out):
    out[...] = (x[pl.ds(0, out.shape[0]), :].astype(F32) + (y[...] + y_in[...])).astype(BF)


def finish(x, y, y_in, order):
    return pl.pallas_call(
        finish_kernel,
        name="finish",
        out_shape=sh(y.shape, BF),
        in_specs=[VMEM_SPEC] * 3 + [ANY_SPEC],
        out_specs=VMEM_SPEC,
        compiler_params=pltpu.CompilerParams(vmem_limit_bytes=4 * MIB),
        cost_estimate=pl.CostEstimate(flops=1_000_000_000, bytes_accessed=MIB, transcendentals=0),
    )(x, y, y_in, order)


def solution(mesh):
    tp = mesh.shape["tp"]

    def permute(x, hop):
        return lax.ppermute(x, "tp", [(i, i ^ hop) for i in range(tp)])

    def shard_step(ids, table, gain, w1, w2, d_out):
        d_far = permute(d_out, 2)
        part, rows_mine, same, zero, d_table = lookup(ids, table)
        send, w1 = pair(part, w1)
        got = permute(send, 2)
        puts, w2, d_table = fill1(rows_mine, zero, w2, send, d_table)
        x_f, d_full, n_a, h_a, du_a = share(send, got, d_out, d_far, w1, w2, gain)
        n, h, du, dn_p, d_table = mlp(x_f, d_full, n_a, h_a, du_a, w1, w2, gain, zero, d_table)
        dn_own, dn_far, y_a, y_b = sums(dn_p, du, h, w1, w2)
        g2 = permute(dn_far, 2)
        y_sib = permute(y_b, 1)
        d_w1, d_table = grads1(n, du, zero, dn_own, d_table)
        d_w2, y_own, y_far, d_table = grads2(h, d_full, y_a, y_sib, zero, d_table)
        dx = dx_rows(dn_own, g2, x_f, d_out, gain, y_own)
        dx_far = permute(dx, 2)
        dx, y_far = lax.optimization_barrier((dx, y_far))
        y_in = permute(y_far, 2)
        token, d_table = fill3(zero, dx, d_table)
        dx_full = dx_all(dx, dx_far, token)
        d_table, done = put_rows(puts, same, dx_full, zero, d_table)
        out = finish(x_f, y_own, y_in, done)
        return out, d_table, d_w1, d_w2

    return jax.shard_map(
        shard_step,
        mesh=mesh,
        in_specs=(P("dp"), P("tp", None), P(None), P(None, "tp"), P("tp", None), P(("dp", "tp"), None)),
        out_specs=(P(("dp", "tp"), None), P(("dp", "tp"), None), P("dp", "tp"), P(("dp", "tp"), None)),
        check_vma=False,
    )
```

```python
import jax
import jax.numpy as jnp
from jax import lax
from jax.experimental import pallas as pl
from jax.experimental.pallas import tpu as pltpu
from jax.sharding import PartitionSpec as P

EPS = 1e-6
BF = jnp.bfloat16
F32 = jnp.float32
I32 = jnp.int32
GELU_C = 0.7978845608028654
GELU_A = 0.044715
VMEM = pltpu.VMEM
SMEM_SPEC = pl.BlockSpec(memory_space=pltpu.SMEM)
ANY_SPEC = pl.BlockSpec(memory_space=pl.ANY)
HBM_SPEC = pl.BlockSpec(memory_space=pltpu.HBM)
VMEM_SPEC = pl.BlockSpec(memory_space=VMEM)
DMA = pltpu.SemaphoreType.DMA
TILE = 256
ZERO_ROWS = 96
FILL_AT = (0, 4, 69, 82, 93, 102, 131)
LATE_FILL = (5, 13)
MIB = 1 << 20
LOOKUP_VMEM = 48 * MIB
PAIR_VMEM = 8 * MIB


def mm(a, b, ca, cb):
    return lax.dot_general(a, b, (((ca,), (cb,)), ((), ())), preferred_element_type=F32)


def in_hbm(x):
    return pltpu.with_memory_space_constraint(x, pltpu.HBM)


def sh(shape, dtype):
    return jax.ShapeDtypeStruct(shape, dtype)


def fill_copy(zero, table_g, sem, i):
    return pltpu.make_async_copy(zero, table_g.at[pl.ds(pl.multiple_of(i * ZERO_ROWS, ZERO_ROWS), ZERO_ROWS)], sem)


def fill_range(part):
    late = LATE_FILL[0] + (lax.axis_index("tp") >> 1) * (LATE_FILL[1] - LATE_FILL[0])
    if part == "late":
        return FILL_AT[2] - late, FILL_AT[2]
    return FILL_AT[part], FILL_AT[part + 1] - (late if part == 1 else 0)


def fill_start(zero, table_g, sem, part):
    def body(i, carry):
        fill_copy(zero, table_g, sem, i).start()
        return carry

    lax.fori_loop(*fill_range(part), body, 0)


def fill_wait(zero, table_g, sem, part):
    def body(i, carry):
        fill_copy(zero, table_g, sem, i).wait()
        return carry

    lax.fori_loop(*fill_range(part), body, 0)


def swap_with_sibling():
    sib = lax.axis_index("tp") ^ 1
    barrier = pltpu.get_barrier_semaphore()
    pl.semaphore_signal(barrier, inc=1, device_id={"tp": sib}, device_id_type=pl.DeviceIdType.MESH)
    pl.semaphore_wait(barrier, 1)

    def remote(src, dst, sems, i):
        return pltpu.make_async_remote_copy(
            src_ref=src, dst_ref=dst, send_sem=sems.at[0, i], recv_sem=sems.at[1, i],
            device_id={"tp": sib}, device_id_type=pl.DeviceIdType.MESH)

    return remote


def lookup_kernel(ids, ids_row, table, part, rows_mine, same, zero, table_g, ids_s, ids_v, pairs, sems, s_zero, s_ids):
    tokens, vocab = part.shape[0], table.shape[0]
    base = lax.axis_index("tp") * vocab
    group = 64
    groups = tokens // group
    loads = [pltpu.make_async_copy(ids, ids_s, s_ids.at[0]), pltpu.make_async_copy(ids_row, ids_v, s_ids.at[1])]
    for c in loads:
        c.start()
    zero[...] = jnp.zeros_like(zero)
    fill_start(zero, table_g, s_zero, 0)
    loads[0].wait()

    def fetch(k, carry):
        for i in range(group):
            token = k * group + i
            lid = ids_s[token] - base
            owned = (lid >= 0) & (lid < vocab)
            row = jnp.where(owned, lid & -2, 2 * token)
            pltpu.make_async_copy(table.at[pl.ds(pl.multiple_of(row, 2), 2)], pairs.at[k, pl.ds(2 * i, 2)], sems.at[k]).start()
        return carry

    lax.fori_loop(0, groups, fetch, 0)
    loads[1].wait()
    row = jnp.broadcast_to(ids_v[...].astype(F32), (tokens, tokens))
    col = row.T
    equal = row == col
    same[...] = jnp.where(equal, 1.0, 0.0).astype(BF)
    earlier = lax.broadcasted_iota(I32, (tokens, tokens), 0) < lax.broadcasted_iota(I32, (tokens, tokens), 1)
    repeat = jnp.max(jnp.where(equal & earlier, 1, 0), axis=0, keepdims=True)
    mine = ids_v[...] - base
    rows_mine[...] = jnp.where((mine >= 0) & (mine < vocab) & (repeat == 0), mine, -1)
    lid = col.astype(I32) - base
    lane = lax.broadcasted_iota(I32, (group, 2 * group), 1)
    first = lax.broadcasted_iota(I32, (group, 2 * group), 0) * 2
    for k in range(groups):
        at = lid[k * group:(k + 1) * group, :2 * group]
        owned = (at >= 0) & (at < vocab)
        pick = jnp.where(owned & (lane == first + (at & 1)), 1.0, 0.0).astype(BF)
        pltpu.make_async_copy(table.at[pl.ds(0, group * 2)], pairs.at[k], sems.at[k]).wait()
        part[pl.ds(k * group, group), :] = mm(pick, pairs[k], 1, 0).astype(BF)
    fill_wait(zero, table_g, s_zero, 0)


def lookup(ids, table):
    tokens, (vocab, width) = ids.shape[0], table.shape
    return pl.pallas_call(
        lookup_kernel,
        name="lookup",
        out_shape=[sh((tokens, width), BF), sh((1, tokens), I32), sh((tokens, tokens), BF), sh((ZERO_ROWS, width), F32), sh((vocab, width), F32)],
        in_specs=[HBM_SPEC] * 3,
        out_specs=[VMEM_SPEC] * 4 + [HBM_SPEC],
        scratch_shapes=[pltpu.SMEM((tokens,), I32), VMEM((1, tokens), I32), VMEM((4, tokens // 2, width), BF), DMA((4,)), DMA(()), DMA((2,))],
        compiler_params=pltpu.CompilerParams(vmem_limit_bytes=LOOKUP_VMEM),
        cost_estimate=pl.CostEstimate(flops=5_000_000_000, bytes_accessed=10 * MIB, transcendentals=0),
    )(in_hbm(ids), in_hbm(ids.reshape(1, tokens)), in_hbm(table))


def pair_kernel(part, w1, send, w1_v, part_r, sems, s_in):
    me = lax.axis_index("tp")
    rows = part.shape[0] // 4
    blocks = (me, me ^ 2, me ^ 1, me ^ 3)
    load = pltpu.make_async_copy(w1, w1_v, s_in)
    load.start()
    remote = swap_with_sibling()
    block = lambda k: pl.ds(pl.multiple_of(blocks[k] * rows, rows), rows)
    copies = [remote(part.at[block(2 + k)], part_r.at[pl.ds(k * rows, rows)], sems, k) for k in range(2)]
    for c in copies:
        c.start()
    for k in range(2):
        copies[k].wait()
        at = pl.ds(k * rows, rows)
        send[at, :] = part[block(k), :] + part_r[at, :]
    load.wait()


def pair(part, w1):
    rows, width = part.shape[0] // 4, part.shape[1]
    return pl.pallas_call(
        pair_kernel,
        name="pair",
        out_shape=[sh((2 * rows, width), BF), sh(w1.shape, BF)],
        in_specs=[VMEM_SPEC, HBM_SPEC],
        out_specs=[VMEM_SPEC] * 2,
        scratch_shapes=[VMEM((2 * rows, width), BF), DMA((2, 2)), DMA(())],
        compiler_params=pltpu.CompilerParams(collective_id=0, has_side_effects=True, vmem_limit_bytes=PAIR_VMEM),
        cost_estimate=pl.CostEstimate(flops=3_000_000_000, bytes_accessed=MIB, transcendentals=0),
    )(part, in_hbm(w1))


def fill1_kernel(rows_mine, zero, w2, order, table_in, puts, w2_v, table_g, mine_s, puts_s, s_zero, s_list, s_w):
    load = pltpu.make_async_copy(rows_mine, mine_s, s_list)
    load.start()
    load_w = pltpu.make_async_copy(w2, w2_v, s_w)
    load_w.start()
    fill_start(zero, table_g, s_zero, 1)
    tokens = rows_mine.shape[1]
    load.wait()

    def body(i, count):
        lid = mine_s[0, i]
        puts_s[count] = lid | (i << 16)
        return count + (lid >= 0).astype(I32)

    puts_s[tokens] = lax.fori_loop(0, tokens, body, 0, unroll=8)
    store = pltpu.make_async_copy(puts_s, puts, s_list)
    store.start()
    store.wait()
    load_w.wait()
    fill_wait(zero, table_g, s_zero, 1)


def fill1(rows_mine, zero, w2, order, table_g):
    tokens = rows_mine.shape[1]
    return pl.pallas_call(
        fill1_kernel,
        name="fill1",
        out_shape=[sh((2 * tokens,), I32), sh(w2.shape, BF), sh(table_g.shape, F32)],
        in_specs=[ANY_SPEC, VMEM_SPEC, HBM_SPEC, ANY_SPEC, HBM_SPEC],
        out_specs=[ANY_SPEC, VMEM_SPEC, HBM_SPEC],
        input_output_aliases={4: 2},
        scratch_shapes=[pltpu.SMEM((1, tokens), I32), pltpu.SMEM((2 * tokens,), I32), DMA(()), DMA(()), DMA(())],
        compiler_params=pltpu.CompilerParams(vmem_limit_bytes=8 * MIB),
        cost_estimate=pl.CostEstimate(flops=9_000_000_000, bytes_accessed=20 * MIB, transcendentals=0),
    )(rows_mine, zero, in_hbm(w2), order, table_g)


def mlp_half(x, d, n, h, du, at, w1, w2, gain):
    first, count = at
    width, hid = n.shape[1], h.shape[1]
    gain_f = gain[...].astype(F32).reshape(1, width)
    for j in range(count // 32):
        rows = pl.ds(first + j * 32, 32)
        x_f = x[rows, :].astype(F32)
        r = lax.rsqrt(jnp.mean(x_f * x_f, axis=-1, keepdims=True) + EPS)
        n[rows, :] = (x_f * r * gain_f).astype(BF)
    rows = pl.ds(first, count)
    for j in range(hid // TILE):
        cols = pl.ds(j * TILE, TILE)
        g = mm(d[rows, :], w2[cols, :], 1, 1).astype(BF).astype(F32)
        u = mm(n[rows, :], w1[:, cols], 1, 0).astype(BF).astype(F32)
        t = jnp.tanh(GELU_C * (u + GELU_A * (u * u * u)))
        cdf = 0.5 * (1.0 + t)
        h[rows, cols] = (u * cdf).astype(BF)
        du[rows, cols] = (g * (cdf + u * (0.5 * (1.0 - t * t)) * (GELU_C * (1.0 + 3.0 * GELU_A * (u * u))))).astype(BF)


def share_kernel(send, got, d_own, d_far, d_own_s, d_far_s, w1, w2, gain, x_f, d_full, n_a, h_a, du_a, x_r, sems):
    rows = d_own.shape[0]
    half = 2 * rows
    remote = swap_with_sibling()
    copies = []
    for k in range(2):
        at, other = pl.ds(k * rows, rows), pl.ds((1 - k) * rows, rows)
        x_f[at, :] = send[at, :] + got[other, :]
        copies.append(remote(x_f.at[at], x_r.at[at], sems, k))
        copies[-1].start()
    for k, src in enumerate((d_own, d_far, d_own_s, d_far_s)):
        d_full[pl.ds(k * rows, rows), :] = src[...]
    mlp_half(x_f, d_full, n_a, h_a, du_a, (0, half), w1, w2, gain)
    for k in range(2):
        copies[k].wait()
        x_f[pl.ds(half + k * rows, rows), :] = x_r[pl.ds(k * rows, rows), :]


def share(send, got, ds, w1, w2, gain):
    rows, width = ds[0].shape
    hid = w1.shape[1]
    return pl.pallas_call(
        share_kernel,
        name="share",
        out_shape=[sh((4 * rows, width), BF)] * 2 + [sh((2 * rows, width), BF)] + [sh((2 * rows, hid), BF)] * 2,
        in_specs=[VMEM_SPEC] * 9,
        out_specs=[VMEM_SPEC] * 5,
        scratch_shapes=[VMEM((2 * rows, width), BF), DMA((2, 2))],
        compiler_params=pltpu.CompilerParams(collective_id=1, has_side_effects=True, vmem_limit_bytes=16 * MIB),
        cost_estimate=pl.CostEstimate(flops=3_000_000_000, bytes_accessed=MIB, transcendentals=0),
    )(send, got, *ds, w1, w2, gain)


def mlp_kernel(x_f, d_full, n_a, h_a, du_a, w1, w2, gain, zero, table_in, n, h, du, dn_b0, dn_b1, table_g, s_zero):
    fill_start(zero, table_g, s_zero, 2)
    tokens, width = n.shape
    half = tokens // 2
    for out, src in ((n, n_a), (h, h_a), (du, du_a)):
        out[pl.ds(0, half), :] = src[...]
    mlp_half(x_f, d_full, n, h, du, (half, half), w1, w2, gain)
    for j in range(width // TILE):
        cols = pl.ds(j * TILE, TILE)
        dn = mm(du[pl.ds(half, half), :], w1[cols, :], 1, 1)
        dn_b0[:, cols] = dn[:half // 2]
        dn_b1[:, cols] = dn[half // 2:]
    fill_wait(zero, table_g, s_zero, 2)


def mlp(x_f, d_full, n_a, h_a, du_a, w1, w2, gain, zero, table_g):
    tokens, width = x_f.shape
    hid = w1.shape[1]
    return pl.pallas_call(
        mlp_kernel,
        name="mlp",
        out_shape=[sh((tokens, width), BF), sh((tokens, hid), BF), sh((tokens, hid), BF), sh((tokens // 4, width), F32),
                   sh((tokens // 4, width), F32), sh(table_g.shape, F32)],
        in_specs=[VMEM_SPEC] * 9 + [HBM_SPEC],
        out_specs=[VMEM_SPEC] * 5 + [HBM_SPEC],
        input_output_aliases={9: 5},
        scratch_shapes=[DMA(())],
        compiler_params=pltpu.CompilerParams(vmem_limit_bytes=16 * MIB),
        cost_estimate=pl.CostEstimate(flops=6_000_000_000, bytes_accessed=4 * MIB, transcendentals=0),
    )(x_f, d_full, n_a, h_a, du_a, w1, w2, gain, zero, table_g)


def sums_kernel(dn_b1, du, h, w1, w2, dn_own, dn_far, y_a, y_b, dn_r, sems):
    rows, width = dn_own.shape
    half = 2 * rows
    remote = swap_with_sibling()
    copy = remote(dn_b1, dn_r, sems, 0)
    copy.start()
    for j in range(width // TILE):
        cols = pl.ds(j * TILE, TILE)
        dn = mm(du[pl.ds(0, half), :], w1[cols, :], 1, 1)
        dn_own[:, cols] = dn[:rows]
        dn_far[:, cols] = dn[rows:]
    for j in range(width // TILE):
        cols = pl.ds(j * TILE, TILE)
        y = mm(h[...], w2[:, cols], 1, 0)
        y_a[:, cols] = y[:half]
        y_b[:, cols] = y[half:]
    copy.wait()
    dn_far[...] += dn_r[...]


def sums(dn_b1, du, h, w1, w2):
    rows, width = dn_b1.shape
    return pl.pallas_call(
        sums_kernel,
        name="sums",
        out_shape=[sh((rows, width), F32)] * 2 + [sh((2 * rows, width), F32)] * 2,
        in_specs=[VMEM_SPEC] * 5,
        out_specs=[VMEM_SPEC] * 4,
        scratch_shapes=[VMEM((rows, width), F32), DMA((2, 1))],
        compiler_params=pltpu.CompilerParams(collective_id=2, has_side_effects=True, vmem_limit_bytes=16 * MIB),
        cost_estimate=pl.CostEstimate(flops=4_000_000_000, bytes_accessed=4 * MIB, transcendentals=0),
    )(dn_b1, du, h, w1, w2)


def grads1_kernel(n, du, zero, order, table_in, dw1, table_g, dw1_v, s_zero, s_w):
    width = n.shape[1]
    n_t = n[...].T
    for j in range(width // TILE):
        at = slice(j * TILE, (j + 1) * TILE)
        dw1_v[at, :] = mm(n_t[at, :], du[...], 1, 0)
        pltpu.make_async_copy(dw1_v.at[pl.ds(j * TILE, TILE)], dw1.at[pl.ds(j * TILE, TILE)], s_w).start()
        if j == 0:
            fill_start(zero, table_g, s_zero, 3)
    pltpu.make_async_copy(dw1_v, dw1, s_w).wait()
    fill_wait(zero, table_g, s_zero, 3)


def grads1(n, du, zero, order, table_g):
    width, hid = n.shape[1], du.shape[1]
    return pl.pallas_call(
        grads1_kernel,
        name="grads1",
        out_shape=[sh((width, hid), F32), sh(table_g.shape, F32)],
        in_specs=[VMEM_SPEC] * 3 + [ANY_SPEC, HBM_SPEC],
        out_specs=[HBM_SPEC, HBM_SPEC],
        input_output_aliases={4: 1},
        scratch_shapes=[VMEM((width, hid), F32), DMA(()), DMA(())],
        compiler_params=pltpu.CompilerParams(vmem_limit_bytes=16 * MIB),
        cost_estimate=pl.CostEstimate(flops=4_000_000_000, bytes_accessed=8 * MIB, transcendentals=0),
    )(n, du, zero, order, table_g)


def grads2_kernel(h, d_full, y_a, y_sib, zero, table_in, dw2, y_own, y_far, table_g, dw2_v, s_zero, s_w):
    rows = y_own.shape[0]
    hid = h.shape[1]
    fill_start(zero, table_g, s_zero, 4)
    for k, out in enumerate((y_own, y_far)):
        at = pl.ds(k * rows, rows)
        out[...] = y_a[at, :] + y_sib[at, :]
    h_t = h[...].T
    for j in range(hid // TILE):
        at = slice(j * TILE, (j + 1) * TILE)
        dw2_v[at, :] = mm(h_t[at, :], d_full[...], 1, 0)
        pltpu.make_async_copy(dw2_v.at[pl.ds(j * TILE, TILE)], dw2.at[pl.ds(j * TILE, TILE)], s_w).start()
    pltpu.make_async_copy(dw2_v, dw2, s_w).wait()
    fill_wait(zero, table_g, s_zero, 4)


def grads2(h, d_full, y_a, y_sib, zero, table_g):
    hid, width = h.shape[1], d_full.shape[1]
    rows = y_a.shape[0] // 2
    return pl.pallas_call(
        grads2_kernel,
        name="grads2",
        out_shape=[sh((hid, width), F32)] + [sh((rows, width), F32)] * 2 + [sh(table_g.shape, F32)],
        in_specs=[VMEM_SPEC] * 5 + [HBM_SPEC],
        out_specs=[HBM_SPEC, VMEM_SPEC, VMEM_SPEC, HBM_SPEC],
        input_output_aliases={5: 3},
        scratch_shapes=[VMEM((hid, width), F32), DMA(()), DMA(())],
        compiler_params=pltpu.CompilerParams(vmem_limit_bytes=16 * MIB),
        cost_estimate=pl.CostEstimate(flops=4_000_000_000, bytes_accessed=8 * MIB, transcendentals=0),
    )(h, d_full, y_a, y_sib, zero, table_g)


def dx_kernel(dn_own, dn_sib, g2, x_own, d_own, gain, order, dx):
    gain_f = gain[...].astype(F32).reshape(1, dx.shape[1])
    for j in range(dx.shape[0] // 16):
        at = pl.ds(j * 16, 16)
        a = (dn_own[at, :] + dn_sib[at, :] + g2[at, :]) * gain_f
        x = x_own[at, :].astype(F32)
        r = lax.rsqrt(jnp.mean(x * x, axis=-1, keepdims=True) + EPS)
        proj = jnp.mean(a * x, axis=-1, keepdims=True)
        dx[at, :] = (d_own[at, :].astype(F32) + r * (a - x * r * r * proj)).astype(BF)


def dx_rows(dn_own, dn_sib, g2, x_own, d_own, gain, order):
    return pl.pallas_call(
        dx_kernel,
        name="dx_rows",
        out_shape=sh(d_own.shape, BF),
        in_specs=[VMEM_SPEC] * 6 + [ANY_SPEC],
        out_specs=VMEM_SPEC,
        compiler_params=pltpu.CompilerParams(vmem_limit_bytes=4 * MIB),
        cost_estimate=pl.CostEstimate(flops=1_000_000_000, bytes_accessed=MIB, transcendentals=0),
    )(dn_own, dn_sib, g2, x_own, d_own, gain, order)


def fill3_kernel(zero, order, table_in, token, table_g, s_zero):
    fill_start(zero, table_g, s_zero, 5)
    token[...] = jnp.zeros_like(token)
    fill_wait(zero, table_g, s_zero, 5)


def fill3(zero, order, table_g):
    return pl.pallas_call(
        fill3_kernel,
        name="fill3",
        out_shape=[sh((8, 128), F32), sh(table_g.shape, F32)],
        in_specs=[VMEM_SPEC, ANY_SPEC, HBM_SPEC],
        out_specs=[VMEM_SPEC, HBM_SPEC],
        input_output_aliases={2: 1},
        scratch_shapes=[DMA(())],
        compiler_params=pltpu.CompilerParams(vmem_limit_bytes=4 * MIB),
        cost_estimate=pl.CostEstimate(flops=4_000_000_000, bytes_accessed=16 * MIB, transcendentals=0),
    )(zero, order, table_g)


def dx_all_kernel(dx, dx_sib, dx_far, order, dx_out, dx_r, sems):
    me = lax.axis_index("tp")
    rows = dx.shape[0]
    remote = swap_with_sibling()
    block = lambda m: pl.ds(pl.multiple_of((me ^ m) * rows, rows), rows)
    copy = remote(dx_far, dx_r, sems, 0)
    copy.start()
    for m, src in enumerate((dx, dx_sib, dx_far)):
        dx_out[block(m), :] = src[...]
    copy.wait()
    dx_out[block(3), :] = dx_r[...]


def dx_all(dx, dx_sib, dx_far, order):
    rows, width = dx.shape
    return pl.pallas_call(
        dx_all_kernel,
        name="dx_all",
        out_shape=sh((4 * rows, width), BF),
        in_specs=[VMEM_SPEC] * 3 + [ANY_SPEC],
        out_specs=VMEM_SPEC,
        scratch_shapes=[VMEM((rows, width), BF), DMA((2, 1))],
        compiler_params=pltpu.CompilerParams(collective_id=3, has_side_effects=True, vmem_limit_bytes=4 * MIB),
        cost_estimate=pl.CostEstimate(flops=2_000_000_000, bytes_accessed=MIB, transcendentals=0),
    )(dx, dx_sib, dx_far, order)


def put_kernel(puts, same, dx, zero, table_in, table_g, token, puts_s, total, s_in, s_row, s_zero):
    fill_start(zero, table_g, s_zero, "late")
    tokens = dx.shape[0]
    load = pltpu.make_async_copy(puts, puts_s, s_in)
    load.start()
    total[...] = mm(same[...], dx[...], 1, 0)
    token[...] = jnp.zeros_like(token)
    load.wait()
    fill_wait(zero, table_g, s_zero, "late")
    count = puts_s[tokens]

    def put(i):
        word = puts_s[i]
        pltpu.make_async_copy(total.at[pl.ds(word >> 16, 1)], table_g.at[pl.ds(word & 0xFFFF, 1)], s_row).start()

    def put_four(i, carry):
        for k in range(4):
            put(i * 4 + k)
        return carry

    def put_one(i, carry):
        put(i)
        return carry

    lax.fori_loop(0, count >> 2, put_four, 0)
    lax.fori_loop((count >> 2) * 4, count, put_one, 0)

    def put_wait(size):
        def body(i, carry):
            pltpu.make_async_copy(total.at[pl.ds(0, size)], table_g.at[pl.ds(0, size)], s_row).wait()
            return carry

        return body

    lax.fori_loop(0, count >> 3, put_wait(8), 0)
    lax.fori_loop(0, count & 7, put_wait(1), 0)


def put_rows(puts, same, dx, zero, table_g):
    return pl.pallas_call(
        put_kernel,
        name="put_rows",
        out_shape=[sh(table_g.shape, F32), sh((8, 128), F32)],
        in_specs=[ANY_SPEC, VMEM_SPEC, VMEM_SPEC, VMEM_SPEC, HBM_SPEC],
        out_specs=[HBM_SPEC, VMEM_SPEC],
        input_output_aliases={4: 0},
        scratch_shapes=[pltpu.SMEM(puts.shape, I32), VMEM(dx.shape, F32), DMA(()), DMA(()), DMA(())],
        compiler_params=pltpu.CompilerParams(vmem_limit_bytes=4 * MIB),
        cost_estimate=pl.CostEstimate(flops=3_000_000_000, bytes_accessed=2 * MIB, transcendentals=0),
    )(puts, same, dx, zero, table_g)


def finish_kernel(x, y, y_in, order, out):
    out[...] = (x[pl.ds(0, out.shape[0]), :].astype(F32) + (y[...] + y_in[...])).astype(BF)


def finish(x, y, y_in, order):
    return pl.pallas_call(
        finish_kernel,
        name="finish",
        out_shape=sh(y.shape, BF),
        in_specs=[VMEM_SPEC] * 3 + [ANY_SPEC],
        out_specs=VMEM_SPEC,
        compiler_params=pltpu.CompilerParams(vmem_limit_bytes=4 * MIB),
        cost_estimate=pl.CostEstimate(flops=1_000_000_000, bytes_accessed=MIB, transcendentals=0),
    )(x, y, y_in, order)


def solution(mesh):
    tp = mesh.shape["tp"]

    def permute(x, hop):
        return lax.ppermute(x, "tp", [(i, i ^ hop) for i in range(tp)])

    def shard_step(ids, table, gain, w1, w2, d_out):
        d_far = permute(d_out, 2)
        part, rows_mine, same, zero, d_table = lookup(ids, table)
        send, w1 = pair(part, w1)
        got = permute(send, 2)
        ds = (d_out, d_far, permute(d_out, 1), permute(d_far, 1))
        puts, w2, d_table = fill1(rows_mine, zero, w2, send, d_table)
        x_f, d_full, n_a, h_a, du_a = share(send, got, ds, w1, w2, gain)
        n, h, du, dn_b0, dn_b1, d_table = mlp(x_f, d_full, n_a, h_a, du_a, w1, w2, gain, zero, d_table)
        dn_own, dn_far, y_a, y_b = sums(dn_b1, du, h, w1, w2)
        g2 = permute(dn_far, 2)
        dn_sib = permute(dn_b0, 1)
        y_sib = permute(y_b, 1)
        d_w1, d_table = grads1(n, du, zero, dn_own, d_table)
        d_w2, y_own, y_far, d_table = grads2(h, d_full, y_a, y_sib, zero, d_table)
        dx = dx_rows(dn_own, dn_sib, g2, x_f, d_out, gain, y_own)
        dx_far = permute(dx, 2)
        dx_sib = permute(dx, 1)
        dx, y_far = lax.optimization_barrier((dx, y_far))
        y_in = permute(y_far, 2)
        token, d_table = fill3(zero, dx, d_table)
        dx_full = dx_all(dx, dx_sib, dx_far, token)
        d_table, done = put_rows(puts, same, dx_full, zero, d_table)
        out = finish(x_f, y_own, y_in, done)
        return out, d_table, d_w1, d_w2

    return jax.shard_map(
        shard_step,
        mesh=mesh,
        in_specs=(P("dp"), P("tp", None), P(None), P(None, "tp"), P("tp", None), P(("dp", "tp"), None)),
        out_specs=(P(("dp", "tp"), None), P(("dp", "tp"), None), P("dp", "tp"), P(("dp", "tp"), None)),
        check_vma=False,
    )
```

```python
import jax
import jax.numpy as jnp
from jax import lax
from jax.experimental import pallas as pl
from jax.experimental.pallas import tpu as pltpu
from jax.sharding import PartitionSpec as P

EPS = 1e-6
BF = jnp.bfloat16
F32 = jnp.float32
I32 = jnp.int32
GELU_C = 0.7978845608028654
GELU_A = 0.044715
VMEM = pltpu.VMEM
SMEM_SPEC = pl.BlockSpec(memory_space=pltpu.SMEM)
ANY_SPEC = pl.BlockSpec(memory_space=pl.ANY)
HBM_SPEC = pl.BlockSpec(memory_space=pltpu.HBM)
VMEM_SPEC = pl.BlockSpec(memory_space=VMEM)
DMA = pltpu.SemaphoreType.DMA
TILE = 256
ZERO_ROWS = 96
FILL_COUNTS = ((22, 54, 13, 8, 8, 21, 5), (4, 50, 13, 9, 9, 23, 23))
LATE = 6
MIB = 1 << 20
LOOKUP_VMEM = 48 * MIB
PAIR_VMEM = 8 * MIB


def mm(a, b, ca, cb):
    return lax.dot_general(a, b, (((ca,), (cb,)), ((), ())), preferred_element_type=F32)


def in_hbm(x):
    return pltpu.with_memory_space_constraint(x, pltpu.HBM)


def sh(shape, dtype):
    return jax.ShapeDtypeStruct(shape, dtype)


def fill_copy(zero, table_g, sem, i):
    return pltpu.make_async_copy(zero, table_g.at[pl.ds(pl.multiple_of(i * ZERO_ROWS, ZERO_ROWS), ZERO_ROWS)], sem)


def fill_range(part):
    chip = lax.axis_index("tp") >> 1
    (lo0, hi0), (lo1, hi1) = ((sum(c[:part]), sum(c[:part + 1])) for c in FILL_COUNTS)
    return lo0 + chip * (lo1 - lo0), hi0 + chip * (hi1 - hi0)


def fill_start(zero, table_g, sem, part):
    def body(i, carry):
        fill_copy(zero, table_g, sem, i).start()
        return carry

    lax.fori_loop(*fill_range(part), body, 0)


def fill_wait(zero, table_g, sem, part):
    def body(i, carry):
        fill_copy(zero, table_g, sem, i).wait()
        return carry

    lax.fori_loop(*fill_range(part), body, 0)


def swap_with_sibling():
    sib = lax.axis_index("tp") ^ 1
    barrier = pltpu.get_barrier_semaphore()
    pl.semaphore_signal(barrier, inc=1, device_id={"tp": sib}, device_id_type=pl.DeviceIdType.MESH)
    pl.semaphore_wait(barrier, 1)

    def remote(src, dst, sems, i):
        return pltpu.make_async_remote_copy(
            src_ref=src, dst_ref=dst, send_sem=sems.at[0, i], recv_sem=sems.at[1, i],
            device_id={"tp": sib}, device_id_type=pl.DeviceIdType.MESH)

    return remote


def lookup_kernel(ids, ids_row, table, part, rows_mine, same, zero, table_g, ids_s, ids_v, pairs, sems, s_zero, s_ids):
    tokens, vocab = part.shape[0], table.shape[0]
    base = lax.axis_index("tp") * vocab
    group = 64
    groups = tokens // group
    loads = [pltpu.make_async_copy(ids, ids_s, s_ids.at[0]), pltpu.make_async_copy(ids_row, ids_v, s_ids.at[1])]
    for c in loads:
        c.start()
    zero[...] = jnp.zeros_like(zero)
    fill_start(zero, table_g, s_zero, 0)
    loads[0].wait()

    def fetch(k, carry):
        for i in range(group):
            token = k * group + i
            lid = ids_s[token] - base
            owned = (lid >= 0) & (lid < vocab)
            row = jnp.where(owned, lid & -2, 2 * token)
            pltpu.make_async_copy(table.at[pl.ds(pl.multiple_of(row, 2), 2)], pairs.at[k, pl.ds(2 * i, 2)], sems.at[k]).start()
        return carry

    lax.fori_loop(0, groups, fetch, 0)
    loads[1].wait()
    row = jnp.broadcast_to(ids_v[...].astype(F32), (tokens, tokens))
    col = row.T
    equal = row == col
    same[...] = jnp.where(equal, 1.0, 0.0).astype(BF)
    earlier = lax.broadcasted_iota(I32, (tokens, tokens), 0) < lax.broadcasted_iota(I32, (tokens, tokens), 1)
    repeat = jnp.max(jnp.where(equal & earlier, 1, 0), axis=0, keepdims=True)
    mine = ids_v[...] - base
    rows_mine[...] = jnp.where((mine >= 0) & (mine < vocab) & (repeat == 0), mine, -1)
    lid = col.astype(I32) - base
    lane = lax.broadcasted_iota(I32, (group, 2 * group), 1)
    first = lax.broadcasted_iota(I32, (group, 2 * group), 0) * 2
    for k in range(groups):
        at = lid[k * group:(k + 1) * group, :2 * group]
        owned = (at >= 0) & (at < vocab)
        pick = jnp.where(owned & (lane == first + (at & 1)), 1.0, 0.0).astype(BF)
        pltpu.make_async_copy(table.at[pl.ds(0, group * 2)], pairs.at[k], sems.at[k]).wait()
        part[pl.ds(k * group, group), :] = mm(pick, pairs[k], 1, 0).astype(BF)
    fill_wait(zero, table_g, s_zero, 0)


def lookup(ids, table):
    tokens, (vocab, width) = ids.shape[0], table.shape
    return pl.pallas_call(
        lookup_kernel,
        name="lookup",
        out_shape=[sh((tokens, width), BF), sh((1, tokens), I32), sh((tokens, tokens), BF), sh((ZERO_ROWS, width), F32), sh((vocab, width), F32)],
        in_specs=[HBM_SPEC] * 3,
        out_specs=[VMEM_SPEC] * 4 + [HBM_SPEC],
        scratch_shapes=[pltpu.SMEM((tokens,), I32), VMEM((1, tokens), I32), VMEM((4, tokens // 2, width), BF), DMA((4,)), DMA(()), DMA((2,))],
        compiler_params=pltpu.CompilerParams(vmem_limit_bytes=LOOKUP_VMEM),
        cost_estimate=pl.CostEstimate(flops=5_000_000_000, bytes_accessed=10 * MIB, transcendentals=0),
    )(in_hbm(ids), in_hbm(ids.reshape(1, tokens)), in_hbm(table))


def pair_kernel(part, w1, send, w1_v, part_r, sems, s_in):
    me = lax.axis_index("tp")
    rows = part.shape[0] // 4
    blocks = (me, me ^ 2, me ^ 1, me ^ 3)
    load = pltpu.make_async_copy(w1, w1_v, s_in)
    load.start()
    remote = swap_with_sibling()
    block = lambda k: pl.ds(pl.multiple_of(blocks[k] * rows, rows), rows)
    copies = [remote(part.at[block(2 + k)], part_r.at[pl.ds(k * rows, rows)], sems, k) for k in range(2)]
    for c in copies:
        c.start()
    for k in range(2):
        copies[k].wait()
        at = pl.ds(k * rows, rows)
        send[at, :] = part[block(k), :] + part_r[at, :]
    load.wait()


def pair(part, w1):
    rows, width = part.shape[0] // 4, part.shape[1]
    return pl.pallas_call(
        pair_kernel,
        name="pair",
        out_shape=[sh((2 * rows, width), BF), sh(w1.shape, BF)],
        in_specs=[VMEM_SPEC, HBM_SPEC],
        out_specs=[VMEM_SPEC] * 2,
        scratch_shapes=[VMEM((2 * rows, width), BF), DMA((2, 2)), DMA(())],
        compiler_params=pltpu.CompilerParams(collective_id=0, has_side_effects=True, vmem_limit_bytes=PAIR_VMEM),
        cost_estimate=pl.CostEstimate(flops=3_000_000_000, bytes_accessed=MIB, transcendentals=0),
    )(part, in_hbm(w1))


def fill1_kernel(rows_mine, zero, w2, order, table_in, puts, w2_v, table_g, mine_s, puts_s, s_zero, s_list, s_w):
    load = pltpu.make_async_copy(rows_mine, mine_s, s_list)
    load.start()
    load_w = pltpu.make_async_copy(w2, w2_v, s_w)
    load_w.start()
    fill_start(zero, table_g, s_zero, 1)
    tokens = rows_mine.shape[1]
    load.wait()

    def body(i, count):
        lid = mine_s[0, i]
        puts_s[count] = lid | (i << 16)
        return count + (lid >= 0).astype(I32)

    puts_s[tokens] = lax.fori_loop(0, tokens, body, 0, unroll=8)
    store = pltpu.make_async_copy(puts_s, puts, s_list)
    store.start()
    store.wait()
    load_w.wait()
    fill_wait(zero, table_g, s_zero, 1)


def fill1(rows_mine, zero, w2, order, table_g):
    tokens = rows_mine.shape[1]
    return pl.pallas_call(
        fill1_kernel,
        name="fill1",
        out_shape=[sh((2 * tokens,), I32), sh(w2.shape, BF), sh(table_g.shape, F32)],
        in_specs=[ANY_SPEC, VMEM_SPEC, HBM_SPEC, ANY_SPEC, HBM_SPEC],
        out_specs=[ANY_SPEC, VMEM_SPEC, HBM_SPEC],
        input_output_aliases={4: 2},
        scratch_shapes=[pltpu.SMEM((1, tokens), I32), pltpu.SMEM((2 * tokens,), I32), DMA(()), DMA(()), DMA(())],
        compiler_params=pltpu.CompilerParams(vmem_limit_bytes=8 * MIB),
        cost_estimate=pl.CostEstimate(flops=9_000_000_000, bytes_accessed=20 * MIB, transcendentals=0),
    )(rows_mine, zero, in_hbm(w2), order, table_g)


def mlp_half(x, d, n, h, du, at, w1, w2, gain):
    first, count = at
    width, hid = n.shape[1], h.shape[1]
    gain_f = gain[...].astype(F32).reshape(1, width)
    for j in range(count // 32):
        rows = pl.ds(first + j * 32, 32)
        x_f = x[rows, :].astype(F32)
        r = lax.rsqrt(jnp.mean(x_f * x_f, axis=-1, keepdims=True) + EPS)
        n[rows, :] = (x_f * r * gain_f).astype(BF)
    rows = pl.ds(first, count)
    for j in range(hid // TILE):
        cols = pl.ds(j * TILE, TILE)
        g = mm(d[rows, :], w2[cols, :], 1, 1).astype(BF).astype(F32)
        u = mm(n[rows, :], w1[:, cols], 1, 0).astype(BF).astype(F32)
        t = jnp.tanh(GELU_C * (u + GELU_A * (u * u * u)))
        cdf = 0.5 * (1.0 + t)
        h[rows, cols] = (u * cdf).astype(BF)
        du[rows, cols] = (g * (cdf + u * (0.5 * (1.0 - t * t)) * (GELU_C * (1.0 + 3.0 * GELU_A * (u * u))))).astype(BF)


def share_kernel(send, got, d_own, d_far, d_own_s, d_far_s, w1, w2, gain, x_f, d_full, n_a, h_a, du_a, x_r, sems):
    rows = d_own.shape[0]
    half = 2 * rows
    remote = swap_with_sibling()
    copies = []
    for k in range(2):
        at, other = pl.ds(k * rows, rows), pl.ds((1 - k) * rows, rows)
        x_f[at, :] = send[at, :] + got[other, :]
        copies.append(remote(x_f.at[at], x_r.at[at], sems, k))
        copies[-1].start()
    for k, src in enumerate((d_own, d_far, d_own_s, d_far_s)):
        d_full[pl.ds(k * rows, rows), :] = src[...]
    mlp_half(x_f, d_full, n_a, h_a, du_a, (0, half), w1, w2, gain)
    for k in range(2):
        copies[k].wait()
        x_f[pl.ds(half + k * rows, rows), :] = x_r[pl.ds(k * rows, rows), :]


def share(send, got, ds, w1, w2, gain):
    rows, width = ds[0].shape
    hid = w1.shape[1]
    return pl.pallas_call(
        share_kernel,
        name="share",
        out_shape=[sh((4 * rows, width), BF)] * 2 + [sh((2 * rows, width), BF)] + [sh((2 * rows, hid), BF)] * 2,
        in_specs=[VMEM_SPEC] * 9,
        out_specs=[VMEM_SPEC] * 5,
        scratch_shapes=[VMEM((2 * rows, width), BF), DMA((2, 2))],
        compiler_params=pltpu.CompilerParams(collective_id=1, has_side_effects=True, vmem_limit_bytes=16 * MIB),
        cost_estimate=pl.CostEstimate(flops=3_000_000_000, bytes_accessed=MIB, transcendentals=0),
    )(send, got, *ds, w1, w2, gain)


def mlp_kernel(x_f, d_full, n_a, h_a, du_a, w1, w2, gain, zero, table_in, n, h, du, dn_b0, dn_b1, table_g, s_zero):
    fill_start(zero, table_g, s_zero, 2)
    tokens, width = n.shape
    half = tokens // 2
    for out, src in ((n, n_a), (h, h_a), (du, du_a)):
        out[pl.ds(0, half), :] = src[...]
    mlp_half(x_f, d_full, n, h, du, (half, half), w1, w2, gain)
    for j in range(width // TILE):
        cols = pl.ds(j * TILE, TILE)
        dn = mm(du[pl.ds(half, half), :], w1[cols, :], 1, 1)
        dn_b0[:, cols] = dn[:half // 2]
        dn_b1[:, cols] = dn[half // 2:]
    fill_wait(zero, table_g, s_zero, 2)


def mlp(x_f, d_full, n_a, h_a, du_a, w1, w2, gain, zero, table_g):
    tokens, width = x_f.shape
    hid = w1.shape[1]
    return pl.pallas_call(
        mlp_kernel,
        name="mlp",
        out_shape=[sh((tokens, width), BF), sh((tokens, hid), BF), sh((tokens, hid), BF), sh((tokens // 4, width), F32),
                   sh((tokens // 4, width), F32), sh(table_g.shape, F32)],
        in_specs=[VMEM_SPEC] * 9 + [HBM_SPEC],
        out_specs=[VMEM_SPEC] * 5 + [HBM_SPEC],
        input_output_aliases={9: 5},
        scratch_shapes=[DMA(())],
        compiler_params=pltpu.CompilerParams(vmem_limit_bytes=16 * MIB),
        cost_estimate=pl.CostEstimate(flops=6_000_000_000, bytes_accessed=4 * MIB, transcendentals=0),
    )(x_f, d_full, n_a, h_a, du_a, w1, w2, gain, zero, table_g)


def sums_kernel(dn_b1, du, h, w1, w2, dn_own, dn_far, y_a, y_b, dn_r, sems):
    rows, width = dn_own.shape
    half = 2 * rows
    remote = swap_with_sibling()
    copy = remote(dn_b1, dn_r, sems, 0)
    copy.start()
    for j in range(width // TILE):
        cols = pl.ds(j * TILE, TILE)
        dn = mm(du[pl.ds(0, half), :], w1[cols, :], 1, 1)
        dn_own[:, cols] = dn[:rows]
        dn_far[:, cols] = dn[rows:]
    for j in range(width // TILE):
        cols = pl.ds(j * TILE, TILE)
        y = mm(h[...], w2[:, cols], 1, 0)
        y_a[:, cols] = y[:half]
        y_b[:, cols] = y[half:]
    copy.wait()
    dn_far[...] += dn_r[...]


def sums(dn_b1, du, h, w1, w2):
    rows, width = dn_b1.shape
    return pl.pallas_call(
        sums_kernel,
        name="sums",
        out_shape=[sh((rows, width), F32)] * 2 + [sh((2 * rows, width), F32)] * 2,
        in_specs=[VMEM_SPEC] * 5,
        out_specs=[VMEM_SPEC] * 4,
        scratch_shapes=[VMEM((rows, width), F32), DMA((2, 1))],
        compiler_params=pltpu.CompilerParams(collective_id=2, has_side_effects=True, vmem_limit_bytes=16 * MIB),
        cost_estimate=pl.CostEstimate(flops=4_000_000_000, bytes_accessed=4 * MIB, transcendentals=0),
    )(dn_b1, du, h, w1, w2)


def grads1_kernel(n, du, zero, order, table_in, dw1, table_g, dw1_v, s_zero, s_w):
    width = n.shape[1]
    n_t = n[...].T
    for j in range(width // TILE):
        at = slice(j * TILE, (j + 1) * TILE)
        dw1_v[at, :] = mm(n_t[at, :], du[...], 1, 0)
        pltpu.make_async_copy(dw1_v.at[pl.ds(j * TILE, TILE)], dw1.at[pl.ds(j * TILE, TILE)], s_w).start()
        if j == 0:
            fill_start(zero, table_g, s_zero, 3)
    pltpu.make_async_copy(dw1_v, dw1, s_w).wait()
    fill_wait(zero, table_g, s_zero, 3)


def grads1(n, du, zero, order, table_g):
    width, hid = n.shape[1], du.shape[1]
    return pl.pallas_call(
        grads1_kernel,
        name="grads1",
        out_shape=[sh((width, hid), F32), sh(table_g.shape, F32)],
        in_specs=[VMEM_SPEC] * 3 + [ANY_SPEC, HBM_SPEC],
        out_specs=[HBM_SPEC, HBM_SPEC],
        input_output_aliases={4: 1},
        scratch_shapes=[VMEM((width, hid), F32), DMA(()), DMA(())],
        compiler_params=pltpu.CompilerParams(vmem_limit_bytes=16 * MIB),
        cost_estimate=pl.CostEstimate(flops=4_000_000_000, bytes_accessed=8 * MIB, transcendentals=0),
    )(n, du, zero, order, table_g)


def grads2_kernel(h, d_full, y_a, y_sib, zero, table_in, dw2, y_own, y_far, table_g, dw2_v, s_zero, s_w):
    rows = y_own.shape[0]
    hid = h.shape[1]
    fill_start(zero, table_g, s_zero, 4)
    for k, out in enumerate((y_own, y_far)):
        at = pl.ds(k * rows, rows)
        out[...] = y_a[at, :] + y_sib[at, :]
    h_t = h[...].T
    for j in range(hid // TILE):
        at = slice(j * TILE, (j + 1) * TILE)
        dw2_v[at, :] = mm(h_t[at, :], d_full[...], 1, 0)
        pltpu.make_async_copy(dw2_v.at[pl.ds(j * TILE, TILE)], dw2.at[pl.ds(j * TILE, TILE)], s_w).start()
    pltpu.make_async_copy(dw2_v, dw2, s_w).wait()
    fill_wait(zero, table_g, s_zero, 4)


def grads2(h, d_full, y_a, y_sib, zero, table_g):
    hid, width = h.shape[1], d_full.shape[1]
    rows = y_a.shape[0] // 2
    return pl.pallas_call(
        grads2_kernel,
        name="grads2",
        out_shape=[sh((hid, width), F32)] + [sh((rows, width), F32)] * 2 + [sh(table_g.shape, F32)],
        in_specs=[VMEM_SPEC] * 5 + [HBM_SPEC],
        out_specs=[HBM_SPEC, VMEM_SPEC, VMEM_SPEC, HBM_SPEC],
        input_output_aliases={5: 3},
        scratch_shapes=[VMEM((hid, width), F32), DMA(()), DMA(())],
        compiler_params=pltpu.CompilerParams(vmem_limit_bytes=16 * MIB),
        cost_estimate=pl.CostEstimate(flops=4_000_000_000, bytes_accessed=8 * MIB, transcendentals=0),
    )(h, d_full, y_a, y_sib, zero, table_g)


def dx_kernel(dn_own, dn_sib, g2, x_own, d_own, gain, order, dx):
    gain_f = gain[...].astype(F32).reshape(1, dx.shape[1])
    for j in range(dx.shape[0] // 16):
        at = pl.ds(j * 16, 16)
        a = (dn_own[at, :] + dn_sib[at, :] + g2[at, :]) * gain_f
        x = x_own[at, :].astype(F32)
        r = lax.rsqrt(jnp.mean(x * x, axis=-1, keepdims=True) + EPS)
        proj = jnp.mean(a * x, axis=-1, keepdims=True)
        dx[at, :] = (d_own[at, :].astype(F32) + r * (a - x * r * r * proj)).astype(BF)


def dx_rows(dn_own, dn_sib, g2, x_own, d_own, gain, order):
    return pl.pallas_call(
        dx_kernel,
        name="dx_rows",
        out_shape=sh(d_own.shape, BF),
        in_specs=[VMEM_SPEC] * 6 + [ANY_SPEC],
        out_specs=VMEM_SPEC,
        compiler_params=pltpu.CompilerParams(vmem_limit_bytes=4 * MIB),
        cost_estimate=pl.CostEstimate(flops=1_000_000_000, bytes_accessed=MIB, transcendentals=0),
    )(dn_own, dn_sib, g2, x_own, d_own, gain, order)


def fill3_kernel(zero, order, table_in, token, table_g, s_zero):
    fill_start(zero, table_g, s_zero, 5)
    token[...] = jnp.zeros_like(token)
    fill_wait(zero, table_g, s_zero, 5)


def fill3(zero, order, table_g):
    return pl.pallas_call(
        fill3_kernel,
        name="fill3",
        out_shape=[sh((8, 128), F32), sh(table_g.shape, F32)],
        in_specs=[VMEM_SPEC, ANY_SPEC, HBM_SPEC],
        out_specs=[VMEM_SPEC, HBM_SPEC],
        input_output_aliases={2: 1},
        scratch_shapes=[DMA(())],
        compiler_params=pltpu.CompilerParams(vmem_limit_bytes=4 * MIB),
        cost_estimate=pl.CostEstimate(flops=4_000_000_000, bytes_accessed=16 * MIB, transcendentals=0),
    )(zero, order, table_g)


def dx_all_kernel(dx, dx_sib, dx_far, order, dx_out, dx_r, sems):
    me = lax.axis_index("tp")
    rows = dx.shape[0]
    remote = swap_with_sibling()
    block = lambda m: pl.ds(pl.multiple_of((me ^ m) * rows, rows), rows)
    copy = remote(dx_far, dx_r, sems, 0)
    copy.start()
    for m, src in enumerate((dx, dx_sib, dx_far)):
        dx_out[block(m), :] = src[...]
    copy.wait()
    dx_out[block(3), :] = dx_r[...]


def dx_all(dx, dx_sib, dx_far, order):
    rows, width = dx.shape
    return pl.pallas_call(
        dx_all_kernel,
        name="dx_all",
        out_shape=sh((4 * rows, width), BF),
        in_specs=[VMEM_SPEC] * 3 + [ANY_SPEC],
        out_specs=VMEM_SPEC,
        scratch_shapes=[VMEM((rows, width), BF), DMA((2, 1))],
        compiler_params=pltpu.CompilerParams(collective_id=3, has_side_effects=True, vmem_limit_bytes=4 * MIB),
        cost_estimate=pl.CostEstimate(flops=2_000_000_000, bytes_accessed=MIB, transcendentals=0),
    )(dx, dx_sib, dx_far, order)


def put_kernel(puts, same, dx, zero, table_in, table_g, token, puts_s, total, s_in, s_row, s_zero):
    fill_start(zero, table_g, s_zero, LATE)
    tokens = dx.shape[0]
    load = pltpu.make_async_copy(puts, puts_s, s_in)
    load.start()
    total[...] = mm(same[...], dx[...], 1, 0)
    token[...] = jnp.zeros_like(token)
    load.wait()
    fill_wait(zero, table_g, s_zero, LATE)
    count = puts_s[tokens]

    def put(i):
        word = puts_s[i]
        pltpu.make_async_copy(total.at[pl.ds(word >> 16, 1)], table_g.at[pl.ds(word & 0xFFFF, 1)], s_row).start()

    def put_four(i, carry):
        for k in range(4):
            put(i * 4 + k)
        return carry

    def put_one(i, carry):
        put(i)
        return carry

    lax.fori_loop(0, count >> 2, put_four, 0)
    lax.fori_loop((count >> 2) * 4, count, put_one, 0)

    def put_wait(size):
        def body(i, carry):
            pltpu.make_async_copy(total.at[pl.ds(0, size)], table_g.at[pl.ds(0, size)], s_row).wait()
            return carry

        return body

    lax.fori_loop(0, count >> 3, put_wait(8), 0)
    lax.fori_loop(0, count & 7, put_wait(1), 0)


def put_rows(puts, same, dx, zero, table_g):
    return pl.pallas_call(
        put_kernel,
        name="put_rows",
        out_shape=[sh(table_g.shape, F32), sh((8, 128), F32)],
        in_specs=[ANY_SPEC, VMEM_SPEC, VMEM_SPEC, VMEM_SPEC, HBM_SPEC],
        out_specs=[HBM_SPEC, VMEM_SPEC],
        input_output_aliases={4: 0},
        scratch_shapes=[pltpu.SMEM(puts.shape, I32), VMEM(dx.shape, F32), DMA(()), DMA(()), DMA(())],
        compiler_params=pltpu.CompilerParams(vmem_limit_bytes=4 * MIB),
        cost_estimate=pl.CostEstimate(flops=3_000_000_000, bytes_accessed=2 * MIB, transcendentals=0),
    )(puts, same, dx, zero, table_g)


def finish_kernel(x, y, y_in, order, out):
    out[...] = (x[pl.ds(0, out.shape[0]), :].astype(F32) + (y[...] + y_in[...])).astype(BF)


def finish(x, y, y_in, order):
    return pl.pallas_call(
        finish_kernel,
        name="finish",
        out_shape=sh(y.shape, BF),
        in_specs=[VMEM_SPEC] * 3 + [ANY_SPEC],
        out_specs=VMEM_SPEC,
        compiler_params=pltpu.CompilerParams(vmem_limit_bytes=4 * MIB),
        cost_estimate=pl.CostEstimate(flops=1_000_000_000, bytes_accessed=MIB, transcendentals=0),
    )(x, y, y_in, order)


def solution(mesh):
    tp = mesh.shape["tp"]

    def permute(x, hop):
        return lax.ppermute(x, "tp", [(i, i ^ hop) for i in range(tp)])

    def shard_step(ids, table, gain, w1, w2, d_out):
        part, rows_mine, same, zero, d_table = lookup(ids, table)
        part, d_send = lax.optimization_barrier((part, d_out))
        d_far = permute(d_send, 2)
        send, w1 = pair(part, w1)
        got = permute(send, 2)
        ds = (d_out, d_far, permute(d_out, 1), permute(d_far, 1))
        puts, w2, d_table = fill1(rows_mine, zero, w2, send, d_table)
        x_f, d_full, n_a, h_a, du_a = share(send, got, ds, w1, w2, gain)
        n, h, du, dn_b0, dn_b1, d_table = mlp(x_f, d_full, n_a, h_a, du_a, w1, w2, gain, zero, d_table)
        dn_own, dn_far, y_a, y_b = sums(dn_b1, du, h, w1, w2)
        g2 = permute(dn_far, 2)
        dn_sib = permute(dn_b0, 1)
        y_sib = permute(y_b, 1)
        d_w1, d_table = grads1(n, du, zero, dn_own, d_table)
        d_w2, y_own, y_far, d_table = grads2(h, d_full, y_a, y_sib, zero, d_table)
        dx = dx_rows(dn_own, dn_sib, g2, x_f, d_out, gain, y_own)
        dx_far = permute(dx, 2)
        dx_sib = permute(dx, 1)
        dx, y_far = lax.optimization_barrier((dx, y_far))
        y_in = permute(y_far, 2)
        token, d_table = fill3(zero, dx, d_table)
        dx_full = dx_all(dx, dx_sib, dx_far, token)
        d_table, done = put_rows(puts, same, dx_full, zero, d_table)
        out = finish(x_f, y_own, y_in, done)
        return out, d_table, d_w1, d_w2

    return jax.shard_map(
        shard_step,
        mesh=mesh,
        in_specs=(P("dp"), P("tp", None), P(None), P(None, "tp"), P("tp", None), P(("dp", "tp"), None)),
        out_specs=(P(("dp", "tp"), None), P(("dp", "tp"), None), P("dp", "tp"), P(("dp", "tp"), None)),
        check_vma=False,
    )
```

```python
import jax
import jax.numpy as jnp
from jax import lax
from jax.experimental import pallas as pl
from jax.experimental.pallas import tpu as pltpu
from jax.sharding import PartitionSpec as P

EPS = 1e-6
BF = jnp.bfloat16
F32 = jnp.float32
I32 = jnp.int32
GELU_C = 0.7978845608028654
GELU_A = 0.044715
VMEM = pltpu.VMEM
SMEM_SPEC = pl.BlockSpec(memory_space=pltpu.SMEM)
ANY_SPEC = pl.BlockSpec(memory_space=pl.ANY)
HBM_SPEC = pl.BlockSpec(memory_space=pltpu.HBM)
VMEM_SPEC = pl.BlockSpec(memory_space=VMEM)
DMA = pltpu.SemaphoreType.DMA
TILE = 256
ZERO_ROWS = 96
FILL_COUNTS = ((22, 54, 13, 8, 8, 21, 5), (4, 50, 13, 9, 9, 23, 23))
LATE = 6
MIB = 1 << 20
LOOKUP_VMEM = 48 * MIB
PAIR_VMEM = 8 * MIB


def mm(a, b, ca, cb):
    return lax.dot_general(a, b, (((ca,), (cb,)), ((), ())), preferred_element_type=F32)


def in_hbm(x):
    return pltpu.with_memory_space_constraint(x, pltpu.HBM)


def sh(shape, dtype):
    return jax.ShapeDtypeStruct(shape, dtype)


def fill_copy(zero, table_g, sem, i):
    return pltpu.make_async_copy(zero, table_g.at[pl.ds(pl.multiple_of(i * ZERO_ROWS, ZERO_ROWS), ZERO_ROWS)], sem)


def fill_range(part):
    chip = lax.axis_index("tp") >> 1
    (lo0, hi0), (lo1, hi1) = ((sum(c[:part]), sum(c[:part + 1])) for c in FILL_COUNTS)
    return lo0 + chip * (lo1 - lo0), hi0 + chip * (hi1 - hi0)


def fill_start(zero, table_g, sem, part):
    def body(i, carry):
        fill_copy(zero, table_g, sem, i).start()
        return carry

    lax.fori_loop(*fill_range(part), body, 0)


def fill_wait(zero, table_g, sem, part):
    def body(i, carry):
        fill_copy(zero, table_g, sem, i).wait()
        return carry

    lax.fori_loop(*fill_range(part), body, 0)


def swap_with_sibling():
    sib = lax.axis_index("tp") ^ 1
    barrier = pltpu.get_barrier_semaphore()
    pl.semaphore_signal(barrier, inc=1, device_id={"tp": sib}, device_id_type=pl.DeviceIdType.MESH)
    pl.semaphore_wait(barrier, 1)

    def remote(src, dst, sems, i):
        return pltpu.make_async_remote_copy(
            src_ref=src, dst_ref=dst, send_sem=sems.at[0, i], recv_sem=sems.at[1, i],
            device_id={"tp": sib}, device_id_type=pl.DeviceIdType.MESH)

    return remote


def lookup_kernel(ids, ids_row, table, part, rows_mine, same, zero, table_g, ids_s, ids_v, pairs, sems, s_zero, s_ids):
    tokens, vocab = part.shape[0], table.shape[0]
    base = lax.axis_index("tp") * vocab
    group = 64
    groups = tokens // group
    loads = [pltpu.make_async_copy(ids, ids_s, s_ids.at[0]), pltpu.make_async_copy(ids_row, ids_v, s_ids.at[1])]
    for c in loads:
        c.start()
    zero[...] = jnp.zeros_like(zero)
    fill_start(zero, table_g, s_zero, 0)
    loads[0].wait()

    def fetch(k, carry):
        for i in range(group):
            token = k * group + i
            lid = ids_s[token] - base
            owned = (lid >= 0) & (lid < vocab)
            row = jnp.where(owned, lid & -2, 2 * token)
            pltpu.make_async_copy(table.at[pl.ds(pl.multiple_of(row, 2), 2)], pairs.at[k, pl.ds(2 * i, 2)], sems.at[k]).start()
        return carry

    lax.fori_loop(0, groups, fetch, 0)
    loads[1].wait()
    row = jnp.broadcast_to(ids_v[...].astype(F32), (tokens, tokens))
    col = row.T
    equal = row == col
    same[...] = jnp.where(equal, 1.0, 0.0).astype(BF)
    earlier = lax.broadcasted_iota(I32, (tokens, tokens), 0) < lax.broadcasted_iota(I32, (tokens, tokens), 1)
    repeat = jnp.max(jnp.where(equal & earlier, 1, 0), axis=0, keepdims=True)
    mine = ids_v[...] - base
    rows_mine[...] = jnp.where((mine >= 0) & (mine < vocab) & (repeat == 0), mine, -1)
    lid = col.astype(I32) - base
    lane = lax.broadcasted_iota(I32, (group, 2 * group), 1)
    first = lax.broadcasted_iota(I32, (group, 2 * group), 0) * 2
    for k in range(groups):
        at = lid[k * group:(k + 1) * group, :2 * group]
        owned = (at >= 0) & (at < vocab)
        pick = jnp.where(owned & (lane == first + (at & 1)), 1.0, 0.0).astype(BF)
        pltpu.make_async_copy(table.at[pl.ds(0, group * 2)], pairs.at[k], sems.at[k]).wait()
        part[pl.ds(k * group, group), :] = mm(pick, pairs[k], 1, 0).astype(BF)
    fill_wait(zero, table_g, s_zero, 0)


def lookup(ids, table):
    tokens, (vocab, width) = ids.shape[0], table.shape
    return pl.pallas_call(
        lookup_kernel,
        name="lookup",
        out_shape=[sh((tokens, width), BF), sh((1, tokens), I32), sh((tokens, tokens), BF), sh((ZERO_ROWS, width), F32), sh((vocab, width), F32)],
        in_specs=[HBM_SPEC] * 3,
        out_specs=[VMEM_SPEC] * 4 + [HBM_SPEC],
        scratch_shapes=[pltpu.SMEM((tokens,), I32), VMEM((1, tokens), I32), VMEM((4, tokens // 2, width), BF), DMA((4,)), DMA(()), DMA((2,))],
        compiler_params=pltpu.CompilerParams(vmem_limit_bytes=LOOKUP_VMEM),
        cost_estimate=pl.CostEstimate(flops=5_000_000_000, bytes_accessed=10 * MIB, transcendentals=0),
    )(in_hbm(ids), in_hbm(ids.reshape(1, tokens)), in_hbm(table))


def pair_kernel(part, w1, send, w1_v, part_r, sems, s_in):
    me = lax.axis_index("tp")
    rows = part.shape[0] // 4
    blocks = (me, me ^ 2, me ^ 1, me ^ 3)
    load = pltpu.make_async_copy(w1, w1_v, s_in)
    load.start()
    remote = swap_with_sibling()
    block = lambda k: pl.ds(pl.multiple_of(blocks[k] * rows, rows), rows)
    copies = [remote(part.at[block(2 + k)], part_r.at[pl.ds(k * rows, rows)], sems, k) for k in range(2)]
    for c in copies:
        c.start()
    for k in range(2):
        copies[k].wait()
        at = pl.ds(k * rows, rows)
        send[at, :] = part[block(k), :] + part_r[at, :]
    load.wait()


def pair(part, w1):
    rows, width = part.shape[0] // 4, part.shape[1]
    return pl.pallas_call(
        pair_kernel,
        name="pair",
        out_shape=[sh((2 * rows, width), BF), sh(w1.shape, BF)],
        in_specs=[VMEM_SPEC, HBM_SPEC],
        out_specs=[VMEM_SPEC] * 2,
        scratch_shapes=[VMEM((2 * rows, width), BF), DMA((2, 2)), DMA(())],
        compiler_params=pltpu.CompilerParams(collective_id=0, has_side_effects=True, vmem_limit_bytes=PAIR_VMEM),
        cost_estimate=pl.CostEstimate(flops=3_000_000_000, bytes_accessed=MIB, transcendentals=0),
    )(part, in_hbm(w1))


def fill1_kernel(rows_mine, zero, w2, order, table_in, puts, w2_v, table_g, mine_s, puts_s, s_zero, s_list, s_w):
    load = pltpu.make_async_copy(rows_mine, mine_s, s_list)
    load.start()
    load_w = pltpu.make_async_copy(w2, w2_v, s_w)
    load_w.start()
    fill_start(zero, table_g, s_zero, 1)
    tokens = rows_mine.shape[1]
    load.wait()

    def body(i, count):
        lid = mine_s[0, i]
        puts_s[count] = lid | (i << 16)
        return count + (lid >= 0).astype(I32)

    puts_s[tokens] = lax.fori_loop(0, tokens, body, 0, unroll=8)
    store = pltpu.make_async_copy(puts_s, puts, s_list)
    store.start()
    store.wait()
    load_w.wait()
    fill_wait(zero, table_g, s_zero, 1)


def fill1(rows_mine, zero, w2, order, table_g):
    tokens = rows_mine.shape[1]
    return pl.pallas_call(
        fill1_kernel,
        name="fill1",
        out_shape=[sh((2 * tokens,), I32), sh(w2.shape, BF), sh(table_g.shape, F32)],
        in_specs=[ANY_SPEC, VMEM_SPEC, HBM_SPEC, ANY_SPEC, HBM_SPEC],
        out_specs=[ANY_SPEC, VMEM_SPEC, HBM_SPEC],
        input_output_aliases={4: 2},
        scratch_shapes=[pltpu.SMEM((1, tokens), I32), pltpu.SMEM((2 * tokens,), I32), DMA(()), DMA(()), DMA(())],
        compiler_params=pltpu.CompilerParams(vmem_limit_bytes=8 * MIB),
        cost_estimate=pl.CostEstimate(flops=9_000_000_000, bytes_accessed=20 * MIB, transcendentals=0),
    )(rows_mine, zero, in_hbm(w2), order, table_g)


def mlp_half(x, d, n, h, du, at, w1, w2, gain):
    first, count = at
    width, hid = n.shape[1], h.shape[1]
    gain_f = gain[...].astype(F32).reshape(1, width)
    for j in range(count // 32):
        rows = pl.ds(first + j * 32, 32)
        x_f = x[rows, :].astype(F32)
        r = lax.rsqrt(jnp.mean(x_f * x_f, axis=-1, keepdims=True) + EPS)
        n[rows, :] = (x_f * r * gain_f).astype(BF)
    rows = pl.ds(first, count)
    for j in range(hid // TILE):
        cols = pl.ds(j * TILE, TILE)
        g = mm(d[rows, :], w2[cols, :], 1, 1).astype(BF).astype(F32)
        u = mm(n[rows, :], w1[:, cols], 1, 0).astype(BF).astype(F32)
        t = jnp.tanh(GELU_C * (u + GELU_A * (u * u * u)))
        cdf = 0.5 * (1.0 + t)
        h[rows, cols] = (u * cdf).astype(BF)
        du[rows, cols] = (g * (cdf + u * (0.5 * (1.0 - t * t)) * (GELU_C * (1.0 + 3.0 * GELU_A * (u * u))))).astype(BF)


def share_kernel(send, got, d_own, d_far, w1, w2, gain, x_f, n_a, h_a, du_a, x_r, d_a, sems):
    rows = d_own.shape[0]
    half = 2 * rows
    remote = swap_with_sibling()
    copies = []
    for k in range(2):
        at, other = pl.ds(k * rows, rows), pl.ds((1 - k) * rows, rows)
        x_f[at, :] = send[at, :] + got[other, :]
        copies.append(remote(x_f.at[at], x_r.at[at], sems, k))
        copies[-1].start()
    for k, src in enumerate((d_own, d_far)):
        d_a[pl.ds(k * rows, rows), :] = src[...]
    mlp_half(x_f, d_a, n_a, h_a, du_a, (0, half), w1, w2, gain)
    for k in range(2):
        copies[k].wait()
        x_f[pl.ds(half + k * rows, rows), :] = x_r[pl.ds(k * rows, rows), :]


def share(send, got, d_own, d_far, w1, w2, gain):
    rows, width = d_own.shape
    hid = w1.shape[1]
    return pl.pallas_call(
        share_kernel,
        name="share",
        out_shape=[sh((4 * rows, width), BF), sh((2 * rows, width), BF)] + [sh((2 * rows, hid), BF)] * 2,
        in_specs=[VMEM_SPEC] * 7,
        out_specs=[VMEM_SPEC] * 4,
        scratch_shapes=[VMEM((2 * rows, width), BF), VMEM((2 * rows, width), BF), DMA((2, 2))],
        compiler_params=pltpu.CompilerParams(collective_id=1, has_side_effects=True, vmem_limit_bytes=16 * MIB),
        cost_estimate=pl.CostEstimate(flops=3_000_000_000, bytes_accessed=MIB, transcendentals=0),
    )(send, got, d_own, d_far, w1, w2, gain)


def mlp_kernel(x_f, d_own, d_far, d_own_s, d_far_s, n_a, h_a, du_a, w1, w2, gain, zero, table_in,
               n, h, du, d_full, dn_b0, dn_b1, table_g, s_zero):
    fill_start(zero, table_g, s_zero, 2)
    rows = d_own.shape[0]
    for k, src in enumerate((d_own, d_far, d_own_s, d_far_s)):
        d_full[pl.ds(k * rows, rows), :] = src[...]
    tokens, width = n.shape
    half = tokens // 2
    for out, src in ((n, n_a), (h, h_a), (du, du_a)):
        out[pl.ds(0, half), :] = src[...]
    mlp_half(x_f, d_full, n, h, du, (half, half), w1, w2, gain)
    for j in range(width // TILE):
        cols = pl.ds(j * TILE, TILE)
        dn = mm(du[pl.ds(half, half), :], w1[cols, :], 1, 1)
        dn_b0[:, cols] = dn[:half // 2]
        dn_b1[:, cols] = dn[half // 2:]
    fill_wait(zero, table_g, s_zero, 2)


def mlp(x_f, ds, n_a, h_a, du_a, w1, w2, gain, zero, table_g):
    tokens, width = x_f.shape
    hid = w1.shape[1]
    return pl.pallas_call(
        mlp_kernel,
        name="mlp",
        out_shape=[sh((tokens, width), BF), sh((tokens, hid), BF), sh((tokens, hid), BF), sh((tokens, width), BF),
                   sh((tokens // 4, width), F32), sh((tokens // 4, width), F32), sh(table_g.shape, F32)],
        in_specs=[VMEM_SPEC] * 12 + [HBM_SPEC],
        out_specs=[VMEM_SPEC] * 6 + [HBM_SPEC],
        input_output_aliases={12: 6},
        scratch_shapes=[DMA(())],
        compiler_params=pltpu.CompilerParams(vmem_limit_bytes=16 * MIB),
        cost_estimate=pl.CostEstimate(flops=6_000_000_000, bytes_accessed=4 * MIB, transcendentals=0),
    )(x_f, *ds, n_a, h_a, du_a, w1, w2, gain, zero, table_g)


def sums_kernel(dn_b1, du, h, w1, w2, dn_own, dn_far, y_a, y_b, dn_r, sems):
    rows, width = dn_own.shape
    half = 2 * rows
    remote = swap_with_sibling()
    copy = remote(dn_b1, dn_r, sems, 0)
    copy.start()
    for j in range(width // TILE):
        cols = pl.ds(j * TILE, TILE)
        dn = mm(du[pl.ds(0, half), :], w1[cols, :], 1, 1)
        dn_own[:, cols] = dn[:rows]
        dn_far[:, cols] = dn[rows:]
    for j in range(width // TILE):
        cols = pl.ds(j * TILE, TILE)
        y = mm(h[...], w2[:, cols], 1, 0)
        y_a[:, cols] = y[:half]
        y_b[:, cols] = y[half:]
    copy.wait()
    dn_far[...] += dn_r[...]


def sums(dn_b1, du, h, w1, w2):
    rows, width = dn_b1.shape
    return pl.pallas_call(
        sums_kernel,
        name="sums",
        out_shape=[sh((rows, width), F32)] * 2 + [sh((2 * rows, width), F32)] * 2,
        in_specs=[VMEM_SPEC] * 5,
        out_specs=[VMEM_SPEC] * 4,
        scratch_shapes=[VMEM((rows, width), F32), DMA((2, 1))],
        compiler_params=pltpu.CompilerParams(collective_id=2, has_side_effects=True, vmem_limit_bytes=16 * MIB),
        cost_estimate=pl.CostEstimate(flops=4_000_000_000, bytes_accessed=4 * MIB, transcendentals=0),
    )(dn_b1, du, h, w1, w2)


def grads1_kernel(n, du, zero, order, table_in, dw1, table_g, dw1_v, s_zero, s_w):
    width = n.shape[1]
    n_t = n[...].T
    for j in range(width // TILE):
        at = slice(j * TILE, (j + 1) * TILE)
        dw1_v[at, :] = mm(n_t[at, :], du[...], 1, 0)
        pltpu.make_async_copy(dw1_v.at[pl.ds(j * TILE, TILE)], dw1.at[pl.ds(j * TILE, TILE)], s_w).start()
        if j == 0:
            fill_start(zero, table_g, s_zero, 3)
    pltpu.make_async_copy(dw1_v, dw1, s_w).wait()
    fill_wait(zero, table_g, s_zero, 3)


def grads1(n, du, zero, order, table_g):
    width, hid = n.shape[1], du.shape[1]
    return pl.pallas_call(
        grads1_kernel,
        name="grads1",
        out_shape=[sh((width, hid), F32), sh(table_g.shape, F32)],
        in_specs=[VMEM_SPEC] * 3 + [ANY_SPEC, HBM_SPEC],
        out_specs=[HBM_SPEC, HBM_SPEC],
        input_output_aliases={4: 1},
        scratch_shapes=[VMEM((width, hid), F32), DMA(()), DMA(())],
        compiler_params=pltpu.CompilerParams(vmem_limit_bytes=16 * MIB),
        cost_estimate=pl.CostEstimate(flops=4_000_000_000, bytes_accessed=8 * MIB, transcendentals=0),
    )(n, du, zero, order, table_g)


def grads2_kernel(h, d_full, y_a, y_sib, zero, table_in, dw2, y_own, y_far, table_g, dw2_v, s_zero, s_w):
    rows = y_own.shape[0]
    hid = h.shape[1]
    fill_start(zero, table_g, s_zero, 4)
    for k, out in enumerate((y_own, y_far)):
        at = pl.ds(k * rows, rows)
        out[...] = y_a[at, :] + y_sib[at, :]
    h_t = h[...].T
    for j in range(hid // TILE):
        at = slice(j * TILE, (j + 1) * TILE)
        dw2_v[at, :] = mm(h_t[at, :], d_full[...], 1, 0)
        pltpu.make_async_copy(dw2_v.at[pl.ds(j * TILE, TILE)], dw2.at[pl.ds(j * TILE, TILE)], s_w).start()
    pltpu.make_async_copy(dw2_v, dw2, s_w).wait()
    fill_wait(zero, table_g, s_zero, 4)


def grads2(h, d_full, y_a, y_sib, zero, table_g):
    hid, width = h.shape[1], d_full.shape[1]
    rows = y_a.shape[0] // 2
    return pl.pallas_call(
        grads2_kernel,
        name="grads2",
        out_shape=[sh((hid, width), F32)] + [sh((rows, width), F32)] * 2 + [sh(table_g.shape, F32)],
        in_specs=[VMEM_SPEC] * 5 + [HBM_SPEC],
        out_specs=[HBM_SPEC, VMEM_SPEC, VMEM_SPEC, HBM_SPEC],
        input_output_aliases={5: 3},
        scratch_shapes=[VMEM((hid, width), F32), DMA(()), DMA(())],
        compiler_params=pltpu.CompilerParams(vmem_limit_bytes=16 * MIB),
        cost_estimate=pl.CostEstimate(flops=4_000_000_000, bytes_accessed=8 * MIB, transcendentals=0),
    )(h, d_full, y_a, y_sib, zero, table_g)


def dx_kernel(dn_own, dn_sib, g2, x_own, d_own, gain, order, dx):
    gain_f = gain[...].astype(F32).reshape(1, dx.shape[1])
    for j in range(dx.shape[0] // 16):
        at = pl.ds(j * 16, 16)
        a = (dn_own[at, :] + dn_sib[at, :] + g2[at, :]) * gain_f
        x = x_own[at, :].astype(F32)
        r = lax.rsqrt(jnp.mean(x * x, axis=-1, keepdims=True) + EPS)
        proj = jnp.mean(a * x, axis=-1, keepdims=True)
        dx[at, :] = (d_own[at, :].astype(F32) + r * (a - x * r * r * proj)).astype(BF)


def dx_rows(dn_own, dn_sib, g2, x_own, d_own, gain, order):
    return pl.pallas_call(
        dx_kernel,
        name="dx_rows",
        out_shape=sh(d_own.shape, BF),
        in_specs=[VMEM_SPEC] * 6 + [ANY_SPEC],
        out_specs=VMEM_SPEC,
        compiler_params=pltpu.CompilerParams(vmem_limit_bytes=4 * MIB),
        cost_estimate=pl.CostEstimate(flops=1_000_000_000, bytes_accessed=MIB, transcendentals=0),
    )(dn_own, dn_sib, g2, x_own, d_own, gain, order)


def fill3_kernel(zero, order, table_in, token, table_g, s_zero):
    fill_start(zero, table_g, s_zero, 5)
    token[...] = jnp.zeros_like(token)
    fill_wait(zero, table_g, s_zero, 5)


def fill3(zero, order, table_g):
    return pl.pallas_call(
        fill3_kernel,
        name="fill3",
        out_shape=[sh((8, 128), F32), sh(table_g.shape, F32)],
        in_specs=[VMEM_SPEC, ANY_SPEC, HBM_SPEC],
        out_specs=[VMEM_SPEC, HBM_SPEC],
        input_output_aliases={2: 1},
        scratch_shapes=[DMA(())],
        compiler_params=pltpu.CompilerParams(vmem_limit_bytes=4 * MIB),
        cost_estimate=pl.CostEstimate(flops=4_000_000_000, bytes_accessed=16 * MIB, transcendentals=0),
    )(zero, order, table_g)


def dx_all_kernel(dx, dx_sib, dx_far, order, dx_out, dx_r, sems):
    me = lax.axis_index("tp")
    rows = dx.shape[0]
    remote = swap_with_sibling()
    block = lambda m: pl.ds(pl.multiple_of((me ^ m) * rows, rows), rows)
    copy = remote(dx_far, dx_r, sems, 0)
    copy.start()
    for m, src in enumerate((dx, dx_sib, dx_far)):
        dx_out[block(m), :] = src[...]
    copy.wait()
    dx_out[block(3), :] = dx_r[...]


def dx_all(dx, dx_sib, dx_far, order):
    rows, width = dx.shape
    return pl.pallas_call(
        dx_all_kernel,
        name="dx_all",
        out_shape=sh((4 * rows, width), BF),
        in_specs=[VMEM_SPEC] * 3 + [ANY_SPEC],
        out_specs=VMEM_SPEC,
        scratch_shapes=[VMEM((rows, width), BF), DMA((2, 1))],
        compiler_params=pltpu.CompilerParams(collective_id=3, has_side_effects=True, vmem_limit_bytes=4 * MIB),
        cost_estimate=pl.CostEstimate(flops=2_000_000_000, bytes_accessed=MIB, transcendentals=0),
    )(dx, dx_sib, dx_far, order)


def put_kernel(puts, same, dx, zero, table_in, table_g, token, puts_s, total, s_in, s_row, s_zero):
    fill_start(zero, table_g, s_zero, LATE)
    tokens = dx.shape[0]
    load = pltpu.make_async_copy(puts, puts_s, s_in)
    load.start()
    total[...] = mm(same[...], dx[...], 1, 0)
    token[...] = jnp.zeros_like(token)
    load.wait()
    fill_wait(zero, table_g, s_zero, LATE)
    count = puts_s[tokens]

    def put(i):
        word = puts_s[i]
        pltpu.make_async_copy(total.at[pl.ds(word >> 16, 1)], table_g.at[pl.ds(word & 0xFFFF, 1)], s_row).start()

    def put_four(i, carry):
        for k in range(4):
            put(i * 4 + k)
        return carry

    def put_one(i, carry):
        put(i)
        return carry

    lax.fori_loop(0, count >> 2, put_four, 0)
    lax.fori_loop((count >> 2) * 4, count, put_one, 0)

    def put_wait(size):
        def body(i, carry):
            pltpu.make_async_copy(total.at[pl.ds(0, size)], table_g.at[pl.ds(0, size)], s_row).wait()
            return carry

        return body

    lax.fori_loop(0, count >> 3, put_wait(8), 0)
    lax.fori_loop(0, count & 7, put_wait(1), 0)


def put_rows(puts, same, dx, zero, table_g):
    return pl.pallas_call(
        put_kernel,
        name="put_rows",
        out_shape=[sh(table_g.shape, F32), sh((8, 128), F32)],
        in_specs=[ANY_SPEC, VMEM_SPEC, VMEM_SPEC, VMEM_SPEC, HBM_SPEC],
        out_specs=[HBM_SPEC, VMEM_SPEC],
        input_output_aliases={4: 0},
        scratch_shapes=[pltpu.SMEM(puts.shape, I32), VMEM(dx.shape, F32), DMA(()), DMA(()), DMA(())],
        compiler_params=pltpu.CompilerParams(vmem_limit_bytes=4 * MIB),
        cost_estimate=pl.CostEstimate(flops=3_000_000_000, bytes_accessed=2 * MIB, transcendentals=0),
    )(puts, same, dx, zero, table_g)


def finish_kernel(x, y, y_in, order, out):
    out[...] = (x[pl.ds(0, out.shape[0]), :].astype(F32) + (y[...] + y_in[...])).astype(BF)


def finish(x, y, y_in, order):
    return pl.pallas_call(
        finish_kernel,
        name="finish",
        out_shape=sh(y.shape, BF),
        in_specs=[VMEM_SPEC] * 3 + [ANY_SPEC],
        out_specs=VMEM_SPEC,
        compiler_params=pltpu.CompilerParams(vmem_limit_bytes=4 * MIB),
        cost_estimate=pl.CostEstimate(flops=1_000_000_000, bytes_accessed=MIB, transcendentals=0),
    )(x, y, y_in, order)


def solution(mesh):
    tp = mesh.shape["tp"]

    def permute(x, hop):
        return lax.ppermute(x, "tp", [(i, i ^ hop) for i in range(tp)])

    def shard_step(ids, table, gain, w1, w2, d_out):
        part, rows_mine, same, zero, d_table = lookup(ids, table)
        part, d_send = lax.optimization_barrier((part, d_out))
        d_far = permute(d_send, 2)
        send, w1 = pair(part, w1)
        got = permute(send, 2)
        d_own_s = permute(d_out, 1)
        puts, w2, d_table = fill1(rows_mine, zero, w2, send, d_table)
        d_far_s = permute(d_far, 1)
        x_f, n_a, h_a, du_a = share(send, got, d_out, d_far, w1, w2, gain)
        ds = (d_out, d_far, d_own_s, d_far_s)
        n, h, du, d_full, dn_b0, dn_b1, d_table = mlp(x_f, ds, n_a, h_a, du_a, w1, w2, gain, zero, d_table)
        dn_own, dn_far, y_a, y_b = sums(dn_b1, du, h, w1, w2)
        g2 = permute(dn_far, 2)
        dn_sib = permute(dn_b0, 1)
        y_sib = permute(y_b, 1)
        d_w1, d_table = grads1(n, du, zero, dn_own, d_table)
        d_w2, y_own, y_far, d_table = grads2(h, d_full, y_a, y_sib, zero, d_table)
        dx = dx_rows(dn_own, dn_sib, g2, x_f, d_out, gain, y_own)
        dx_far = permute(dx, 2)
        dx_sib = permute(dx, 1)
        dx, y_far = lax.optimization_barrier((dx, y_far))
        y_in = permute(y_far, 2)
        token, d_table = fill3(zero, dx, d_table)
        dx_full = dx_all(dx, dx_sib, dx_far, token)
        d_table, done = put_rows(puts, same, dx_full, zero, d_table)
        out = finish(x_f, y_own, y_in, done)
        return out, d_table, d_w1, d_w2

    return jax.shard_map(
        shard_step,
        mesh=mesh,
        in_specs=(P("dp"), P("tp", None), P(None), P(None, "tp"), P("tp", None), P(("dp", "tp"), None)),
        out_specs=(P(("dp", "tp"), None), P(("dp", "tp"), None), P("dp", "tp"), P(("dp", "tp"), None)),
        check_vma=False,
    )
```

```python
import jax
import jax.numpy as jnp
from jax import lax
from jax.experimental import pallas as pl
from jax.experimental.pallas import tpu as pltpu
from jax.sharding import PartitionSpec as P

EPS = 1e-6
BF = jnp.bfloat16
F32 = jnp.float32
I32 = jnp.int32
GELU_C = 0.7978845608028654
GELU_A = 0.044715
VMEM = pltpu.VMEM
SMEM_SPEC = pl.BlockSpec(memory_space=pltpu.SMEM)
ANY_SPEC = pl.BlockSpec(memory_space=pl.ANY)
HBM_SPEC = pl.BlockSpec(memory_space=pltpu.HBM)
VMEM_SPEC = pl.BlockSpec(memory_space=VMEM)
DMA = pltpu.SemaphoreType.DMA
TILE = 256
ZERO_ROWS = 96
FILL_COUNTS = ((24, 54, 13, 9, 9, 19, 3), (4, 51, 13, 10, 10, 23, 20), (4, 57, 13, 12, 11, 26, 8))
LATE = 6
MIB = 1 << 20
LOOKUP_VMEM = 48 * MIB
PAIR_VMEM = 8 * MIB


def mm(a, b, ca, cb):
    return lax.dot_general(a, b, (((ca,), (cb,)), ((), ())), preferred_element_type=F32)


def in_hbm(x):
    return pltpu.with_memory_space_constraint(x, pltpu.HBM)


def sh(shape, dtype):
    return jax.ShapeDtypeStruct(shape, dtype)


def fill_copy(zero, table_g, sem, i):
    return pltpu.make_async_copy(zero, table_g.at[pl.ds(pl.multiple_of(i * ZERO_ROWS, ZERO_ROWS), ZERO_ROWS)], sem)


def fill_range(part):
    group, chip = lax.axis_index("dp"), lax.axis_index("tp") >> 1
    (lo0, hi0), (lo1, hi1), (lo2, hi2) = ((sum(c[:part]), sum(c[:part + 1])) for c in FILL_COUNTS)
    pick = lambda a, b, c: group * c + (1 - group) * (a + chip * (b - a))
    return pick(lo0, lo1, lo2), pick(hi0, hi1, hi2)


def fill_start(zero, table_g, sem, part):
    def body(i, carry):
        fill_copy(zero, table_g, sem, i).start()
        return carry

    lax.fori_loop(*fill_range(part), body, 0)


def fill_wait(zero, table_g, sem, part):
    def body(i, carry):
        fill_copy(zero, table_g, sem, i).wait()
        return carry

    lax.fori_loop(*fill_range(part), body, 0)


def swap_with_sibling():
    sib = lax.axis_index("tp") ^ 1
    barrier = pltpu.get_barrier_semaphore()
    pl.semaphore_signal(barrier, inc=1, device_id={"tp": sib}, device_id_type=pl.DeviceIdType.MESH)
    pl.semaphore_wait(barrier, 1)

    def remote(src, dst, sems, i):
        return pltpu.make_async_remote_copy(
            src_ref=src, dst_ref=dst, send_sem=sems.at[0, i], recv_sem=sems.at[1, i],
            device_id={"tp": sib}, device_id_type=pl.DeviceIdType.MESH)

    return remote


def lookup_kernel(ids, ids_row, table, part, rows_mine, same, zero, table_g, ids_s, ids_v, pairs, sems, s_zero, s_ids):
    tokens, vocab = part.shape[0], table.shape[0]
    base = lax.axis_index("tp") * vocab
    group = 64
    groups = tokens // group
    loads = [pltpu.make_async_copy(ids, ids_s, s_ids.at[0]), pltpu.make_async_copy(ids_row, ids_v, s_ids.at[1])]
    for c in loads:
        c.start()
    zero[...] = jnp.zeros_like(zero)
    fill_start(zero, table_g, s_zero, 0)
    loads[0].wait()

    def fetch(k, carry):
        for i in range(group):
            token = k * group + i
            lid = ids_s[token] - base
            owned = (lid >= 0) & (lid < vocab)
            row = jnp.where(owned, lid & -2, 2 * token)
            pltpu.make_async_copy(table.at[pl.ds(pl.multiple_of(row, 2), 2)], pairs.at[k, pl.ds(2 * i, 2)], sems.at[k]).start()
        return carry

    lax.fori_loop(0, groups, fetch, 0)
    loads[1].wait()
    row = jnp.broadcast_to(ids_v[...].astype(F32), (tokens, tokens))
    col = row.T
    equal = row == col
    same[...] = jnp.where(equal, 1.0, 0.0).astype(BF)
    earlier = lax.broadcasted_iota(I32, (tokens, tokens), 0) < lax.broadcasted_iota(I32, (tokens, tokens), 1)
    repeat = jnp.max(jnp.where(equal & earlier, 1, 0), axis=0, keepdims=True)
    mine = ids_v[...] - base
    rows_mine[...] = jnp.where((mine >= 0) & (mine < vocab) & (repeat == 0), mine, -1)
    lid = col.astype(I32) - base
    lane = lax.broadcasted_iota(I32, (group, 2 * group), 1)
    first = lax.broadcasted_iota(I32, (group, 2 * group), 0) * 2
    for k in range(groups):
        at = lid[k * group:(k + 1) * group, :2 * group]
        owned = (at >= 0) & (at < vocab)
        pick = jnp.where(owned & (lane == first + (at & 1)), 1.0, 0.0).astype(BF)
        pltpu.make_async_copy(table.at[pl.ds(0, group * 2)], pairs.at[k], sems.at[k]).wait()
        part[pl.ds(k * group, group), :] = mm(pick, pairs[k], 1, 0).astype(BF)
    fill_wait(zero, table_g, s_zero, 0)


def lookup(ids, table):
    tokens, (vocab, width) = ids.shape[0], table.shape
    return pl.pallas_call(
        lookup_kernel,
        name="lookup",
        out_shape=[sh((tokens, width), BF), sh((1, tokens), I32), sh((tokens, tokens), BF), sh((ZERO_ROWS, width), F32), sh((vocab, width), F32)],
        in_specs=[HBM_SPEC] * 3,
        out_specs=[VMEM_SPEC] * 4 + [HBM_SPEC],
        scratch_shapes=[pltpu.SMEM((tokens,), I32), VMEM((1, tokens), I32), VMEM((4, tokens // 2, width), BF), DMA((4,)), DMA(()), DMA((2,))],
        compiler_params=pltpu.CompilerParams(vmem_limit_bytes=LOOKUP_VMEM),
        cost_estimate=pl.CostEstimate(flops=5_000_000_000, bytes_accessed=10 * MIB, transcendentals=0),
    )(in_hbm(ids), in_hbm(ids.reshape(1, tokens)), in_hbm(table))


def pair_kernel(part, w1, send, w1_v, part_r, sems, s_in):
    me = lax.axis_index("tp")
    rows = part.shape[0] // 4
    blocks = (me, me ^ 2, me ^ 1, me ^ 3)
    load = pltpu.make_async_copy(w1, w1_v, s_in)
    load.start()
    remote = swap_with_sibling()
    block = lambda k: pl.ds(pl.multiple_of(blocks[k] * rows, rows), rows)
    copies = [remote(part.at[block(2 + k)], part_r.at[pl.ds(k * rows, rows)], sems, k) for k in range(2)]
    for c in copies:
        c.start()
    for k in range(2):
        copies[k].wait()
        at = pl.ds(k * rows, rows)
        send[at, :] = part[block(k), :] + part_r[at, :]
    load.wait()


def pair(part, w1):
    rows, width = part.shape[0] // 4, part.shape[1]
    return pl.pallas_call(
        pair_kernel,
        name="pair",
        out_shape=[sh((2 * rows, width), BF), sh(w1.shape, BF)],
        in_specs=[VMEM_SPEC, HBM_SPEC],
        out_specs=[VMEM_SPEC] * 2,
        scratch_shapes=[VMEM((2 * rows, width), BF), DMA((2, 2)), DMA(())],
        compiler_params=pltpu.CompilerParams(collective_id=0, has_side_effects=True, vmem_limit_bytes=PAIR_VMEM),
        cost_estimate=pl.CostEstimate(flops=3_000_000_000, bytes_accessed=MIB, transcendentals=0),
    )(part, in_hbm(w1))


def fill1_kernel(rows_mine, zero, w2, order, table_in, puts, w2_v, table_g, mine_s, puts_s, s_zero, s_list, s_w):
    load = pltpu.make_async_copy(rows_mine, mine_s, s_list)
    load.start()
    load_w = pltpu.make_async_copy(w2, w2_v, s_w)
    load_w.start()
    fill_start(zero, table_g, s_zero, 1)
    tokens = rows_mine.shape[1]
    load.wait()

    def body(i, count):
        lid = mine_s[0, i]
        puts_s[count] = lid | (i << 16)
        return count + (lid >= 0).astype(I32)

    puts_s[tokens] = lax.fori_loop(0, tokens, body, 0, unroll=8)
    store = pltpu.make_async_copy(puts_s, puts, s_list)
    store.start()
    store.wait()
    load_w.wait()
    fill_wait(zero, table_g, s_zero, 1)


def fill1(rows_mine, zero, w2, order, table_g):
    tokens = rows_mine.shape[1]
    return pl.pallas_call(
        fill1_kernel,
        name="fill1",
        out_shape=[sh((2 * tokens,), I32), sh(w2.shape, BF), sh(table_g.shape, F32)],
        in_specs=[ANY_SPEC, VMEM_SPEC, HBM_SPEC, ANY_SPEC, HBM_SPEC],
        out_specs=[ANY_SPEC, VMEM_SPEC, HBM_SPEC],
        input_output_aliases={4: 2},
        scratch_shapes=[pltpu.SMEM((1, tokens), I32), pltpu.SMEM((2 * tokens,), I32), DMA(()), DMA(()), DMA(())],
        compiler_params=pltpu.CompilerParams(vmem_limit_bytes=8 * MIB),
        cost_estimate=pl.CostEstimate(flops=9_000_000_000, bytes_accessed=20 * MIB, transcendentals=0),
    )(rows_mine, zero, in_hbm(w2), order, table_g)


def mlp_half(x, d, n, h, du, at, w1, w2, gain):
    first, count = at
    width, hid = n.shape[1], h.shape[1]
    gain_f = gain[...].astype(F32).reshape(1, width)
    for j in range(count // 32):
        rows = pl.ds(first + j * 32, 32)
        x_f = x[rows, :].astype(F32)
        r = lax.rsqrt(jnp.mean(x_f * x_f, axis=-1, keepdims=True) + EPS)
        n[rows, :] = (x_f * r * gain_f).astype(BF)
    rows = pl.ds(first, count)
    for j in range(hid // TILE):
        cols = pl.ds(j * TILE, TILE)
        g = mm(d[rows, :], w2[cols, :], 1, 1).astype(BF).astype(F32)
        u = mm(n[rows, :], w1[:, cols], 1, 0).astype(BF).astype(F32)
        t = jnp.tanh(GELU_C * (u + GELU_A * (u * u * u)))
        cdf = 0.5 * (1.0 + t)
        h[rows, cols] = (u * cdf).astype(BF)
        du[rows, cols] = (g * (cdf + u * (0.5 * (1.0 - t * t)) * (GELU_C * (1.0 + 3.0 * GELU_A * (u * u))))).astype(BF)


def share_kernel(send, got, d_own, d_far, w1, w2, gain, x_f, n_a, h_a, du_a, d_far_s, x_r, d_a, d_r, sems):
    rows = d_own.shape[0]
    half = 2 * rows
    remote = swap_with_sibling()
    copies = []
    for k in range(2):
        at, other = pl.ds(k * rows, rows), pl.ds((1 - k) * rows, rows)
        x_f[at, :] = send[at, :] + got[other, :]
        copies.append(remote(x_f.at[at], x_r.at[at], sems, k))
        copies[-1].start()
    copies.append(remote(d_far, d_r, sems, 2))
    copies[-1].start()
    for k, src in enumerate((d_own, d_far)):
        d_a[pl.ds(k * rows, rows), :] = src[...]
    mlp_half(x_f, d_a, n_a, h_a, du_a, (0, half), w1, w2, gain)
    for k in range(2):
        copies[k].wait()
        x_f[pl.ds(half + k * rows, rows), :] = x_r[pl.ds(k * rows, rows), :]
    copies[2].wait()
    d_far_s[...] = d_r[...]


def share(send, got, d_own, d_far, w1, w2, gain):
    rows, width = d_own.shape
    hid = w1.shape[1]
    return pl.pallas_call(
        share_kernel,
        name="share",
        out_shape=[sh((4 * rows, width), BF), sh((2 * rows, width), BF)] + [sh((2 * rows, hid), BF)] * 2 + [sh((rows, width), BF)],
        in_specs=[VMEM_SPEC] * 7,
        out_specs=[VMEM_SPEC] * 5,
        scratch_shapes=[VMEM((2 * rows, width), BF), VMEM((2 * rows, width), BF), VMEM((rows, width), BF), DMA((2, 3))],
        compiler_params=pltpu.CompilerParams(collective_id=1, has_side_effects=True, vmem_limit_bytes=16 * MIB),
        cost_estimate=pl.CostEstimate(flops=3_000_000_000, bytes_accessed=MIB, transcendentals=0),
    )(send, got, d_own, d_far, w1, w2, gain)


def mlp_kernel(x_f, d_own, d_far, d_own_s, d_far_s, n_a, h_a, du_a, w1, w2, gain, zero, table_in,
               n, h, du, d_full, dn_b0, dn_b1, table_g, s_zero):
    fill_start(zero, table_g, s_zero, 2)
    rows = d_own.shape[0]
    for k, src in enumerate((d_own, d_far, d_own_s, d_far_s)):
        d_full[pl.ds(k * rows, rows), :] = src[...]
    tokens, width = n.shape
    half = tokens // 2
    for out, src in ((n, n_a), (h, h_a), (du, du_a)):
        out[pl.ds(0, half), :] = src[...]
    mlp_half(x_f, d_full, n, h, du, (half, half), w1, w2, gain)
    for j in range(width // TILE):
        cols = pl.ds(j * TILE, TILE)
        dn = mm(du[pl.ds(half, half), :], w1[cols, :], 1, 1)
        dn_b0[:, cols] = dn[:half // 2]
        dn_b1[:, cols] = dn[half // 2:]
    fill_wait(zero, table_g, s_zero, 2)


def mlp(x_f, ds, n_a, h_a, du_a, w1, w2, gain, zero, table_g):
    tokens, width = x_f.shape
    hid = w1.shape[1]
    return pl.pallas_call(
        mlp_kernel,
        name="mlp",
        out_shape=[sh((tokens, width), BF), sh((tokens, hid), BF), sh((tokens, hid), BF), sh((tokens, width), BF),
                   sh((tokens // 4, width), F32), sh((tokens // 4, width), F32), sh(table_g.shape, F32)],
        in_specs=[VMEM_SPEC] * 12 + [HBM_SPEC],
        out_specs=[VMEM_SPEC] * 6 + [HBM_SPEC],
        input_output_aliases={12: 6},
        scratch_shapes=[DMA(())],
        compiler_params=pltpu.CompilerParams(vmem_limit_bytes=16 * MIB),
        cost_estimate=pl.CostEstimate(flops=6_000_000_000, bytes_accessed=4 * MIB, transcendentals=0),
    )(x_f, *ds, n_a, h_a, du_a, w1, w2, gain, zero, table_g)


def sums_kernel(dn_b0, dn_b1, du, h, w1, w2, dn_own, dn_far, y_a, y_b, dn_r, sems):
    rows, width = dn_own.shape
    half = 2 * rows
    remote = swap_with_sibling()
    copy = remote(dn_b1, dn_r, sems, 0)
    copy.start()
    for j in range(width // TILE):
        cols = pl.ds(j * TILE, TILE)
        dn = mm(du[pl.ds(0, half), :], w1[cols, :], 1, 1)
        dn_own[:, cols] = dn[:rows]
        dn_far[:, cols] = dn[rows:]
    for j in range(width // TILE):
        cols = pl.ds(j * TILE, TILE)
        y = mm(h[...], w2[:, cols], 1, 0)
        y_a[:, cols] = y[:half]
        y_b[pl.ds(0, half), cols] = y[half:]
    y_b[pl.ds(half, rows), :] = dn_b0[...]
    copy.wait()
    dn_far[...] += dn_r[...]


def sums(dn_b0, dn_b1, du, h, w1, w2):
    rows, width = dn_b1.shape
    return pl.pallas_call(
        sums_kernel,
        name="sums",
        out_shape=[sh((rows, width), F32)] * 2 + [sh((2 * rows, width), F32), sh((3 * rows, width), F32)],
        in_specs=[VMEM_SPEC] * 6,
        out_specs=[VMEM_SPEC] * 4,
        scratch_shapes=[VMEM((rows, width), F32), DMA((2, 1))],
        compiler_params=pltpu.CompilerParams(collective_id=2, has_side_effects=True, vmem_limit_bytes=16 * MIB),
        cost_estimate=pl.CostEstimate(flops=4_000_000_000, bytes_accessed=4 * MIB, transcendentals=0),
    )(dn_b0, dn_b1, du, h, w1, w2)


def grads1_kernel(n, du, zero, order, table_in, dw1, table_g, dw1_v, s_zero, s_w):
    width = n.shape[1]
    n_t = n[...].T
    for j in range(width // TILE):
        at = slice(j * TILE, (j + 1) * TILE)
        dw1_v[at, :] = mm(n_t[at, :], du[...], 1, 0)
        pltpu.make_async_copy(dw1_v.at[pl.ds(j * TILE, TILE)], dw1.at[pl.ds(j * TILE, TILE)], s_w).start()
        if j == 0:
            fill_start(zero, table_g, s_zero, 3)
    pltpu.make_async_copy(dw1_v, dw1, s_w).wait()
    fill_wait(zero, table_g, s_zero, 3)


def grads1(n, du, zero, order, table_g):
    width, hid = n.shape[1], du.shape[1]
    return pl.pallas_call(
        grads1_kernel,
        name="grads1",
        out_shape=[sh((width, hid), F32), sh(table_g.shape, F32)],
        in_specs=[VMEM_SPEC] * 3 + [ANY_SPEC, HBM_SPEC],
        out_specs=[HBM_SPEC, HBM_SPEC],
        input_output_aliases={4: 1},
        scratch_shapes=[VMEM((width, hid), F32), DMA(()), DMA(())],
        compiler_params=pltpu.CompilerParams(vmem_limit_bytes=16 * MIB),
        cost_estimate=pl.CostEstimate(flops=4_000_000_000, bytes_accessed=8 * MIB, transcendentals=0),
    )(n, du, zero, order, table_g)


def grads2_kernel(h, d_full, y_a, y_sib, zero, table_in, dw2, y_own, y_far, table_g, dw2_v, s_zero, s_w):
    rows = y_own.shape[0]
    hid = h.shape[1]
    fill_start(zero, table_g, s_zero, 4)
    for k, out in enumerate((y_own, y_far)):
        at = pl.ds(k * rows, rows)
        out[...] = y_a[at, :] + y_sib[at, :]
    h_t = h[...].T
    for j in range(hid // TILE):
        at = slice(j * TILE, (j + 1) * TILE)
        dw2_v[at, :] = mm(h_t[at, :], d_full[...], 1, 0)
        pltpu.make_async_copy(dw2_v.at[pl.ds(j * TILE, TILE)], dw2.at[pl.ds(j * TILE, TILE)], s_w).start()
    pltpu.make_async_copy(dw2_v, dw2, s_w).wait()
    fill_wait(zero, table_g, s_zero, 4)


def grads2(h, d_full, y_a, y_sib, zero, table_g):
    hid, width = h.shape[1], d_full.shape[1]
    rows = y_a.shape[0] // 2
    return pl.pallas_call(
        grads2_kernel,
        name="grads2",
        out_shape=[sh((hid, width), F32)] + [sh((rows, width), F32)] * 2 + [sh(table_g.shape, F32)],
        in_specs=[VMEM_SPEC] * 5 + [HBM_SPEC],
        out_specs=[HBM_SPEC, VMEM_SPEC, VMEM_SPEC, HBM_SPEC],
        input_output_aliases={5: 3},
        scratch_shapes=[VMEM((hid, width), F32), DMA(()), DMA(())],
        compiler_params=pltpu.CompilerParams(vmem_limit_bytes=16 * MIB),
        cost_estimate=pl.CostEstimate(flops=4_000_000_000, bytes_accessed=8 * MIB, transcendentals=0),
    )(h, d_full, y_a, y_sib, zero, table_g)


def dx_kernel(dn_own, y_sib, g2, x_own, d_own, gain, order, dx):
    gain_f = gain[...].astype(F32).reshape(1, dx.shape[1])
    for j in range(dx.shape[0] // 16):
        at = pl.ds(j * 16, 16)
        sib_at = pl.ds(2 * dx.shape[0] + j * 16, 16)
        a = (dn_own[at, :] + y_sib[sib_at, :] + g2[at, :]) * gain_f
        x = x_own[at, :].astype(F32)
        r = lax.rsqrt(jnp.mean(x * x, axis=-1, keepdims=True) + EPS)
        proj = jnp.mean(a * x, axis=-1, keepdims=True)
        dx[at, :] = (d_own[at, :].astype(F32) + r * (a - x * r * r * proj)).astype(BF)


def dx_rows(dn_own, y_sib, g2, x_own, d_own, gain, order):
    return pl.pallas_call(
        dx_kernel,
        name="dx_rows",
        out_shape=sh(d_own.shape, BF),
        in_specs=[VMEM_SPEC] * 6 + [ANY_SPEC],
        out_specs=VMEM_SPEC,
        compiler_params=pltpu.CompilerParams(vmem_limit_bytes=4 * MIB),
        cost_estimate=pl.CostEstimate(flops=1_000_000_000, bytes_accessed=MIB, transcendentals=0),
    )(dn_own, y_sib, g2, x_own, d_own, gain, order)


def fill3_kernel(zero, order, table_in, token, table_g, s_zero):
    fill_start(zero, table_g, s_zero, 5)
    token[...] = jnp.zeros_like(token)
    fill_wait(zero, table_g, s_zero, 5)


def fill3(zero, order, table_g):
    return pl.pallas_call(
        fill3_kernel,
        name="fill3",
        out_shape=[sh((8, 128), F32), sh(table_g.shape, F32)],
        in_specs=[VMEM_SPEC, ANY_SPEC, HBM_SPEC],
        out_specs=[VMEM_SPEC, HBM_SPEC],
        input_output_aliases={2: 1},
        scratch_shapes=[DMA(())],
        compiler_params=pltpu.CompilerParams(vmem_limit_bytes=4 * MIB),
        cost_estimate=pl.CostEstimate(flops=4_000_000_000, bytes_accessed=16 * MIB, transcendentals=0),
    )(zero, order, table_g)


def dx_all_kernel(dx, dx_sib, dx_far, order, dx_out, dx_r, sems):
    me = lax.axis_index("tp")
    rows = dx.shape[0]
    remote = swap_with_sibling()
    block = lambda m: pl.ds(pl.multiple_of((me ^ m) * rows, rows), rows)
    copy = remote(dx_far, dx_r, sems, 0)
    copy.start()
    for m, src in enumerate((dx, dx_sib, dx_far)):
        dx_out[block(m), :] = src[...]
    copy.wait()
    dx_out[block(3), :] = dx_r[...]


def dx_all(dx, dx_sib, dx_far, order):
    rows, width = dx.shape
    return pl.pallas_call(
        dx_all_kernel,
        name="dx_all",
        out_shape=sh((4 * rows, width), BF),
        in_specs=[VMEM_SPEC] * 3 + [ANY_SPEC],
        out_specs=VMEM_SPEC,
        scratch_shapes=[VMEM((rows, width), BF), DMA((2, 1))],
        compiler_params=pltpu.CompilerParams(collective_id=3, has_side_effects=True, vmem_limit_bytes=4 * MIB),
        cost_estimate=pl.CostEstimate(flops=2_000_000_000, bytes_accessed=MIB, transcendentals=0),
    )(dx, dx_sib, dx_far, order)


def put_kernel(puts, same, dx, zero, table_in, table_g, token, puts_s, total, s_in, s_row, s_zero):
    fill_start(zero, table_g, s_zero, LATE)
    tokens = dx.shape[0]
    load = pltpu.make_async_copy(puts, puts_s, s_in)
    load.start()
    total[...] = mm(same[...], dx[...], 1, 0)
    token[...] = jnp.zeros_like(token)
    load.wait()
    fill_wait(zero, table_g, s_zero, LATE)
    count = puts_s[tokens]

    def put(i):
        word = puts_s[i]
        pltpu.make_async_copy(total.at[pl.ds(word >> 16, 1)], table_g.at[pl.ds(word & 0xFFFF, 1)], s_row).start()

    def put_four(i, carry):
        for k in range(4):
            put(i * 4 + k)
        return carry

    def put_one(i, carry):
        put(i)
        return carry

    lax.fori_loop(0, count >> 2, put_four, 0)
    lax.fori_loop((count >> 2) * 4, count, put_one, 0)

    def put_wait(size):
        def body(i, carry):
            pltpu.make_async_copy(total.at[pl.ds(0, size)], table_g.at[pl.ds(0, size)], s_row).wait()
            return carry

        return body

    lax.fori_loop(0, count >> 3, put_wait(8), 0)
    lax.fori_loop(0, count & 7, put_wait(1), 0)


def put_rows(puts, same, dx, zero, table_g):
    return pl.pallas_call(
        put_kernel,
        name="put_rows",
        out_shape=[sh(table_g.shape, F32), sh((8, 128), F32)],
        in_specs=[ANY_SPEC, VMEM_SPEC, VMEM_SPEC, VMEM_SPEC, HBM_SPEC],
        out_specs=[HBM_SPEC, VMEM_SPEC],
        input_output_aliases={4: 0},
        scratch_shapes=[pltpu.SMEM(puts.shape, I32), VMEM(dx.shape, F32), DMA(()), DMA(()), DMA(())],
        compiler_params=pltpu.CompilerParams(vmem_limit_bytes=4 * MIB),
        cost_estimate=pl.CostEstimate(flops=3_000_000_000, bytes_accessed=2 * MIB, transcendentals=0),
    )(puts, same, dx, zero, table_g)


def finish_kernel(x, y, y_in, order, out):
    out[...] = (x[pl.ds(0, out.shape[0]), :].astype(F32) + (y[...] + y_in[...])).astype(BF)


def finish(x, y, y_in, order):
    return pl.pallas_call(
        finish_kernel,
        name="finish",
        out_shape=sh(y.shape, BF),
        in_specs=[VMEM_SPEC] * 3 + [ANY_SPEC],
        out_specs=VMEM_SPEC,
        compiler_params=pltpu.CompilerParams(vmem_limit_bytes=4 * MIB),
        cost_estimate=pl.CostEstimate(flops=1_000_000_000, bytes_accessed=MIB, transcendentals=0),
    )(x, y, y_in, order)


def solution(mesh):
    tp = mesh.shape["tp"]

    def permute(x, hop):
        return lax.ppermute(x, "tp", [(i, i ^ hop) for i in range(tp)])

    def shard_step(ids, table, gain, w1, w2, d_out):
        part, rows_mine, same, zero, d_table = lookup(ids, table)
        part, d_send = lax.optimization_barrier((part, d_out))
        d_far = permute(d_send, 2)
        send, w1 = pair(part, w1)
        got = permute(send, 2)
        d_own_s = permute(d_out, 1)
        puts, w2, d_table = fill1(rows_mine, zero, w2, send, d_table)
        x_f, n_a, h_a, du_a, d_far_s = share(send, got, d_out, d_far, w1, w2, gain)
        ds = (d_out, d_far, d_own_s, d_far_s)
        n, h, du, d_full, dn_b0, dn_b1, d_table = mlp(x_f, ds, n_a, h_a, du_a, w1, w2, gain, zero, d_table)
        dn_own, dn_far, y_a, y_b = sums(dn_b0, dn_b1, du, h, w1, w2)
        g2 = permute(dn_far, 2)
        y_sib = permute(y_b, 1)
        d_w1, d_table = grads1(n, du, zero, dn_own, d_table)
        d_w2, y_own, y_far, d_table = grads2(h, d_full, y_a, y_sib, zero, d_table)
        dx = dx_rows(dn_own, y_sib, g2, x_f, d_out, gain, y_own)
        dx_far = permute(dx, 2)
        dx_sib = permute(dx, 1)
        dx, y_far = lax.optimization_barrier((dx, y_far))
        y_in = permute(y_far, 2)
        token, d_table = fill3(zero, dx, d_table)
        dx_full = dx_all(dx, dx_sib, dx_far, token)
        d_table, done = put_rows(puts, same, dx_full, zero, d_table)
        out = finish(x_f, y_own, y_in, done)
        return out, d_table, d_w1, d_w2

    return jax.shard_map(
        shard_step,
        mesh=mesh,
        in_specs=(P("dp"), P("tp", None), P(None), P(None, "tp"), P("tp", None), P(("dp", "tp"), None)),
        out_specs=(P(("dp", "tp"), None), P(("dp", "tp"), None), P("dp", "tp"), P(("dp", "tp"), None)),
        check_vma=False,
    )
```

```python
import jax
import jax.numpy as jnp
from jax import lax
from jax.experimental import pallas as pl
from jax.experimental.pallas import tpu as pltpu
from jax.sharding import PartitionSpec as P

EPS = 1e-6
BF = jnp.bfloat16
F32 = jnp.float32
I32 = jnp.int32
GELU_C = 0.7978845608028654
GELU_A = 0.044715
VMEM = pltpu.VMEM
SMEM_SPEC = pl.BlockSpec(memory_space=pltpu.SMEM)
ANY_SPEC = pl.BlockSpec(memory_space=pl.ANY)
HBM_SPEC = pl.BlockSpec(memory_space=pltpu.HBM)
VMEM_SPEC = pl.BlockSpec(memory_space=VMEM)
DMA = pltpu.SemaphoreType.DMA
TILE = 256
ZERO_ROWS = 96
FILL_COUNTS = ((22, 54, 2, 10, 10, 26, 7), (3, 50, 2, 9, 9, 31, 27), (4, 57, 13, 10, 9, 27, 11))
LATE = 6
MIB = 1 << 20
LOOKUP_VMEM = 48 * MIB
PAIR_VMEM = 8 * MIB


def mm(a, b, ca, cb):
    return lax.dot_general(a, b, (((ca,), (cb,)), ((), ())), preferred_element_type=F32)


def in_hbm(x):
    return pltpu.with_memory_space_constraint(x, pltpu.HBM)


def sh(shape, dtype):
    return jax.ShapeDtypeStruct(shape, dtype)


def fill_copy(zero, table_g, sem, i):
    return pltpu.make_async_copy(zero, table_g.at[pl.ds(pl.multiple_of(i * ZERO_ROWS, ZERO_ROWS), ZERO_ROWS)], sem)


def fill_range(part):
    group, chip = lax.axis_index("dp"), lax.axis_index("tp") >> 1
    (lo0, hi0), (lo1, hi1), (lo2, hi2) = ((sum(c[:part]), sum(c[:part + 1])) for c in FILL_COUNTS)
    pick = lambda a, b, c: group * c + (1 - group) * (a + chip * (b - a))
    return pick(lo0, lo1, lo2), pick(hi0, hi1, hi2)


def fill_start(zero, table_g, sem, part):
    def body(i, carry):
        fill_copy(zero, table_g, sem, i).start()
        return carry

    lax.fori_loop(*fill_range(part), body, 0)


def fill_wait(zero, table_g, sem, part):
    def body(i, carry):
        fill_copy(zero, table_g, sem, i).wait()
        return carry

    lax.fori_loop(*fill_range(part), body, 0)


def swap_with_sibling():
    sib = lax.axis_index("tp") ^ 1
    barrier = pltpu.get_barrier_semaphore()
    pl.semaphore_signal(barrier, inc=1, device_id={"tp": sib}, device_id_type=pl.DeviceIdType.MESH)
    pl.semaphore_wait(barrier, 1)

    def remote(src, dst, sems, i):
        return pltpu.make_async_remote_copy(
            src_ref=src, dst_ref=dst, send_sem=sems.at[0, i], recv_sem=sems.at[1, i],
            device_id={"tp": sib}, device_id_type=pl.DeviceIdType.MESH)

    return remote


def lookup_kernel(ids, ids_row, table, part, rows_mine, same, zero, table_g, ids_s, ids_v, pairs, sems, s_zero, s_ids):
    tokens, vocab = part.shape[0], table.shape[0]
    base = lax.axis_index("tp") * vocab
    group = 64
    groups = tokens // group
    loads = [pltpu.make_async_copy(ids, ids_s, s_ids.at[0]), pltpu.make_async_copy(ids_row, ids_v, s_ids.at[1])]
    for c in loads:
        c.start()
    zero[...] = jnp.zeros_like(zero)
    fill_start(zero, table_g, s_zero, 0)
    loads[0].wait()

    def fetch(k, carry):
        for i in range(group):
            token = k * group + i
            lid = ids_s[token] - base
            owned = (lid >= 0) & (lid < vocab)
            row = jnp.where(owned, lid & -2, 2 * token)
            pltpu.make_async_copy(table.at[pl.ds(pl.multiple_of(row, 2), 2)], pairs.at[k, pl.ds(2 * i, 2)], sems.at[k]).start()
        return carry

    lax.fori_loop(0, groups, fetch, 0)
    loads[1].wait()
    row = jnp.broadcast_to(ids_v[...].astype(F32), (tokens, tokens))
    col = row.T
    equal = row == col
    same[...] = jnp.where(equal, 1.0, 0.0).astype(BF)
    earlier = lax.broadcasted_iota(I32, (tokens, tokens), 0) < lax.broadcasted_iota(I32, (tokens, tokens), 1)
    repeat = jnp.max(jnp.where(equal & earlier, 1, 0), axis=0, keepdims=True)
    mine = ids_v[...] - base
    rows_mine[...] = jnp.where((mine >= 0) & (mine < vocab) & (repeat == 0), mine, -1)
    lid = col.astype(I32) - base
    lane = lax.broadcasted_iota(I32, (group, 2 * group), 1)
    first = lax.broadcasted_iota(I32, (group, 2 * group), 0) * 2
    for k in range(groups):
        at = lid[k * group:(k + 1) * group, :2 * group]
        owned = (at >= 0) & (at < vocab)
        pick = jnp.where(owned & (lane == first + (at & 1)), 1.0, 0.0).astype(BF)
        pltpu.make_async_copy(table.at[pl.ds(0, group * 2)], pairs.at[k], sems.at[k]).wait()
        part[pl.ds(k * group, group), :] = mm(pick, pairs[k], 1, 0).astype(BF)
    fill_wait(zero, table_g, s_zero, 0)


def lookup(ids, table):
    tokens, (vocab, width) = ids.shape[0], table.shape
    return pl.pallas_call(
        lookup_kernel,
        name="lookup",
        out_shape=[sh((tokens, width), BF), sh((1, tokens), I32), sh((tokens, tokens), BF), sh((ZERO_ROWS, width), F32), sh((vocab, width), F32)],
        in_specs=[HBM_SPEC] * 3,
        out_specs=[VMEM_SPEC] * 4 + [HBM_SPEC],
        scratch_shapes=[pltpu.SMEM((tokens,), I32), VMEM((1, tokens), I32), VMEM((4, tokens // 2, width), BF), DMA((4,)), DMA(()), DMA((2,))],
        compiler_params=pltpu.CompilerParams(vmem_limit_bytes=LOOKUP_VMEM),
        cost_estimate=pl.CostEstimate(flops=5_000_000_000, bytes_accessed=10 * MIB, transcendentals=0),
    )(in_hbm(ids), in_hbm(ids.reshape(1, tokens)), in_hbm(table))


def pair_kernel(part, w1, send, w1_v, part_r, sems, s_in):
    me = lax.axis_index("tp")
    rows = part.shape[0] // 4
    blocks = (me, me ^ 2, me ^ 1, me ^ 3)
    load = pltpu.make_async_copy(w1, w1_v, s_in)
    load.start()
    remote = swap_with_sibling()
    block = lambda k: pl.ds(pl.multiple_of(blocks[k] * rows, rows), rows)
    copies = [remote(part.at[block(2 + k)], part_r.at[pl.ds(k * rows, rows)], sems, k) for k in range(2)]
    for c in copies:
        c.start()
    for k in range(2):
        copies[k].wait()
        at = pl.ds(k * rows, rows)
        send[at, :] = part[block(k), :] + part_r[at, :]
    load.wait()


def pair(part, w1):
    rows, width = part.shape[0] // 4, part.shape[1]
    return pl.pallas_call(
        pair_kernel,
        name="pair",
        out_shape=[sh((2 * rows, width), BF), sh(w1.shape, BF)],
        in_specs=[VMEM_SPEC, HBM_SPEC],
        out_specs=[VMEM_SPEC] * 2,
        scratch_shapes=[VMEM((2 * rows, width), BF), DMA((2, 2)), DMA(())],
        compiler_params=pltpu.CompilerParams(collective_id=0, has_side_effects=True, vmem_limit_bytes=PAIR_VMEM),
        cost_estimate=pl.CostEstimate(flops=3_000_000_000, bytes_accessed=MIB, transcendentals=0),
    )(part, in_hbm(w1))


def fill1_kernel(rows_mine, zero, w2, order, table_in, puts, w2_v, table_g, mine_s, puts_s, s_zero, s_list, s_w):
    load = pltpu.make_async_copy(rows_mine, mine_s, s_list)
    load.start()
    load_w = pltpu.make_async_copy(w2, w2_v, s_w)
    load_w.start()
    fill_start(zero, table_g, s_zero, 1)
    tokens = rows_mine.shape[1]
    load.wait()

    def body(i, count):
        lid = mine_s[0, i]
        puts_s[count] = lid | (i << 16)
        return count + (lid >= 0).astype(I32)

    puts_s[tokens] = lax.fori_loop(0, tokens, body, 0, unroll=8)
    store = pltpu.make_async_copy(puts_s, puts, s_list)
    store.start()
    store.wait()
    load_w.wait()
    fill_wait(zero, table_g, s_zero, 1)


def fill1(rows_mine, zero, w2, order, table_g):
    tokens = rows_mine.shape[1]
    return pl.pallas_call(
        fill1_kernel,
        name="fill1",
        out_shape=[sh((2 * tokens,), I32), sh(w2.shape, BF), sh(table_g.shape, F32)],
        in_specs=[ANY_SPEC, VMEM_SPEC, HBM_SPEC, ANY_SPEC, HBM_SPEC],
        out_specs=[ANY_SPEC, VMEM_SPEC, HBM_SPEC],
        input_output_aliases={4: 2},
        scratch_shapes=[pltpu.SMEM((1, tokens), I32), pltpu.SMEM((2 * tokens,), I32), DMA(()), DMA(()), DMA(())],
        compiler_params=pltpu.CompilerParams(vmem_limit_bytes=8 * MIB),
        cost_estimate=pl.CostEstimate(flops=9_000_000_000, bytes_accessed=20 * MIB, transcendentals=0),
    )(rows_mine, zero, in_hbm(w2), order, table_g)


def mlp_half(x, d, n, h, du, at, w1, w2, gain):
    first, count = at
    width, hid = n.shape[1], h.shape[1]
    gain_f = gain[...].astype(F32).reshape(1, width)
    for j in range(count // 32):
        rows = pl.ds(first + j * 32, 32)
        x_f = x[rows, :].astype(F32)
        r = lax.rsqrt(jnp.mean(x_f * x_f, axis=-1, keepdims=True) + EPS)
        n[rows, :] = (x_f * r * gain_f).astype(BF)
    rows = pl.ds(first, count)
    for j in range(hid // TILE):
        cols = pl.ds(j * TILE, TILE)
        g = mm(d[rows, :], w2[cols, :], 1, 1).astype(BF).astype(F32)
        u = mm(n[rows, :], w1[:, cols], 1, 0).astype(BF).astype(F32)
        t = jnp.tanh(GELU_C * (u + GELU_A * (u * u * u)))
        cdf = 0.5 * (1.0 + t)
        h[rows, cols] = (u * cdf).astype(BF)
        du[rows, cols] = (g * (cdf + u * (0.5 * (1.0 - t * t)) * (GELU_C * (1.0 + 3.0 * GELU_A * (u * u))))).astype(BF)


def share_kernel(send, got, d_own, d_far, w1, w2, gain, x_f, n_a, h_a, du_a, x_r, d_a, sems):
    rows = d_own.shape[0]
    half = 2 * rows
    remote = swap_with_sibling()
    copies = []
    for k in range(2):
        at, other = pl.ds(k * rows, rows), pl.ds((1 - k) * rows, rows)
        x_f[at, :] = send[at, :] + got[other, :]
        copies.append(remote(x_f.at[at], x_r.at[at], sems, k))
        copies[-1].start()
    for k, src in enumerate((d_own, d_far)):
        d_a[pl.ds(k * rows, rows), :] = src[...]
    mlp_half(x_f, d_a, n_a, h_a, du_a, (0, half), w1, w2, gain)
    for k in range(2):
        copies[k].wait()
        x_f[pl.ds(half + k * rows, rows), :] = x_r[pl.ds(k * rows, rows), :]


def share(send, got, d_own, d_far, w1, w2, gain):
    rows, width = d_own.shape
    hid = w1.shape[1]
    return pl.pallas_call(
        share_kernel,
        name="share",
        out_shape=[sh((4 * rows, width), BF), sh((2 * rows, width), BF)] + [sh((2 * rows, hid), BF)] * 2,
        in_specs=[VMEM_SPEC] * 7,
        out_specs=[VMEM_SPEC] * 4,
        scratch_shapes=[VMEM((2 * rows, width), BF), VMEM((2 * rows, width), BF), DMA((2, 2))],
        compiler_params=pltpu.CompilerParams(collective_id=1, has_side_effects=True, vmem_limit_bytes=16 * MIB),
        cost_estimate=pl.CostEstimate(flops=3_000_000_000, bytes_accessed=MIB, transcendentals=0),
    )(send, got, d_own, d_far, w1, w2, gain)


def mlp_kernel(x_f, d_own, d_far, d_own_s, d_far_s, n_a, h_a, du_a, w1, w2, gain, zero, table_in,
               n, h, du, d_full, dn_b0, dn_b1, table_g, s_zero):
    fill_start(zero, table_g, s_zero, 2)
    rows = d_own.shape[0]
    for k, src in enumerate((d_own, d_far, d_own_s, d_far_s)):
        d_full[pl.ds(k * rows, rows), :] = src[...]
    tokens, width = n.shape
    half = tokens // 2
    for out, src in ((n, n_a), (h, h_a), (du, du_a)):
        out[pl.ds(0, half), :] = src[...]
    mlp_half(x_f, d_full, n, h, du, (half, half), w1, w2, gain)
    for j in range(width // TILE):
        cols = pl.ds(j * TILE, TILE)
        dn = mm(du[pl.ds(half, half), :], w1[cols, :], 1, 1)
        dn_b0[:, cols] = dn[:half // 2]
        dn_b1[:, cols] = dn[half // 2:]
    fill_wait(zero, table_g, s_zero, 2)


def mlp(x_f, ds, n_a, h_a, du_a, w1, w2, gain, zero, table_g):
    tokens, width = x_f.shape
    hid = w1.shape[1]
    return pl.pallas_call(
        mlp_kernel,
        name="mlp",
        out_shape=[sh((tokens, width), BF), sh((tokens, hid), BF), sh((tokens, hid), BF), sh((tokens, width), BF),
                   sh((tokens // 4, width), F32), sh((tokens // 4, width), F32), sh(table_g.shape, F32)],
        in_specs=[VMEM_SPEC] * 12 + [HBM_SPEC],
        out_specs=[VMEM_SPEC] * 6 + [HBM_SPEC],
        input_output_aliases={12: 6},
        scratch_shapes=[DMA(())],
        compiler_params=pltpu.CompilerParams(vmem_limit_bytes=16 * MIB),
        cost_estimate=pl.CostEstimate(flops=6_000_000_000, bytes_accessed=4 * MIB, transcendentals=0),
    )(x_f, *ds, n_a, h_a, du_a, w1, w2, gain, zero, table_g)


def sums_kernel(dn_b1, du, h, w1, w2, dn_own, dn_far, y_a, y_b, dn_r, sems):
    rows, width = dn_own.shape
    half = 2 * rows
    remote = swap_with_sibling()
    copy = remote(dn_b1, dn_r, sems, 0)
    copy.start()
    for j in range(width // TILE):
        cols = pl.ds(j * TILE, TILE)
        dn = mm(du[pl.ds(0, half), :], w1[cols, :], 1, 1)
        dn_own[:, cols] = dn[:rows]
        dn_far[:, cols] = dn[rows:]
    for j in range(width // TILE):
        cols = pl.ds(j * TILE, TILE)
        y = mm(h[...], w2[:, cols], 1, 0)
        y_a[:, cols] = y[:half]
        y_b[:, cols] = y[half:]
    copy.wait()
    dn_far[...] += dn_r[...]


def sums(dn_b1, du, h, w1, w2):
    rows, width = dn_b1.shape
    return pl.pallas_call(
        sums_kernel,
        name="sums",
        out_shape=[sh((rows, width), F32)] * 2 + [sh((2 * rows, width), F32)] * 2,
        in_specs=[VMEM_SPEC] * 5,
        out_specs=[VMEM_SPEC] * 4,
        scratch_shapes=[VMEM((rows, width), F32), DMA((2, 1))],
        compiler_params=pltpu.CompilerParams(collective_id=2, has_side_effects=True, vmem_limit_bytes=16 * MIB),
        cost_estimate=pl.CostEstimate(flops=4_000_000_000, bytes_accessed=4 * MIB, transcendentals=0),
    )(dn_b1, du, h, w1, w2)


def grads1_kernel(n, du, zero, order, table_in, dw1, table_g, dw1_v, s_zero, s_w):
    width = n.shape[1]
    n_t = n[...].T
    for j in range(width // TILE):
        at = slice(j * TILE, (j + 1) * TILE)
        dw1_v[at, :] = mm(n_t[at, :], du[...], 1, 0)
        pltpu.make_async_copy(dw1_v.at[pl.ds(j * TILE, TILE)], dw1.at[pl.ds(j * TILE, TILE)], s_w).start()
        if j == 0:
            fill_start(zero, table_g, s_zero, 3)
    pltpu.make_async_copy(dw1_v, dw1, s_w).wait()
    fill_wait(zero, table_g, s_zero, 3)


def grads1(n, du, zero, order, table_g):
    width, hid = n.shape[1], du.shape[1]
    return pl.pallas_call(
        grads1_kernel,
        name="grads1",
        out_shape=[sh((width, hid), F32), sh(table_g.shape, F32)],
        in_specs=[VMEM_SPEC] * 3 + [ANY_SPEC, HBM_SPEC],
        out_specs=[HBM_SPEC, HBM_SPEC],
        input_output_aliases={4: 1},
        scratch_shapes=[VMEM((width, hid), F32), DMA(()), DMA(())],
        compiler_params=pltpu.CompilerParams(vmem_limit_bytes=16 * MIB),
        cost_estimate=pl.CostEstimate(flops=4_000_000_000, bytes_accessed=8 * MIB, transcendentals=0),
    )(n, du, zero, order, table_g)


def grads2_kernel(h, d_full, y_a, y_sib, zero, table_in, dw2, y_own, y_far, table_g, dw2_v, s_zero, s_w):
    rows = y_own.shape[0]
    hid = h.shape[1]
    fill_start(zero, table_g, s_zero, 4)
    for k, out in enumerate((y_own, y_far)):
        at = pl.ds(k * rows, rows)
        out[...] = y_a[at, :] + y_sib[at, :]
    h_t = h[...].T
    for j in range(hid // TILE):
        at = slice(j * TILE, (j + 1) * TILE)
        dw2_v[at, :] = mm(h_t[at, :], d_full[...], 1, 0)
        pltpu.make_async_copy(dw2_v.at[pl.ds(j * TILE, TILE)], dw2.at[pl.ds(j * TILE, TILE)], s_w).start()
    pltpu.make_async_copy(dw2_v, dw2, s_w).wait()
    fill_wait(zero, table_g, s_zero, 4)


def grads2(h, d_full, y_a, y_sib, zero, table_g):
    hid, width = h.shape[1], d_full.shape[1]
    rows = y_a.shape[0] // 2
    return pl.pallas_call(
        grads2_kernel,
        name="grads2",
        out_shape=[sh((hid, width), F32)] + [sh((rows, width), F32)] * 2 + [sh(table_g.shape, F32)],
        in_specs=[VMEM_SPEC] * 5 + [HBM_SPEC],
        out_specs=[HBM_SPEC, VMEM_SPEC, VMEM_SPEC, HBM_SPEC],
        input_output_aliases={5: 3},
        scratch_shapes=[VMEM((hid, width), F32), DMA(()), DMA(())],
        compiler_params=pltpu.CompilerParams(vmem_limit_bytes=16 * MIB),
        cost_estimate=pl.CostEstimate(flops=4_000_000_000, bytes_accessed=8 * MIB, transcendentals=0),
    )(h, d_full, y_a, y_sib, zero, table_g)


def dx_kernel(dn_own, dn_sib, g2, x_own, d_own, gain, order, dx):
    gain_f = gain[...].astype(F32).reshape(1, dx.shape[1])
    for j in range(dx.shape[0] // 16):
        at = pl.ds(j * 16, 16)
        a = (dn_own[at, :] + dn_sib[at, :] + g2[at, :]) * gain_f
        x = x_own[at, :].astype(F32)
        r = lax.rsqrt(jnp.mean(x * x, axis=-1, keepdims=True) + EPS)
        proj = jnp.mean(a * x, axis=-1, keepdims=True)
        dx[at, :] = (d_own[at, :].astype(F32) + r * (a - x * r * r * proj)).astype(BF)


def dx_rows(dn_own, dn_sib, g2, x_own, d_own, gain, order):
    return pl.pallas_call(
        dx_kernel,
        name="dx_rows",
        out_shape=sh(d_own.shape, BF),
        in_specs=[VMEM_SPEC] * 6 + [ANY_SPEC],
        out_specs=VMEM_SPEC,
        compiler_params=pltpu.CompilerParams(vmem_limit_bytes=4 * MIB),
        cost_estimate=pl.CostEstimate(flops=1_000_000_000, bytes_accessed=MIB, transcendentals=0),
    )(dn_own, dn_sib, g2, x_own, d_own, gain, order)


def fill3_kernel(zero, order, table_in, token, table_g, s_zero):
    fill_start(zero, table_g, s_zero, 5)
    token[...] = jnp.zeros_like(token)
    fill_wait(zero, table_g, s_zero, 5)


def fill3(zero, order, table_g):
    return pl.pallas_call(
        fill3_kernel,
        name="fill3",
        out_shape=[sh((8, 128), F32), sh(table_g.shape, F32)],
        in_specs=[VMEM_SPEC, ANY_SPEC, HBM_SPEC],
        out_specs=[VMEM_SPEC, HBM_SPEC],
        input_output_aliases={2: 1},
        scratch_shapes=[DMA(())],
        compiler_params=pltpu.CompilerParams(vmem_limit_bytes=4 * MIB),
        cost_estimate=pl.CostEstimate(flops=4_000_000_000, bytes_accessed=16 * MIB, transcendentals=0),
    )(zero, order, table_g)


def dx_all_kernel(dx, dx_sib, dx_far, order, dx_out, dx_r, sems):
    me = lax.axis_index("tp")
    rows = dx.shape[0]
    remote = swap_with_sibling()
    block = lambda m: pl.ds(pl.multiple_of((me ^ m) * rows, rows), rows)
    copy = remote(dx_far, dx_r, sems, 0)
    copy.start()
    for m, src in enumerate((dx, dx_sib, dx_far)):
        dx_out[block(m), :] = src[...]
    copy.wait()
    dx_out[block(3), :] = dx_r[...]


def dx_all(dx, dx_sib, dx_far, order):
    rows, width = dx.shape
    return pl.pallas_call(
        dx_all_kernel,
        name="dx_all",
        out_shape=sh((4 * rows, width), BF),
        in_specs=[VMEM_SPEC] * 3 + [ANY_SPEC],
        out_specs=VMEM_SPEC,
        scratch_shapes=[VMEM((rows, width), BF), DMA((2, 1))],
        compiler_params=pltpu.CompilerParams(collective_id=3, has_side_effects=True, vmem_limit_bytes=4 * MIB),
        cost_estimate=pl.CostEstimate(flops=2_000_000_000, bytes_accessed=MIB, transcendentals=0),
    )(dx, dx_sib, dx_far, order)


def put_kernel(puts, same, dx, zero, table_in, table_g, token, puts_s, total, s_in, s_row, s_zero):
    fill_start(zero, table_g, s_zero, LATE)
    tokens = dx.shape[0]
    load = pltpu.make_async_copy(puts, puts_s, s_in)
    load.start()
    total[...] = mm(same[...], dx[...], 1, 0)
    token[...] = jnp.zeros_like(token)
    load.wait()
    fill_wait(zero, table_g, s_zero, LATE)
    count = puts_s[tokens]

    def put(i):
        word = puts_s[i]
        pltpu.make_async_copy(total.at[pl.ds(word >> 16, 1)], table_g.at[pl.ds(word & 0xFFFF, 1)], s_row).start()

    def put_four(i, carry):
        for k in range(4):
            put(i * 4 + k)
        return carry

    def put_one(i, carry):
        put(i)
        return carry

    lax.fori_loop(0, count >> 2, put_four, 0)
    lax.fori_loop((count >> 2) * 4, count, put_one, 0)

    def put_wait(size):
        def body(i, carry):
            pltpu.make_async_copy(total.at[pl.ds(0, size)], table_g.at[pl.ds(0, size)], s_row).wait()
            return carry

        return body

    lax.fori_loop(0, count >> 3, put_wait(8), 0)
    lax.fori_loop(0, count & 7, put_wait(1), 0)


def put_rows(puts, same, dx, zero, table_g):
    return pl.pallas_call(
        put_kernel,
        name="put_rows",
        out_shape=[sh(table_g.shape, F32), sh((8, 128), F32)],
        in_specs=[ANY_SPEC, VMEM_SPEC, VMEM_SPEC, VMEM_SPEC, HBM_SPEC],
        out_specs=[HBM_SPEC, VMEM_SPEC],
        input_output_aliases={4: 0},
        scratch_shapes=[pltpu.SMEM(puts.shape, I32), VMEM(dx.shape, F32), DMA(()), DMA(()), DMA(())],
        compiler_params=pltpu.CompilerParams(vmem_limit_bytes=4 * MIB),
        cost_estimate=pl.CostEstimate(flops=3_000_000_000, bytes_accessed=2 * MIB, transcendentals=0),
    )(puts, same, dx, zero, table_g)


def finish_kernel(x, y, y_in, order, out):
    out[...] = (x[pl.ds(0, out.shape[0]), :].astype(F32) + (y[...] + y_in[...])).astype(BF)


def finish(x, y, y_in, order):
    return pl.pallas_call(
        finish_kernel,
        name="finish",
        out_shape=sh(y.shape, BF),
        in_specs=[VMEM_SPEC] * 3 + [ANY_SPEC],
        out_specs=VMEM_SPEC,
        compiler_params=pltpu.CompilerParams(vmem_limit_bytes=4 * MIB),
        cost_estimate=pl.CostEstimate(flops=1_000_000_000, bytes_accessed=MIB, transcendentals=0),
    )(x, y, y_in, order)


def solution(mesh):
    tp = mesh.shape["tp"]

    def permute(x, hop):
        return lax.ppermute(x, "tp", [(i, i ^ hop) for i in range(tp)])

    def shard_step(ids, table, gain, w1, w2, d_out):
        part, rows_mine, same, zero, d_table = lookup(ids, table)
        part, d_send = lax.optimization_barrier((part, d_out))
        d_far = permute(d_send, 2)
        send, w1 = pair(part, w1)
        got = permute(send, 2)
        d_own_s = permute(d_out, 1)
        puts, w2, d_table = fill1(rows_mine, zero, w2, send, d_table)
        d_far_s = permute(d_far, 1)
        x_f, n_a, h_a, du_a = share(send, got, d_out, d_far, w1, w2, gain)
        ds = (d_out, d_far, d_own_s, d_far_s)
        n, h, du, d_full, dn_b0, dn_b1, d_table = mlp(x_f, ds, n_a, h_a, du_a, w1, w2, gain, zero, d_table)
        dn_own, dn_far, y_a, y_b = sums(dn_b1, du, h, w1, w2)
        g2 = permute(dn_far, 2)
        dn_sib = permute(dn_b0, 1)
        y_sib = permute(y_b, 1)
        d_w1, d_table = grads1(n, du, zero, dn_own, d_table)
        d_w2, y_own, y_far, d_table = grads2(h, d_full, y_a, y_sib, zero, d_table)
        dx = dx_rows(dn_own, dn_sib, g2, x_f, d_out, gain, y_own)
        dx_far = permute(dx, 2)
        dx_sib = permute(dx, 1)
        dx, y_far = lax.optimization_barrier((dx, y_far))
        y_in = permute(y_far, 2)
        token, d_table = fill3(zero, dx, d_table)
        dx_full = dx_all(dx, dx_sib, dx_far, token)
        d_table, done = put_rows(puts, same, dx_full, zero, d_table)
        out = finish(x_f, y_own, y_in, done)
        return out, d_table, d_w1, d_w2

    return jax.shard_map(
        shard_step,
        mesh=mesh,
        in_specs=(P("dp"), P("tp", None), P(None), P(None, "tp"), P("tp", None), P(("dp", "tp"), None)),
        out_specs=(P(("dp", "tp"), None), P(("dp", "tp"), None), P("dp", "tp"), P(("dp", "tp"), None)),
        check_vma=False,
    )
```
